8 devices in a mesh: dp: 2 (over y, z), tp: 4 (over x, core).
Axes of the slice: x: 2, y: 2, z: 1, core: 2. Of those that a mesh axis runs over, the one named last changes fastest.
Arguments:
- x: bfloat16 [2048, 4608], P(('dp', 'tp')), parts along dimension 0
- gain: bfloat16 [4608], replicated
- wq: bfloat16 [4608, 4096], P(None, 'tp')
- wk: bfloat16 [4608, 2048], P(None, 'tp')
- wv: bfloat16 [4608, 2048], P(None, 'tp')
- wo: bfloat16 [4096, 4608], P('tp')
Outputs:
- output: bfloat16 [2048, 4608], P(('dp', 'tp')), parts along dimension 0
There are 2 independent parts. The reference program is written for one: setup_inputs(seed, part) draws one part's arguments, and reference() takes and returns one part's arrays. A program takes and returns all parts, laid end to end along the dimension named above; an argument that names none is the same for every part.
All inputs are finite; a program needn't handle non-finite values.
Results may differ from the reference program's by a relative error of at most 0.012.
Values are sent between devices in bfloat16 or wider.
A program may use at most 2 GiB of HBM per device.

```python
import jax
import jax.numpy as jnp
from jax import lax

ROWS = 1024
D = 4608
HEADS = 32
KV_HEADS = 16
HEAD = 128
THETA = 10000


def setup_inputs(seed: int = 0, part: int = 0) -> dict:
    kx, kn, kq, kk, kv, ko = jax.random.split(jax.random.key(seed), 6)

    def weights(key, rows, columns):
        return jax.random.normal(key, (rows, columns), jnp.float32) * rows**-0.5

    drawn = {
        "x": jax.random.normal(jax.random.fold_in(kx, part), (ROWS, D), jnp.float32),
        "gain": 1 + 0.1 * jax.random.normal(kn, (D,), jnp.float32),
        "wq": 2 * weights(kq, D, HEADS * HEAD),
        "wk": 2 * weights(kk, D, KV_HEADS * HEAD),
        "wv": 4 * weights(kv, D, KV_HEADS * HEAD),
        "wo": weights(ko, HEADS * HEAD, D),
    }
    return {k: v.astype(jnp.bfloat16) for k, v in drawn.items()}


def normed(x, gain):
    wide = x.astype(jnp.float32)
    scale = lax.rsqrt(jnp.mean(wide * wide, -1, keepdims=True) + 1e-6)
    return (wide * scale * gain.astype(jnp.float32)).astype(jnp.bfloat16)


def turned(t, place, theta):
    half = t.shape[-1] // 2
    angle = place.astype(jnp.float32)[:, None] * theta ** (-jnp.arange(half, dtype=jnp.float32) / half)
    cos, sin = jnp.cos(angle)[:, None], jnp.sin(angle)[:, None]
    a, b = t[..., :half].astype(jnp.float32), t[..., half:].astype(jnp.float32)
    return jnp.concatenate([a * cos - b * sin, b * cos + a * sin], -1).astype(jnp.bfloat16)


def matmul(a, w):
    return jnp.dot(a, w, preferred_element_type=jnp.float32).astype(jnp.bfloat16)


def einsum(form, a, b):
    return jnp.einsum(form, a.astype(jnp.float32), b.astype(jnp.float32))


def attention(q, k, v):
    scores = einsum("tgsd,ugd->gstu", q, k) * q.shape[-1] ** -0.5
    token = jnp.arange(q.shape[0])
    scores = jnp.where(token[:, None] >= token, scores, -jnp.inf)
    weights = jax.nn.softmax(scores, -1).astype(jnp.bfloat16)
    return einsum("gstu,ugd->tgsd", weights, v).astype(jnp.bfloat16)


def reference(x, gain, wq, wk, wv, wo):
    a, place = normed(x, gain), jnp.arange(ROWS)
    q = turned(matmul(a, wq).reshape(ROWS, HEADS, HEAD), place, THETA).reshape(ROWS, KV_HEADS, -1, HEAD)
    k = turned(matmul(a, wk).reshape(ROWS, KV_HEADS, HEAD), place, THETA)
    v = matmul(a, wv).reshape(ROWS, KV_HEADS, HEAD)
    seen = attention(q, k, v).reshape(ROWS, HEADS * HEAD)
    return (x.astype(jnp.float32) + jnp.dot(seen, wo, preferred_element_type=jnp.float32)).astype(jnp.bfloat16)
```

```python
import functools

import jax
import jax.numpy as jnp
import numpy as np
from jax import lax
from jax.experimental import pallas as pl
from jax.experimental.pallas import tpu as pltpu
from jax.sharding import PartitionSpec as P

HEAD = 128
THETA = 10000
NEG = -1e30
HIDDEN = 2 * NEG
LOG2E = 1.4426950408889634
VMEM = 67043328
MESH = pl.DeviceIdType.MESH
F32, BF16 = jnp.float32, jnp.bfloat16

B = 256
SUB = 64
TILE = 768


def _dot(a, b, ca=1, cb=0):
    return lax.dot_general(a, b, (((ca,), (cb,)), ((), ())), preferred_element_type=F32)


def _layer(x_ref, gain_ref, cos_ref, sin_ref, wq_ref, wk_ref, wv_ref, wo_ref, y_ref,
           xs, a_s, gain_s, cos_s, sin_s, wq_s, wk_s, wv_s, wo_s, q_s, k_s, v_s, top_s, mix_s,
           peer_out, peer_in, far_in, term_in, acc_s,
           load_sem, own_ss, own_rs, x_ss, x_rs, pass_ss, pass_rs, half_ss, half_rs, far_ss, far_rs, term_ss, term_rs, out_sem):
    d = x_ref.shape[1]
    half = d // 2
    tiles = half // TILE
    nq, nk = wq_s.shape[1], wk_s.shape[1]
    heads, group = nq // HEAD, nq // nk
    me = lax.axis_index("tp")
    p, c = lax.div(me, 2), lax.rem(me, 2)
    peer, cross, diag = 2 * p + 1 - c, 2 * (1 - p) + c, 2 * (1 - p) + 1 - c

    def rows(block, at=0, n=B):
        return pl.ds(pl.multiple_of(block * B + at, SUB), n)

    def load(i, src, dst):
        return pltpu.make_async_copy(src, dst, load_sem.at[i])

    loads = [load(0, x_ref, xs.at[rows(me)]), load(1, gain_ref, gain_s), load(2, cos_ref, cos_s), load(3, sin_ref, sin_s),
             load(4, wk_ref, wk_s), load(5, wv_ref, wv_s), load(6, wq_ref, wq_s), load(7, wo_ref, wo_s)]
    for copy in loads[:2]:
        copy.start()

    def remote(src, dst, send, recv, to):
        return pltpu.make_async_remote_copy(src_ref=src, dst_ref=dst, send_sem=send, recv_sem=recv, device_id={"tp": to}, device_id_type=MESH)

    barrier = pltpu.get_barrier_semaphore()
    for other in (peer, cross, diag):
        pl.semaphore_signal(barrier, inc=1, device_id={"tp": other}, device_id_type=MESH)
    pl.semaphore_wait(barrier, 3)

    def own(i):
        at = (1 - c if i == 0 else c) * (B // 2)
        return remote(x_ref.at[pl.ds(pl.multiple_of(at, B // 2), B // 2)], xs.at[rows(me, at, B // 2)], own_ss.at[i], own_rs.at[i], peer)

    def across(b, h, mine):
        at = c * (B // 2) + h * SUB
        there = xs.at[rows(2 * p + b, at, SUB)]
        src = x_ref.at[pl.ds(pl.multiple_of(at, SUB), SUB)] if mine else there
        return remote(src, there, x_ss.at[b * 2 + h], x_rs.at[b * 2 + h], cross)

    def passed(b, h):
        here = xs.at[rows(2 * (1 - p) + b, c * (B // 2) + h * SUB, SUB)]
        return remote(here, here, pass_ss.at[b * 2 + h], pass_rs.at[b * 2 + h], peer)

    @pl.when(c == 0)
    def _():
        for h in range(2):
            across(0, h, True).start()

    for i in range(2):
        own(i).start()
    for copy in loads[2:]:
        copy.start()
    own(0).wait_recv()

    @pl.when(c == 1)
    def _():
        for h in range(2):
            across(0, h, False).start()
        for h in range(2):
            across(1, h, True).start()

    @pl.when(c == 0)
    def _():
        for h in range(2):
            across(1, h, False).start()

    own(1).wait_recv()
    for copy in loads[:4]:
        copy.wait()
    for g in range(nk // HEAD):
        v_s[g, HEAD:, :] = jnp.ones((v_s.shape[1] - HEAD, v_s.shape[2]), BF16)

    def norm(tb):
        def some(i, _):
            at = pl.ds(pl.multiple_of(tb * B + i * 16, 16), 16)
            wide = xs[at, :].astype(F32)
            scale = lax.rsqrt(jnp.mean(wide * wide, -1, keepdims=True) + 1e-6)
            a_s[pl.ds(pl.multiple_of(i * 16, 16), 16), :] = (wide * scale * gain_s[...].astype(F32)).astype(BF16)

        lax.fori_loop(0, B // 16, some, None)

    def project(tb):
        here = rows(tb)
        cos, sin = cos_s[here, :], sin_s[here, :]

        def turned(t):
            t = t.astype(BF16).astype(F32)
            return (t * cos + pltpu.roll(t, HEAD // 2, 1) * sin).astype(BF16)

        k = _dot(a_s[...], wk_s[...])
        for n in range(0, nk, HEAD):
            k_s[here, n : n + HEAD] = turned(k[:, n : n + HEAD])
        v = _dot(a_s[...], wv_s[...])
        for g in range(nk // HEAD):
            v_s[g, :HEAD, here] = v[:, g * HEAD : (g + 1) * HEAD].T.astype(BF16)

        def queries(i, _):
            at = pl.multiple_of(i * 512, 512)
            q = _dot(a_s[...], wq_s[:, pl.ds(at, 512)])
            for n in range(0, 512, HEAD):
                q_s[here, pl.ds(at + n, HEAD)] = turned(q[:, n : n + HEAD])

        lax.fori_loop(0, nq // 512, queries, None)

    def attend(tb):
        here = rows(tb)
        e = HEAD**-0.5 * LOG2E
        top_s[...] = jnp.full(top_s.shape, NEG, F32)
        mix_s[...] = jnp.zeros(mix_s.shape, F32)

        def block(j, masked):
            keys = rows(j)
            seen = None
            if masked:
                seen = lax.broadcasted_iota(jnp.int32, (B, B), 0) <= lax.broadcasted_iota(jnp.int32, (B, B), 1)
            scores = [_dot(k_s[keys, h // group * HEAD : (h // group + 1) * HEAD], q_s[here, h * HEAD : (h + 1) * HEAD], 1, 1) for h in range(heads)]
            weights, keeps = [], []
            for h, s in enumerate(scores):
                if masked:
                    s = jnp.where(seen, s, HIDDEN)
                old = top_s[h : h + 1, :]
                top = jnp.maximum(old, s.max(axis=0, keepdims=True))
                top_s[h : h + 1, :] = top
                weights.append(jnp.exp2((s - top) * e).astype(BF16))
                keeps.append(jnp.exp2((old - top) * e))
            for h in range(heads):
                mix_s[h] = mix_s[h] * keeps[h] + _dot(v_s[h // group, :, keys], weights[h])

        lax.fori_loop(0, tb, lambda j, _: block(j, False), None)
        block(tb, True)
        for h in range(heads):
            out = mix_s[h, :HEAD, :] * (1 / mix_s[h, HEAD : HEAD + 1, :])
            q_s[here, h * HEAD : (h + 1) * HEAD] = out.T.astype(BF16)

    def columns(side, t):
        return pl.ds(pl.multiple_of(side * half + t * TILE, TILE), TILE)

    def part(tb, side, t):
        return _dot(q_s[rows(tb), :], wo_s[:, columns(side, t)])

    def at_tile(t):
        return pl.ds(pl.multiple_of(t * TILE, TILE), TILE)

    def to_peer(b, t):
        return remote(peer_out.at[b, :, at_tile(t)], peer_in.at[b, :, at_tile(t)], half_ss.at[b * tiles + t], half_rs.at[b * tiles + t], peer)

    def to_far(b, t):
        return remote(peer_in.at[b, :, at_tile(t)], far_in.at[:, columns(c, t)], far_ss.at[b * tiles + t], far_rs.at[c * tiles + t], 2 * (1 - p) + b)

    def to_owner(side, t):
        return remote(peer_out.at[side, :, at_tile(t)], term_in.at[:, columns(side, t)], term_ss.at[side * tiles + t], term_rs.at[side * tiles + t], peer)

    def far(tb, b):
        def give(t, _):
            peer_out[b, :, at_tile(t)] = part(tb, 1 - c, t).astype(BF16)
            to_peer(b, t).start()

        def add(t, _):
            term = part(tb, c, t)
            to_peer(b, t).wait_recv()
            peer_in[b, :, at_tile(t)] = (term + peer_in[b, :, at_tile(t)].astype(F32)).astype(BF16)
            to_far(b, t).start()

        lax.fori_loop(0, tiles, give, None)
        lax.fori_loop(0, tiles, add, None)

    def near(tb):
        def give(i, _):
            side, t = lax.div(i, tiles), lax.rem(i, tiles)
            to_peer(side, t).wait_send()
            peer_out[side, :, at_tile(t)] = part(tb, side, t).astype(BF16)
            to_owner(side, t).start()

        lax.fori_loop(0, 2 * tiles, give, None)

    def mine(tb):
        def keep(i, _):
            side, t = lax.div(i, tiles), lax.rem(i, tiles)
            acc_s[:, columns(side, t)] = xs[rows(tb), columns(side, t)].astype(F32) + part(tb, side, t)

        lax.fori_loop(0, 2 * tiles, keep, None)

    def step(it, _):
        b = it - 2
        away = (it >= 2) & (it < 4)
        tb = jnp.where(it < 4, lax.rem(2 * p + it, 4), 2 * p + lax.rem(it + 1 + c, 2))

        @pl.when(away)
        def _():
            for h in range(2):
                across(b, h, False).wait_recv()
                passed(b, h).start()
            for h in range(2):
                passed(b, h).wait_recv()

        @pl.when(it < 4)
        def _():
            norm(tb)

            @pl.when(it == 0)
            def _():
                for copy in loads[4:7]:
                    copy.wait()

            project(tb)

        @pl.when(it == 2)
        def _():
            loads[7].wait()

        @pl.when(it >= 2)
        def _():
            attend(tb)

        @pl.when(away)
        def _():
            far(tb, b)

        @pl.when(it == 4)
        def _():
            near(tb)

        @pl.when(it == 5)
        def _():
            mine(tb)

    lax.fori_loop(0, 6, step, None)

    def out(side, t):
        return pltpu.make_async_copy(far_in.at[:, columns(side, t)], y_ref.at[:, columns(side, t)], out_sem.at[side * tiles + t])

    def finish(i, _):
        side, t = lax.rem(i, 2), lax.div(i, 2)
        here = columns(side, t)
        to_owner(side, t).wait_recv()
        remote(peer_in.at[0, :, at_tile(t)], far_in.at[:, here], far_ss.at[t], far_rs.at[side * tiles + t], cross).wait_recv()
        far_in[:, here] = (acc_s[:, here] + term_in[:, here].astype(F32) + far_in[:, here].astype(F32)).astype(BF16)
        out(side, t).start()

    lax.fori_loop(0, 2 * tiles, finish, None)
    for i in range(2):
        own(i).wait_send()
        for h in range(2):
            across(i, h, False).wait_send()
            passed(i, h).wait_send()
        for t in range(tiles):
            to_far(i, t).wait_send()
            to_owner(i, t).wait_send()
            out(i, t).wait()


def _tables(tokens):
    half = HEAD // 2
    angle = np.arange(tokens)[:, None] * float(THETA) ** (-np.arange(half) / half)
    cos, sin = np.cos(angle), np.sin(angle)
    return np.concatenate([cos, cos], 1).astype(np.float32), np.concatenate([-sin, sin], 1).astype(np.float32)


def solution(mesh):
    def step(x, gain, wq, wk, wv, wo):
        n, d = x.shape
        tokens = 4 * n
        nq, nk = wq.shape[1], wk.shape[1]
        tiles = d // 2 // TILE
        cos, sin = _tables(tokens)
        vmem, dma = pltpu.VMEM, pltpu.SemaphoreType.DMA
        return pl.pallas_call(
            _layer,
            out_shape=jax.ShapeDtypeStruct((n, d), BF16),
            in_specs=[pl.BlockSpec(memory_space=pltpu.HBM)] * 8,
            out_specs=pl.BlockSpec(memory_space=pltpu.HBM),
            scratch_shapes=[
                vmem((tokens, d), BF16), vmem((n, d), BF16), vmem((1, d), BF16), vmem((tokens, HEAD), F32), vmem((tokens, HEAD), F32),
                vmem(wq.shape, BF16), vmem(wk.shape, BF16), vmem(wv.shape, BF16), vmem(wo.shape, BF16),
                vmem((tokens, nq), BF16), vmem((tokens, nk), BF16), vmem((nk // HEAD, HEAD + 16, tokens), BF16),
                vmem((nq // HEAD, n), F32), vmem((nq // HEAD, HEAD + 16, n), F32),
                vmem((2, n, d // 2), BF16), vmem((2, n, d // 2), BF16), vmem((n, d), BF16), vmem((n, d), BF16), vmem((n, d), F32),
                dma((8,)), dma((2,)), dma((2,)), dma((4,)), dma((4,)), dma((4,)), dma((4,)),
                *[dma((2 * tiles,))] * 7,
            ],
            compiler_params=pltpu.CompilerParams(collective_id=0, has_side_effects=True, vmem_limit_bytes=VMEM),
        )(x, gain.reshape(1, d), cos, sin, wq, wk, wv, wo)

    tokens, columns = P(("dp", "tp"), None), P(None, "tp")
    return jax.shard_map(
        step,
        mesh=mesh,
        in_specs=(tokens, P(None), columns, columns, columns, P("tp", None)),
        out_specs=tokens,
        check_vma=False,
    )
```

```python
import functools

import jax
import jax.numpy as jnp
import numpy as np
from jax import lax
from jax.experimental import pallas as pl
from jax.experimental.pallas import tpu as pltpu
from jax.sharding import PartitionSpec as P

HEAD = 128
THETA = 10000
NEG = -1e30
HIDDEN = 2 * NEG
LOG2E = 1.4426950408889634
VMEM = 67043328 - 2560 * 1024
MESH = pl.DeviceIdType.MESH
F32, BF16 = jnp.float32, jnp.bfloat16

B = 256
SUB = 64
TILE = 256
STORE = 64


def _dot(a, b, ca=1, cb=0):
    return lax.dot_general(a, b, (((ca,), (cb,)), ((), ())), preferred_element_type=F32)


def _layer(x_ref, gain_ref, cos_ref, sin_ref, wq_ref, wk_ref, wv_ref, wo_ref, far_in,
           xs, a_s, gain_s, wide_s, cos_s, sin_s, wq_s, wk_s, wv_s, wo_s, q_s, k_s, v_s, top_s, mix_s,
           peer_out, peer_in, term_in, acc_s,
           load_sem, own_ss, own_rs, x_ss, x_rs, pass_ss, pass_rs, half_ss, half_rs, far_ss, far_rs, term_ss, term_rs):
    d = x_ref.shape[1]
    half = d // 2
    tiles = half // TILE
    nq, nk = wq_s.shape[1], wk_s.shape[1]
    heads, group = nq // HEAD, nq // nk
    me = lax.axis_index("tp")
    p, c = lax.div(me, 2), lax.rem(me, 2)
    peer, cross, diag = 2 * p + 1 - c, 2 * (1 - p) + c, 2 * (1 - p) + 1 - c

    def rows(block, at=0, n=B):
        return pl.ds(pl.multiple_of(block * B + at, SUB), n)

    def load(i, src, dst):
        return pltpu.make_async_copy(src, dst, load_sem.at[i])

    first = [load(8 + i, x_ref.at[pl.ds(i * SUB, SUB)], xs.at[rows(me, i * SUB, SUB)]) for i in range(B // SUB)]
    loads = [load(1, gain_ref, gain_s), load(2, cos_ref, cos_s), load(3, sin_ref, sin_s),
             load(4, wk_ref, wk_s), load(5, wv_ref, wv_s), load(6, wq_ref, wq_s), load(7, wo_ref, wo_s)]
    for copy in first:
        copy.start()

    def remote(src, dst, send, recv, to):
        return pltpu.make_async_remote_copy(src_ref=src, dst_ref=dst, send_sem=send, recv_sem=recv, device_id={"tp": to}, device_id_type=MESH)

    barrier = pltpu.get_barrier_semaphore()
    for other in (peer, cross, diag):
        pl.semaphore_signal(barrier, inc=1, device_id={"tp": other}, device_id_type=MESH)
    pl.semaphore_wait(barrier, 3)

    def own(i):
        at = (1 - c if i == 0 else c) * (B // 2)
        here = xs.at[rows(me, at, B // 2)]
        return remote(here, here, own_ss.at[i], own_rs.at[i], peer)

    def across(b, h):
        here = xs.at[rows(2 * p + b, c * (B // 2) + h * SUB, SUB)]
        return remote(here, here, x_ss.at[b * 2 + h], x_rs.at[b * 2 + h], cross)

    def passed(b, h):
        here = xs.at[rows(2 * (1 - p) + b, c * (B // 2) + h * SUB, SUB)]
        return remote(here, here, pass_ss.at[b * 2 + h], pass_rs.at[b * 2 + h], peer)

    @pl.when(c == 0)
    def _():
        for h in range(2):
            first[h].wait()
            across(0, h).start()

    for copy in first[2:]:
        copy.wait()

    @pl.when(c == 1)
    def _():
        for copy in first[:2]:
            copy.wait()

    for i in range(2):
        own(i).start()
    for copy in loads:
        copy.start()
    own(0).wait_recv()

    @pl.when(c == 1)
    def _():
        for h in range(2):
            across(0, h).start()

    for h in range(2):
        across(1, h).start()

    own(1).wait_recv()
    for copy in loads[:3]:
        copy.wait()
    wide_s[...] = gain_s[...].astype(F32).reshape(wide_s.shape)
    for g in range(nk // HEAD):
        v_s[g, HEAD:, :] = jnp.ones((v_s.shape[1] - HEAD, v_s.shape[2]), BF16)

    def norm(tb):
        def some(i, _):
            at = pl.ds(pl.multiple_of(tb * B + i * 16, 16), 16)
            wide = xs[at, :].astype(F32)
            scale = lax.rsqrt(jnp.mean(wide * wide, -1, keepdims=True) + 1e-6)
            a_s[pl.ds(pl.multiple_of(i * 16, 16), 16), :] = (wide * scale * wide_s[...]).astype(BF16)

        lax.fori_loop(0, B // 16, some, None)

    def project(tb):
        here = rows(tb)
        cos, sin = cos_s[here, :], sin_s[here, :]

        def turned(t):
            t = t.astype(BF16).astype(F32)
            return (t * cos + pltpu.roll(t, HEAD // 2, 1) * sin).astype(BF16)

        k = _dot(a_s[...], wk_s[...])
        for n in range(0, nk, HEAD):
            k_s[here, n : n + HEAD] = turned(k[:, n : n + HEAD])
        v = _dot(a_s[...], wv_s[...])
        for g in range(nk // HEAD):
            v_s[g, :HEAD, here] = v[:, g * HEAD : (g + 1) * HEAD].T.astype(BF16)

        def queries(i, _):
            at = pl.multiple_of(i * 512, 512)
            q = _dot(a_s[...], wq_s[:, pl.ds(at, 512)])
            for n in range(0, 512, HEAD):
                q_s[here, pl.ds(at + n, HEAD)] = turned(q[:, n : n + HEAD])

        lax.fori_loop(0, nq // 512, queries, None)

    def attend(tb):
        here = rows(tb)
        e = HEAD**-0.5 * LOG2E
        top_s[...] = jnp.full(top_s.shape, NEG, F32)
        mix_s[...] = jnp.zeros(mix_s.shape, F32)

        def block(j, masked):
            keys = rows(j)
            seen = None
            if masked:
                seen = lax.broadcasted_iota(jnp.int32, (B, B), 0) <= lax.broadcasted_iota(jnp.int32, (B, B), 1)
            scores = [_dot(k_s[keys, h // group * HEAD : (h // group + 1) * HEAD], q_s[here, h * HEAD : (h + 1) * HEAD], 1, 1) for h in range(heads)]
            weights, keeps = [], []
            for h, s in enumerate(scores):
                if masked:
                    s = jnp.where(seen, s, HIDDEN)
                old = top_s[h : h + 1, :]
                top = jnp.maximum(old, s.max(axis=0, keepdims=True))
                top_s[h : h + 1, :] = top
                weights.append(jnp.exp2((s - top) * e).astype(BF16))
                keeps.append(jnp.exp2((old - top) * e))
            for h in range(heads):
                mix_s[h] = mix_s[h] * keeps[h] + _dot(v_s[h // group, :, keys], weights[h])

        lax.fori_loop(0, tb, lambda j, _: block(j, False), None)
        block(tb, True)
        for h in range(heads):
            out = mix_s[h, :HEAD, :] * (1 / mix_s[h, HEAD : HEAD + 1, :])
            q_s[here, h * HEAD : (h + 1) * HEAD] = out.T.astype(BF16)

    def columns(side, t):
        return pl.ds(pl.multiple_of(side * half + t * TILE, TILE), TILE)

    def part(tb, side, t):
        return _dot(q_s[rows(tb), :], wo_s[:, columns(side, t)])

    def at_tile(t):
        return pl.ds(pl.multiple_of(t * TILE, TILE), TILE)

    def to_peer(b, t):
        return remote(peer_out.at[b, :, at_tile(t)], peer_in.at[b, :, at_tile(t)], half_ss.at[b * tiles + t], half_rs.at[b * tiles + t], peer)

    def to_far(b, t):
        return remote(peer_in.at[b, :, at_tile(t)], far_in.at[:, columns(c, t)], far_ss.at[b * tiles + t], far_rs.at[c * tiles + t], 2 * (1 - p) + b)

    def to_owner(side, t):
        return remote(peer_out.at[side, :, at_tile(t)], term_in.at[:, columns(side, t)], term_ss.at[side * tiles + t], term_rs.at[side * tiles + t], peer)

    def far(tb, b):
        def give(t, _):
            peer_out[b, :, at_tile(t)] = part(tb, 1 - c, t).astype(BF16)
            to_peer(b, t).start()

        def add(t, _):
            term = part(tb, c, t)
            to_peer(b, t).wait_recv()
            peer_in[b, :, at_tile(t)] = (term + peer_in[b, :, at_tile(t)].astype(F32)).astype(BF16)
            to_far(b, t).start()

        lax.fori_loop(0, tiles, give, None)
        lax.fori_loop(0, tiles, add, None)

    def near(tb):
        def give(i, _):
            side, t = lax.div(i, tiles), lax.rem(i, tiles)
            to_peer(side, t).wait_send()
            peer_out[side, :, at_tile(t)] = part(tb, side, t).astype(BF16)
            to_owner(side, t).start()

        lax.fori_loop(0, 2 * tiles, give, None)

    def mine(tb):
        def keep(i, _):
            side, t = lax.div(i, tiles), lax.rem(i, tiles)
            acc_s[:, columns(side, t)] = xs[rows(tb), columns(side, t)].astype(F32) + part(tb, side, t)

        lax.fori_loop(0, 2 * tiles, keep, None)

    def step(it, _):
        b = it - 2
        away = (it >= 2) & (it < 4)
        tb = jnp.where(it < 4, lax.rem(2 * p + it, 4), 2 * p + lax.rem(it + 1 + c, 2))

        @pl.when(away)
        def _():
            for h in range(2):
                across(b, h).wait_recv()
                passed(b, h).start()
            for h in range(2):
                passed(b, h).wait_recv()

        @pl.when(it < 4)
        def _():
            norm(tb)

            @pl.when(it == 0)
            def _():
                for copy in loads[3:6]:
                    copy.wait()

            project(tb)

        @pl.when(it == 2)
        def _():
            loads[6].wait()

        @pl.when(it >= 2)
        def _():
            attend(tb)

        @pl.when(away)
        def _():
            far(tb, b)

        @pl.when(it == 4)
        def _():
            near(tb)

        @pl.when(it == 5)
        def _():
            mine(tb)

    lax.fori_loop(0, 6, step, None)

    def finish(i, _):
        side, t = lax.rem(i, 2), lax.div(i, 2)
        here = columns(side, t)
        to_owner(side, t).wait_recv()
        remote(peer_in.at[0, :, at_tile(t)], far_in.at[:, here], far_ss.at[t], far_rs.at[side * tiles + t], cross).wait_recv()
        far_in[:, here] = (acc_s[:, here] + term_in[:, here].astype(F32) + far_in[:, here].astype(F32)).astype(BF16)

    lax.fori_loop(0, 2 * tiles, finish, None)
    for i in range(2):
        own(i).wait_send()
        for h in range(2):
            across(i, h).wait_send()
            passed(i, h).wait_send()
        for t in range(tiles):
            to_far(i, t).wait_send()
            to_owner(i, t).wait_send()


def _store(from_ref, y_ref, sem):
    copies = [pltpu.make_async_copy(from_ref.at[pl.ds(i * STORE, STORE)], y_ref.at[pl.ds(i * STORE, STORE)], sem.at[i]) for i in range(y_ref.shape[0] // STORE)]
    for copy in copies:
        copy.start()
    for copy in copies:
        copy.wait()


def _tables(tokens):
    half = HEAD // 2
    angle = np.arange(tokens)[:, None] * float(THETA) ** (-np.arange(half) / half)
    cos, sin = np.cos(angle), np.sin(angle)
    return np.concatenate([cos, cos], 1).astype(np.float32), np.concatenate([-sin, sin], 1).astype(np.float32)


def solution(mesh):
    def step(x, gain, wq, wk, wv, wo):
        n, d = x.shape
        tokens = 4 * n
        nq, nk = wq.shape[1], wk.shape[1]
        tiles = d // 2 // TILE
        cos, sin = _tables(tokens)
        vmem, dma = pltpu.VMEM, pltpu.SemaphoreType.DMA
        y = pl.pallas_call(
            _layer,
            out_shape=pltpu.VMEM((n, d), BF16),
            in_specs=[pl.BlockSpec(memory_space=pltpu.HBM)] * 8,
            out_specs=pl.BlockSpec(memory_space=pltpu.VMEM),
            scratch_shapes=[
                vmem((tokens, d), BF16), vmem((n, d), BF16), vmem((d,), BF16), vmem((1, d), F32), vmem((tokens, HEAD), F32), vmem((tokens, HEAD), F32),
                vmem(wq.shape, BF16), vmem(wk.shape, BF16), vmem(wv.shape, BF16), vmem(wo.shape, BF16),
                vmem((tokens, nq), BF16), vmem((tokens, nk), BF16), vmem((nk // HEAD, HEAD + 16, tokens), BF16),
                vmem((nq // HEAD, n), F32), vmem((nq // HEAD, HEAD + 16, n), F32),
                vmem((2, n, d // 2), BF16), vmem((2, n, d // 2), BF16), vmem((n, d), BF16), vmem((n, d), F32),
                dma((12,)), dma((2,)), dma((2,)), dma((4,)), dma((4,)), dma((4,)), dma((4,)),
                *[dma((2 * tiles,))] * 6,
            ],
            compiler_params=pltpu.CompilerParams(collective_id=0, has_side_effects=True, vmem_limit_bytes=VMEM),
        )(x, gain, cos, sin, wq, wk, wv, wo)
        return pl.pallas_call(
            _store,
            out_shape=jax.ShapeDtypeStruct((n, d), BF16),
            in_specs=[pl.BlockSpec(memory_space=pltpu.VMEM)],
            out_specs=pl.BlockSpec(memory_space=pltpu.HBM),
            scratch_shapes=[dma((n // STORE,))],
            compiler_params=pltpu.CompilerParams(vmem_limit_bytes=2**20),
        )(pltpu.with_memory_space_constraint(y, pltpu.VMEM))

    tokens, columns = P(("dp", "tp"), None), P(None, "tp")
    return jax.shard_map(
        step,
        mesh=mesh,
        in_specs=(tokens, P(None), columns, columns, columns, P("tp", None)),
        out_specs=tokens,
        check_vma=False,
    )
```

```python
import functools

import jax
import jax.numpy as jnp
import numpy as np
from jax import lax
from jax.experimental import pallas as pl
from jax.experimental.pallas import tpu as pltpu
from jax.sharding import PartitionSpec as P

HEAD = 128
THETA = 10000
NEG = -1e30
HIDDEN = 2 * NEG
LOG2E = 1.4426950408889634
VMEM = 67043328 - 2560 * 1024
MESH = pl.DeviceIdType.MESH
F32, BF16 = jnp.float32, jnp.bfloat16

B = 256
PIECES = ((0, 16), (16, 112))
TILE = 768


def _dot(a, b, ca=1, cb=0):
    return lax.dot_general(a, b, (((ca,), (cb,)), ((), ())), preferred_element_type=F32)


def _layer(x_ref, gain_ref, cos_ref, sin_ref, wq_ref, wk_ref, wv_ref, wo_ref, far_in,
           xs, a_s, gain_s, wide_s, cos_s, sin_s, wq_s, wk_s, wv_s, wo_s, q_s, k_s, v_s, top_s, mix_s,
           peer_out, peer_in, term_in, acc_s,
           load_sem, own_ss, own_rs, x_ss, x_rs, pass_ss, pass_rs, half_ss, half_rs, far_ss, far_rs, term_ss, term_rs):
    d = x_ref.shape[1]
    half = d // 2
    tiles = half // TILE
    nq, nk = wq_s.shape[1], wk_s.shape[1]
    heads, group = nq // HEAD, nq // nk
    me = lax.axis_index("tp")
    p, c = lax.div(me, 2), lax.rem(me, 2)
    peer, cross, diag = 2 * p + 1 - c, 2 * (1 - p) + c, 2 * (1 - p) + 1 - c

    def rows(block, at=0, n=B):
        return pl.ds(pl.multiple_of(block * B + at, 16), n)

    def load(i, src, dst):
        return pltpu.make_async_copy(src, dst, load_sem.at[i])

    loads = [load(0, x_ref, xs.at[rows(me)]), load(1, gain_ref, gain_s), load(2, cos_ref, cos_s), load(3, sin_ref, sin_s),
             load(4, wk_ref, wk_s), load(5, wv_ref, wv_s), load(6, wq_ref, wq_s), load(7, wo_ref, wo_s)]
    def remote(src, dst, send, recv, to):
        return pltpu.make_async_remote_copy(src_ref=src, dst_ref=dst, send_sem=send, recv_sem=recv, device_id={"tp": to}, device_id_type=MESH)

    barrier = pltpu.get_barrier_semaphore()
    for other in (peer, cross, diag):
        pl.semaphore_signal(barrier, inc=1, device_id={"tp": other}, device_id_type=MESH)
    pl.semaphore_wait(barrier, 3)

    def own(i):
        at = (1 - c if i == 0 else c) * (B // 2)
        return remote(x_ref.at[pl.ds(pl.multiple_of(at, B // 2), B // 2)], xs.at[rows(me, at, B // 2)], own_ss.at[i], own_rs.at[i], peer)

    def across(b, h, fresh=False):
        at, n = c * (B // 2) + PIECES[h][0], PIECES[h][1]
        there = xs.at[rows(2 * p + b, at, n)]
        src = x_ref.at[pl.ds(pl.multiple_of(at, 16), n)] if fresh else there
        return remote(src, there, x_ss.at[b * 2 + h], x_rs.at[b * 2 + h], cross)

    def passed(b, h):
        here = xs.at[rows(2 * (1 - p) + b, c * (B // 2) + PIECES[h][0], PIECES[h][1])]
        return remote(here, here, pass_ss.at[b * 2 + h], pass_rs.at[b * 2 + h], peer)

    @pl.when(c == 0)
    def _():
        across(0, 0, True).start()
        across(0, 1, True).start()

    @pl.when(c == 1)
    def _():
        across(1, 0, True).start()

    for i in range(2):
        own(i).start()
    for copy in loads:
        copy.start()
    own(0).wait_recv()

    @pl.when(c == 0)
    def _():
        across(1, 0).start()
        across(1, 1).start()

    @pl.when(c == 1)
    def _():
        across(0, 0).start()
        across(0, 1).start()
        across(1, 1, True).start()

    own(1).wait_recv()
    for copy in loads[:4]:
        copy.wait()
    wide_s[...] = gain_s[...].astype(F32).reshape(wide_s.shape)
    for g in range(nk // HEAD):
        v_s[g, HEAD:, :] = jnp.ones((v_s.shape[1] - HEAD, v_s.shape[2]), BF16)

    def norm(tb):
        def some(i, _):
            at = pl.ds(pl.multiple_of(tb * B + i * 16, 16), 16)
            wide = xs[at, :].astype(F32)
            scale = lax.rsqrt(jnp.mean(wide * wide, -1, keepdims=True) + 1e-6)
            a_s[pl.ds(pl.multiple_of(i * 16, 16), 16), :] = (wide * scale * wide_s[...]).astype(BF16)

        lax.fori_loop(0, B // 16, some, None)

    def project(tb):
        here = rows(tb)
        cos, sin = cos_s[here, :], sin_s[here, :]

        def turned(t):
            t = t.astype(BF16).astype(F32)
            return (t * cos + pltpu.roll(t, HEAD // 2, 1) * sin).astype(BF16)

        k = _dot(a_s[...], wk_s[...])
        for n in range(0, nk, HEAD):
            k_s[here, n : n + HEAD] = turned(k[:, n : n + HEAD])
        v = _dot(a_s[...], wv_s[...])
        for g in range(nk // HEAD):
            v_s[g, :HEAD, here] = v[:, g * HEAD : (g + 1) * HEAD].T.astype(BF16)

        def queries(i, _):
            at = pl.multiple_of(i * 512, 512)
            q = _dot(a_s[...], wq_s[:, pl.ds(at, 512)])
            for n in range(0, 512, HEAD):
                q_s[here, pl.ds(at + n, HEAD)] = turned(q[:, n : n + HEAD])

        lax.fori_loop(0, nq // 512, queries, None)

    def attend(tb):
        here = rows(tb)
        e = HEAD**-0.5 * LOG2E
        top_s[...] = jnp.full(top_s.shape, NEG, F32)
        mix_s[...] = jnp.zeros(mix_s.shape, F32)

        def block(j, masked):
            keys = rows(j)
            seen = None
            if masked:
                seen = lax.broadcasted_iota(jnp.int32, (B, B), 0) <= lax.broadcasted_iota(jnp.int32, (B, B), 1)
            scores = [_dot(k_s[keys, h // group * HEAD : (h // group + 1) * HEAD], q_s[here, h * HEAD : (h + 1) * HEAD], 1, 1) for h in range(heads)]
            weights, keeps = [], []
            for h, s in enumerate(scores):
                if masked:
                    s = jnp.where(seen, s, HIDDEN)
                old = top_s[h : h + 1, :]
                top = jnp.maximum(old, s.max(axis=0, keepdims=True))
                top_s[h : h + 1, :] = top
                weights.append(jnp.exp2((s - top) * e).astype(BF16))
                keeps.append(jnp.exp2((old - top) * e))
            for h in range(heads):
                mix_s[h] = mix_s[h] * keeps[h] + _dot(v_s[h // group, :, keys], weights[h])

        lax.fori_loop(0, tb, lambda j, _: block(j, False), None)
        block(tb, True)
        for h in range(heads):
            out = mix_s[h, :HEAD, :] * (1 / mix_s[h, HEAD : HEAD + 1, :])
            q_s[here, h * HEAD : (h + 1) * HEAD] = out.T.astype(BF16)

    def columns(side, t):
        return pl.ds(pl.multiple_of(side * half + t * TILE, TILE), TILE)

    def part(tb, side, t):
        return _dot(q_s[rows(tb), :], wo_s[:, columns(side, t)])

    def at_tile(t):
        return pl.ds(pl.multiple_of(t * TILE, TILE), TILE)

    def to_peer(b, t):
        return remote(peer_out.at[b, :, at_tile(t)], peer_in.at[b, :, at_tile(t)], half_ss.at[b * tiles + t], half_rs.at[b * tiles + t], peer)

    def to_far(b, t):
        return remote(peer_in.at[b, :, at_tile(t)], far_in.at[:, columns(c, t)], far_ss.at[b * tiles + t], far_rs.at[c * tiles + t], 2 * (1 - p) + b)

    def to_owner(side, t):
        return remote(peer_out.at[side, :, at_tile(t)], term_in.at[:, columns(side, t)], term_ss.at[side * tiles + t], term_rs.at[side * tiles + t], peer)

    def far(tb, b):
        def give(t, _):
            peer_out[b, :, at_tile(t)] = part(tb, 1 - c, t).astype(BF16)
            to_peer(b, t).start()

        def add(t, _):
            term = part(tb, c, t)
            to_peer(b, t).wait_recv()
            peer_in[b, :, at_tile(t)] = (term + peer_in[b, :, at_tile(t)].astype(F32)).astype(BF16)
            to_far(b, t).start()

        lax.fori_loop(0, tiles, give, None)
        lax.fori_loop(0, tiles, add, None)

    def near(tb):
        def give(i, _):
            side, t = lax.div(i, tiles), lax.rem(i, tiles)
            to_peer(side, t).wait_send()
            peer_out[side, :, at_tile(t)] = part(tb, side, t).astype(BF16)
            to_owner(side, t).start()

        lax.fori_loop(0, 2 * tiles, give, None)

    def mine(tb):
        def keep(i, _):
            side, t = lax.div(i, tiles), lax.rem(i, tiles)
            acc_s[:, columns(side, t)] = xs[rows(tb), columns(side, t)].astype(F32) + part(tb, side, t)

        lax.fori_loop(0, 2 * tiles, keep, None)

    def step(it, _):
        b = it - 2
        away = (it >= 2) & (it < 4)
        tb = jnp.where(it < 4, lax.rem(2 * p + it, 4), 2 * p + lax.rem(it + 1 + c, 2))

        @pl.when(away)
        def _():
            for h in range(2):
                across(b, h).wait_recv()
                passed(b, h).start()
            for h in range(2):
                passed(b, h).wait_recv()

        @pl.when(it < 4)
        def _():
            norm(tb)

            @pl.when(it == 0)
            def _():
                for copy in loads[4:7]:
                    copy.wait()

            project(tb)

        @pl.when(it == 2)
        def _():
            loads[7].wait()

        @pl.when(it >= 2)
        def _():
            attend(tb)

        @pl.when(away)
        def _():
            far(tb, b)

        @pl.when(it == 4)
        def _():
            near(tb)

        @pl.when(it == 5)
        def _():
            mine(tb)

    lax.fori_loop(0, 6, step, None)

    def finish(i, _):
        side, t = lax.rem(i, 2), lax.div(i, 2)
        here = columns(side, t)
        to_owner(side, t).wait_recv()
        remote(peer_in.at[0, :, at_tile(t)], far_in.at[:, here], far_ss.at[t], far_rs.at[side * tiles + t], cross).wait_recv()
        far_in[:, here] = (acc_s[:, here] + term_in[:, here].astype(F32) + far_in[:, here].astype(F32)).astype(BF16)

    lax.fori_loop(0, 2 * tiles, finish, None)
    for i in range(2):
        own(i).wait_send()
        for h in range(2):
            across(i, h).wait_send()
            passed(i, h).wait_send()
        for t in range(tiles):
            to_far(i, t).wait_send()
            to_owner(i, t).wait_send()


def _tables(tokens):
    half = HEAD // 2
    angle = np.arange(tokens)[:, None] * float(THETA) ** (-np.arange(half) / half)
    cos, sin = np.cos(angle), np.sin(angle)
    return np.concatenate([cos, cos], 1).astype(np.float32), np.concatenate([-sin, sin], 1).astype(np.float32)


def solution(mesh):
    def step(x, gain, wq, wk, wv, wo):
        n, d = x.shape
        tokens = 4 * n
        nq, nk = wq.shape[1], wk.shape[1]
        tiles = d // 2 // TILE
        cos, sin = _tables(tokens)
        vmem, dma = pltpu.VMEM, pltpu.SemaphoreType.DMA
        return pl.pallas_call(
            _layer,
            out_shape=pltpu.VMEM((n, d), BF16),
            in_specs=[pl.BlockSpec(memory_space=pltpu.HBM)] * 8,
            out_specs=pl.BlockSpec(memory_space=pltpu.VMEM),
            scratch_shapes=[
                vmem((tokens, d), BF16), vmem((n, d), BF16), vmem((d,), BF16), vmem((1, d), F32), vmem((tokens, HEAD), F32), vmem((tokens, HEAD), F32),
                vmem(wq.shape, BF16), vmem(wk.shape, BF16), vmem(wv.shape, BF16), vmem(wo.shape, BF16),
                vmem((tokens, nq), BF16), vmem((tokens, nk), BF16), vmem((nk // HEAD, HEAD + 16, tokens), BF16),
                vmem((nq // HEAD, n), F32), vmem((nq // HEAD, HEAD + 16, n), F32),
                vmem((2, n, d // 2), BF16), vmem((2, n, d // 2), BF16), vmem((n, d), BF16), vmem((n, d), F32),
                dma((8,)), dma((2,)), dma((2,)), dma((4,)), dma((4,)), dma((4,)), dma((4,)),
                *[dma((2 * tiles,))] * 6,
            ],
            compiler_params=pltpu.CompilerParams(collective_id=0, has_side_effects=True, vmem_limit_bytes=VMEM),
        )(x, gain, cos, sin, wq, wk, wv, wo)

    tokens, columns = P(("dp", "tp"), None), P(None, "tp")
    return jax.shard_map(
        step,
        mesh=mesh,
        in_specs=(tokens, P(None), columns, columns, columns, P("tp", None)),
        out_specs=tokens,
        check_vma=False,
    )
```

```python
import functools

import jax
import jax.numpy as jnp
import numpy as np
from jax import lax
from jax.experimental import pallas as pl
from jax.experimental.pallas import tpu as pltpu
from jax.sharding import PartitionSpec as P

HEAD = 128
THETA = 10000
NEG = -1e30
HIDDEN = 2 * NEG
LOG2E = 1.4426950408889634
VMEM = 67043328 - 2560 * 1024
MESH = pl.DeviceIdType.MESH
F32, BF16 = jnp.float32, jnp.bfloat16

B = 256
PIECES = ((0, 16), (16, 112))
TILES = ((0, 1024), (1024, 1024), (2048, 512))


def _dot(a, b, ca=1, cb=0):
    return lax.dot_general(a, b, (((ca,), (cb,)), ((), ())), preferred_element_type=F32)


def _layer(x_ref, gain_ref, cos_ref, sin_ref, wq_ref, wk_ref, wv_ref, wo_ref, far_in,
           xs, a_s, gain_s, wide_s, cos_s, sin_s, wq_s, wk_s, wv_s, wo_s, q_s, k_s, v_s, top_s, mix_s,
           peer_out, peer_in, term_in, acc_s,
           load_sem, own_ss, own_rs, x_ss, x_rs, pass_ss, pass_rs, half_ss, half_rs, far_ss, far_rs, term_ss, term_rs, in_sem):
    nq, nk = wq_s.shape[1], wk_s.shape[1]
    heads, group = nq // HEAD, nq // nk
    me = lax.axis_index("tp")
    p, c = lax.div(me, 2), lax.rem(me, 2)
    peer, cross, diag = 2 * p + 1 - c, 2 * (1 - p) + c, 2 * (1 - p) + 1 - c

    def rows(block, at=0, n=B):
        return pl.ds(pl.multiple_of(block * B + at, 16), n)

    def load(i, src, dst):
        return pltpu.make_async_copy(src, dst, load_sem.at[i])

    loads = [load(0, x_ref, xs.at[rows(me)]), load(1, gain_ref, gain_s), load(2, cos_ref, cos_s), load(3, sin_ref, sin_s),
             load(4, wk_ref, wk_s), load(5, wv_ref, wv_s), load(6, wq_ref, wq_s), load(7, wo_ref, wo_s)]
    def remote(src, dst, send, recv, to):
        return pltpu.make_async_remote_copy(src_ref=src, dst_ref=dst, send_sem=send, recv_sem=recv, device_id={"tp": to}, device_id_type=MESH)

    barrier = pltpu.get_barrier_semaphore()
    for other in (cross, diag):
        pl.semaphore_signal(barrier, inc=1, device_id={"tp": other}, device_id_type=MESH)
    pl.semaphore_wait(barrier, 2)
    pl.semaphore_signal(in_sem, inc=1, device_id={"tp": cross}, device_id_type=MESH)

    def own(i):
        at = (1 - c if i == 0 else c) * (B // 2)
        return remote(x_ref.at[pl.ds(pl.multiple_of(at, B // 2), B // 2)], xs.at[rows(me, at, B // 2)], own_ss.at[i], own_rs.at[i], peer)

    def across(b, h, fresh=False):
        at, n = c * (B // 2) + PIECES[h][0], PIECES[h][1]
        there = xs.at[rows(2 * p + b, at, n)]
        src = x_ref.at[pl.ds(pl.multiple_of(at, 16), n)] if fresh else there
        return remote(src, there, x_ss.at[b * 2 + h], x_rs.at[b * 2 + h], cross)

    def passed(b, h):
        here = xs.at[rows(2 * (1 - p) + b, c * (B // 2) + PIECES[h][0], PIECES[h][1])]
        return remote(here, here, pass_ss.at[b * 2 + h], pass_rs.at[b * 2 + h], peer)

    @pl.when(c == 0)
    def _():
        across(0, 0, True).start()
        across(0, 1, True).start()

    @pl.when(c == 1)
    def _():
        across(1, 0, True).start()

    pl.semaphore_wait(in_sem, 1)
    for i in range(2):
        own(i).start()
    for copy in loads:
        copy.start()
    own(0).wait_recv()

    @pl.when(c == 0)
    def _():
        across(1, 0).start()
        across(1, 1).start()

    @pl.when(c == 1)
    def _():
        across(0, 0).start()
        across(0, 1).start()
        across(1, 1, True).start()

    own(1).wait_recv()
    for copy in loads[:4]:
        copy.wait()
    wide_s[...] = gain_s[...].astype(F32).reshape(wide_s.shape)
    for g in range(nk // HEAD):
        v_s[g, HEAD:, :] = jnp.ones((v_s.shape[1] - HEAD, v_s.shape[2]), BF16)

    def norm(tb):
        def some(i, _):
            at = pl.ds(pl.multiple_of(tb * B + i * 16, 16), 16)
            wide = xs[at, :].astype(F32)
            scale = lax.rsqrt(jnp.mean(wide * wide, -1, keepdims=True) + 1e-6)
            a_s[pl.ds(pl.multiple_of(i * 16, 16), 16), :] = (wide * scale * wide_s[...]).astype(BF16)

        lax.fori_loop(0, B // 16, some, None)

    def project(tb):
        here = rows(tb)
        cos, sin = cos_s[here, :], sin_s[here, :]

        def turned(t):
            t = t.astype(BF16).astype(F32)
            return (t * cos + pltpu.roll(t, HEAD // 2, 1) * sin).astype(BF16)

        k = _dot(a_s[...], wk_s[...])
        for n in range(0, nk, HEAD):
            k_s[here, n : n + HEAD] = turned(k[:, n : n + HEAD])
        v = _dot(a_s[...], wv_s[...])
        for g in range(nk // HEAD):
            v_s[g, :HEAD, here] = v[:, g * HEAD : (g + 1) * HEAD].T.astype(BF16)

        def queries(i, _):
            at = pl.multiple_of(i * 512, 512)
            q = _dot(a_s[...], wq_s[:, pl.ds(at, 512)])
            for n in range(0, 512, HEAD):
                q_s[here, pl.ds(at + n, HEAD)] = turned(q[:, n : n + HEAD])

        lax.fori_loop(0, nq // 512, queries, None)

    def attend(tb):
        here = rows(tb)
        e = HEAD**-0.5 * LOG2E
        top_s[...] = jnp.full(top_s.shape, NEG, F32)
        mix_s[...] = jnp.zeros(mix_s.shape, F32)

        def block(j, masked):
            keys = rows(j)
            seen = None
            if masked:
                seen = lax.broadcasted_iota(jnp.int32, (B, B), 0) <= lax.broadcasted_iota(jnp.int32, (B, B), 1)
            scores = [_dot(k_s[keys, h // group * HEAD : (h // group + 1) * HEAD], q_s[here, h * HEAD : (h + 1) * HEAD], 1, 1) for h in range(heads)]
            weights, keeps = [], []
            for h, s in enumerate(scores):
                if masked:
                    s = jnp.where(seen, s, HIDDEN)
                old = top_s[h : h + 1, :]
                top = jnp.maximum(old, s.max(axis=0, keepdims=True))
                top_s[h : h + 1, :] = top
                weights.append(jnp.exp2((s - top) * e).astype(BF16))
                keeps.append(jnp.exp2((old - top) * e))
            for h in range(heads):
                mix_s[h] = mix_s[h] * keeps[h] + _dot(v_s[h // group, :, keys], weights[h])

        lax.fori_loop(0, tb, lambda j, _: block(j, False), None)
        block(tb, True)
        for h in range(heads):
            out = mix_s[h, :HEAD, :] * (1 / mix_s[h, HEAD : HEAD + 1, :])
            q_s[here, h * HEAD : (h + 1) * HEAD] = out.T.astype(BF16)

    def columns(side, t):
        return pl.ds(pl.multiple_of(side * TILES[2][0] + TILES[t][0], TILES[2][1]), TILES[t][1])

    def part(tb, side, t):
        return _dot(q_s[rows(tb), :], wo_s[:, columns(side, t)])

    def at_tile(t):
        return pl.ds(*TILES[t])

    def to_peer(b, t):
        return remote(peer_out.at[b, :, at_tile(t)], peer_in.at[b, :, at_tile(t)], half_ss.at[b * 3 + t], half_rs.at[b * 3 + t], peer)

    def to_far(b, t):
        side = 1 if t == 2 else c
        return remote(peer_in.at[b, :, at_tile(t)], far_in.at[:, columns(side, t)], far_ss.at[b * 3 + t], far_rs.at[side * 3 + t], 2 * (1 - p) + b)

    def to_owner(side, t):
        return remote(peer_out.at[side, :, at_tile(t)], term_in.at[:, columns(side, t)], term_ss.at[side * 3 + t], term_rs.at[side * 3 + t], peer)

    def far(tb, b):
        def give(t):
            peer_out[b, :, at_tile(t)] = part(tb, 1 if t == 2 else 1 - c, t).astype(BF16)
            to_peer(b, t).start()

        def add(t):
            term = part(tb, 1 if t == 2 else c, t)
            to_peer(b, t).wait_recv()
            peer_in[b, :, at_tile(t)] = (term + peer_in[b, :, at_tile(t)].astype(F32)).astype(BF16)
            to_far(b, t).start()

        for t in range(2):
            give(t)
        for t in range(2):
            add(t)

        @pl.when(c == 0)
        def _():
            give(2)

        @pl.when(c == 1)
        def _():
            add(2)

    def near(tb):
        def give(side, t):
            peer_out[side, :, at_tile(t)] = part(tb, side, t).astype(BF16)
            to_owner(side, t).start()

        def both(side, _):
            for t in range(2):
                to_peer(side, t).wait_send()
                give(side, t)

        lax.fori_loop(0, 2, both, None)

        @pl.when(c == 0)
        def _():
            to_peer(1, 2).wait_send()

        give(1, 2)

    def mine(tb):
        def keep(side, t):
            acc_s[:, columns(side, t)] = xs[rows(tb), columns(side, t)].astype(F32) + part(tb, side, t)

        def both(side, _):
            for t in range(2):
                keep(side, t)

        lax.fori_loop(0, 2, both, None)
        keep(1, 2)

    def step(it, _):
        b = it - 2
        away = (it >= 2) & (it < 4)
        tb = jnp.where(it < 4, lax.rem(2 * p + it, 4), 2 * p + lax.rem(it + 1 + c, 2))

        @pl.when(away)
        def _():
            for h in range(2):
                across(b, h).wait_recv()
                passed(b, h).start()
            for h in range(2):
                passed(b, h).wait_recv()

        @pl.when(it < 4)
        def _():
            norm(tb)

            @pl.when(it == 0)
            def _():
                for copy in loads[4:7]:
                    copy.wait()

            project(tb)

        @pl.when(it == 2)
        def _():
            loads[7].wait()

        @pl.when(it >= 2)
        def _():
            attend(tb)

        @pl.when(away)
        def _():
            far(tb, b)

        @pl.when(it == 4)
        def _():
            near(tb)

        @pl.when(it == 5)
        def _():
            mine(tb)

    lax.fori_loop(0, 6, step, None)

    def finish(side, t):
        here = columns(side, t)
        to_owner(side, t).wait_recv()
        remote(peer_in.at[0, :, at_tile(t)], far_in.at[:, here], far_ss.at[t], far_rs.at[side * 3 + t], cross).wait_recv()
        far_in[:, here] = (acc_s[:, here] + term_in[:, here].astype(F32) + far_in[:, here].astype(F32)).astype(BF16)

    for t in range(2):
        lax.fori_loop(0, 2, lambda side, _: finish(side, t), None)
    finish(1, 2)

    for i in range(2):
        own(i).wait_send()
        for h in range(2):
            across(i, h).wait_send()
            passed(i, h).wait_send()
            to_far(i, h).wait_send()
            to_owner(i, h).wait_send()
    to_owner(1, 2).wait_send()

    @pl.when(c == 0)
    def _():
        to_peer(0, 2).wait_send()

    @pl.when(c == 1)
    def _():
        for b in range(2):
            to_far(b, 2).wait_send()


def _tables(tokens):
    half = HEAD // 2
    angle = np.arange(tokens)[:, None] * float(THETA) ** (-np.arange(half) / half)
    cos, sin = np.cos(angle), np.sin(angle)
    return np.concatenate([cos, cos], 1).astype(np.float32), np.concatenate([-sin, sin], 1).astype(np.float32)


def solution(mesh):
    def step(x, gain, wq, wk, wv, wo):
        n, d = x.shape
        tokens = 4 * n
        nq, nk = wq.shape[1], wk.shape[1]
        side = TILES[2][0] + TILES[2][1]
        cos, sin = _tables(tokens)
        vmem, dma = pltpu.VMEM, pltpu.SemaphoreType.DMA
        return pl.pallas_call(
            _layer,
            out_shape=pltpu.VMEM((n, d), BF16),
            in_specs=[pl.BlockSpec(memory_space=pltpu.HBM)] * 8,
            out_specs=pl.BlockSpec(memory_space=pltpu.VMEM),
            scratch_shapes=[
                vmem((tokens, d), BF16), vmem((n, d), BF16), vmem((d,), BF16), vmem((1, d), F32), vmem((tokens, HEAD), F32), vmem((tokens, HEAD), F32),
                vmem(wq.shape, BF16), vmem(wk.shape, BF16), vmem(wv.shape, BF16), vmem(wo.shape, BF16),
                vmem((tokens, nq), BF16), vmem((tokens, nk), BF16), vmem((nk // HEAD, HEAD + 16, tokens), BF16),
                vmem((nq // HEAD, n), F32), vmem((nq // HEAD, HEAD + 16, n), F32),
                vmem((2, n, side), BF16), vmem((2, n, side), BF16), vmem((n, d), BF16), vmem((n, d), F32),
                dma((8,)), dma((2,)), dma((2,)), dma((4,)), dma((4,)), dma((4,)), dma((4,)),
                *[dma((6,))] * 6, pltpu.SemaphoreType.REGULAR,
            ],
            compiler_params=pltpu.CompilerParams(collective_id=0, has_side_effects=True, vmem_limit_bytes=VMEM),
        )(x, gain, cos, sin, wq, wk, wv, wo)

    tokens, columns = P(("dp", "tp"), None), P(None, "tp")
    return jax.shard_map(
        step,
        mesh=mesh,
        in_specs=(tokens, P(None), columns, columns, columns, P("tp", None)),
        out_specs=tokens,
        check_vma=False,
    )
```

```python
import functools

import jax
import jax.numpy as jnp
import numpy as np
from jax import lax
from jax.experimental import pallas as pl
from jax.experimental.pallas import tpu as pltpu
from jax.sharding import PartitionSpec as P

HEAD = 128
THETA = 10000
HIDDEN = -float("inf")
LOG2E = 1.4426950408889634
VMEM = 67043328 - 2560 * 1024
MESH = pl.DeviceIdType.MESH
F32, BF16 = jnp.float32, jnp.bfloat16

B = 256
PIECES = ((0, 16), (16, 112))
TILES = ((0, 1024), (1024, 1024), (2048, 512))


def _dot(a, b, ca=1, cb=0):
    return lax.dot_general(a, b, (((ca,), (cb,)), ((), ())), preferred_element_type=F32)


def _layer(x_ref, gain_ref, cos_ref, sin_ref, wq_ref, wk_ref, wv_ref, wo_ref, far_in,
           xs, a_s, gain_s, wide_s, cos_s, sin_s, wq_s, wk_s, wv_s, wo_s, q_s, k_s, v_s, top_s, mix_s,
           peer_out, peer_in, term_in, acc_s,
           load_sem, own_ss, own_rs, x_ss, x_rs, pass_ss, pass_rs, half_ss, half_rs, far_ss, far_rs, term_ss, term_rs, in_sem):
    nq, nk = wq_s.shape[1], wk_s.shape[1]
    heads, group = nq // HEAD, nq // nk
    me = lax.axis_index("tp")
    p, c = lax.div(me, 2), lax.rem(me, 2)
    peer, cross, diag = 2 * p + 1 - c, 2 * (1 - p) + c, 2 * (1 - p) + 1 - c

    def rows(block, at=0, n=B):
        return pl.ds(pl.multiple_of(block * B + at, 16), n)

    def load(i, src, dst):
        return pltpu.make_async_copy(src, dst, load_sem.at[i])

    loads = [load(0, x_ref, xs.at[rows(me)]), load(1, gain_ref, gain_s), load(2, cos_ref, cos_s), load(3, sin_ref, sin_s),
             load(4, wk_ref, wk_s), load(5, wv_ref, wv_s), load(6, wq_ref, wq_s), load(7, wo_ref, wo_s)]
    def remote(src, dst, send, recv, to):
        return pltpu.make_async_remote_copy(src_ref=src, dst_ref=dst, send_sem=send, recv_sem=recv, device_id={"tp": to}, device_id_type=MESH)

    barrier = pltpu.get_barrier_semaphore()
    for other in (cross, diag):
        pl.semaphore_signal(barrier, inc=1, device_id={"tp": other}, device_id_type=MESH)
    pl.semaphore_wait(barrier, 2)
    pl.semaphore_signal(in_sem, inc=1, device_id={"tp": cross}, device_id_type=MESH)

    def own(i):
        at = (1 - c if i == 0 else c) * (B // 2)
        return remote(x_ref.at[pl.ds(pl.multiple_of(at, B // 2), B // 2)], xs.at[rows(me, at, B // 2)], own_ss.at[i], own_rs.at[i], peer)

    def across(b, h, fresh=False):
        at, n = c * (B // 2) + PIECES[h][0], PIECES[h][1]
        there = xs.at[rows(2 * p + b, at, n)]
        src = x_ref.at[pl.ds(pl.multiple_of(at, 16), n)] if fresh else there
        return remote(src, there, x_ss.at[b * 2 + h], x_rs.at[b * 2 + h], cross)

    def passed(b, h):
        here = xs.at[rows(2 * (1 - p) + b, c * (B // 2) + PIECES[h][0], PIECES[h][1])]
        return remote(here, here, pass_ss.at[b * 2 + h], pass_rs.at[b * 2 + h], peer)

    @pl.when(c == 0)
    def _():
        across(0, 0, True).start()
        across(0, 1, True).start()

    @pl.when(c == 1)
    def _():
        across(1, 0, True).start()

    pl.semaphore_wait(in_sem, 1)
    for i in range(2):
        own(i).start()
    for copy in loads:
        copy.start()
    own(0).wait_recv()

    @pl.when(c == 0)
    def _():
        across(1, 0).start()
        across(1, 1).start()

    @pl.when(c == 1)
    def _():
        across(0, 0).start()
        across(0, 1).start()
        across(1, 1, True).start()

    own(1).wait_recv()
    for copy in loads[:4]:
        copy.wait()
    wide_s[...] = gain_s[...].astype(F32).reshape(wide_s.shape)
    for g in range(nk // HEAD):
        v_s[g, HEAD:, :] = jnp.ones((v_s.shape[1] - HEAD, v_s.shape[2]), BF16)

    def norm(tb):
        def some(i, _):
            at = pl.ds(pl.multiple_of(tb * B + i * 16, 16), 16)
            wide = xs[at, :].astype(F32)
            scale = lax.rsqrt(jnp.mean(wide * wide, -1, keepdims=True) + 1e-6)
            a_s[pl.ds(pl.multiple_of(i * 16, 16), 16), :] = (wide * scale * wide_s[...]).astype(BF16)

        lax.fori_loop(0, B // 16, some, None)

    def project(tb):
        here = rows(tb)
        cos, sin = cos_s[here, :], sin_s[here, :]

        def turned(t):
            t = t.astype(BF16).astype(F32)
            return (t * cos + pltpu.roll(t, HEAD // 2, 1) * sin).astype(BF16)

        k = _dot(a_s[...], wk_s[...])
        for n in range(0, nk, HEAD):
            k_s[here, n : n + HEAD] = turned(k[:, n : n + HEAD])
        v = _dot(a_s[...], wv_s[...])
        for g in range(nk // HEAD):
            v_s[g, :HEAD, here] = v[:, g * HEAD : (g + 1) * HEAD].T.astype(BF16)

        def queries(i, _):
            at = pl.multiple_of(i * 512, 512)
            q = _dot(a_s[...], wq_s[:, pl.ds(at, 512)])
            for n in range(0, 512, HEAD):
                q_s[here, pl.ds(at + n, HEAD)] = turned(q[:, n : n + HEAD])

        lax.fori_loop(0, nq // 512, queries, None)

    def attend(tb):
        here = rows(tb)
        e = HEAD**-0.5 * LOG2E
        top_s[...] = jnp.full(top_s.shape, HIDDEN, F32)
        mix_s[...] = jnp.zeros(mix_s.shape, F32)

        def block(j, masked):
            keys = rows(j)
            seen = None
            if masked:
                seen = lax.broadcasted_iota(jnp.int32, (B, B), 0) <= lax.broadcasted_iota(jnp.int32, (B, B), 1)
            scores = [_dot(k_s[keys, h // group * HEAD : (h // group + 1) * HEAD], q_s[here, h * HEAD : (h + 1) * HEAD], 1, 1) for h in range(heads)]
            weights, keeps = [], []
            for h, s in enumerate(scores):
                if masked:
                    s = jnp.where(seen, s, HIDDEN)
                old = top_s[h : h + 1, :]
                top = jnp.maximum(old, s.max(axis=0, keepdims=True))
                top_s[h : h + 1, :] = top
                weights.append(jnp.exp2((s - top) * e).astype(BF16))
                keeps.append(jnp.exp2((old - top) * e))
            for h in range(heads):
                mix_s[h] = mix_s[h] * keeps[h] + _dot(v_s[h // group, :, keys], weights[h])

        lax.fori_loop(0, tb, lambda j, _: block(j, False), None)
        block(tb, True)
        for h in range(heads):
            out = mix_s[h, :HEAD, :] * (1 / mix_s[h, HEAD : HEAD + 1, :])
            q_s[here, h * HEAD : (h + 1) * HEAD] = out.T.astype(BF16)

    def columns(side, t):
        return pl.ds(pl.multiple_of(side * TILES[2][0] + TILES[t][0], TILES[2][1]), TILES[t][1])

    def part(tb, side, t):
        return _dot(q_s[rows(tb), :], wo_s[:, columns(side, t)])

    def at_tile(t):
        return pl.ds(*TILES[t])

    def to_peer(b, t):
        return remote(peer_out.at[b, :, at_tile(t)], peer_in.at[b, :, at_tile(t)], half_ss.at[b * 3 + t], half_rs.at[b * 3 + t], peer)

    def to_far(b, t):
        side = 1 if t == 2 else c
        return remote(peer_in.at[b, :, at_tile(t)], far_in.at[:, columns(side, t)], far_ss.at[b * 3 + t], far_rs.at[side * 3 + t], 2 * (1 - p) + b)

    def to_owner(side, t):
        return remote(peer_out.at[side, :, at_tile(t)], term_in.at[:, columns(side, t)], term_ss.at[side * 3 + t], term_rs.at[side * 3 + t], peer)

    def far(tb, b):
        def give(t):
            peer_out[b, :, at_tile(t)] = part(tb, 1 if t == 2 else 1 - c, t).astype(BF16)
            to_peer(b, t).start()

        def add(t):
            term = part(tb, 1 if t == 2 else c, t)
            to_peer(b, t).wait_recv()
            peer_in[b, :, at_tile(t)] = (term + peer_in[b, :, at_tile(t)].astype(F32)).astype(BF16)
            to_far(b, t).start()

        for t in range(2):
            give(t)
        for t in range(2):
            add(t)

        @pl.when(c == 0)
        def _():
            give(2)

        @pl.when(c == 1)
        def _():
            add(2)

    def near(tb):
        def give(side, t):
            peer_out[side, :, at_tile(t)] = part(tb, side, t).astype(BF16)
            to_owner(side, t).start()

        def both(side, _):
            for t in range(2):
                to_peer(side, t).wait_send()
                give(side, t)

        lax.fori_loop(0, 2, both, None)

        @pl.when(c == 0)
        def _():
            to_peer(1, 2).wait_send()

        give(1, 2)

    def mine(tb):
        def keep(side, t):
            acc_s[:, columns(side, t)] = xs[rows(tb), columns(side, t)].astype(F32) + part(tb, side, t)

        def both(side, _):
            for t in range(2):
                keep(side, t)

        lax.fori_loop(0, 2, both, None)
        keep(1, 2)

    def step(it, _):
        b = it - 2
        away = (it >= 2) & (it < 4)
        tb = jnp.where(it < 4, lax.rem(2 * p + it, 4), 2 * p + lax.rem(it + 1 + c, 2))

        @pl.when(away)
        def _():
            for h in range(2):
                across(b, h).wait_recv()
                passed(b, h).start()
            for h in range(2):
                passed(b, h).wait_recv()

        @pl.when(it < 4)
        def _():
            norm(tb)

            @pl.when(it == 0)
            def _():
                for copy in loads[4:7]:
                    copy.wait()

            project(tb)

        @pl.when(it == 2)
        def _():
            loads[7].wait()

        @pl.when(it >= 2)
        def _():
            attend(tb)

        @pl.when(away)
        def _():
            far(tb, b)

        @pl.when(it == 4)
        def _():
            near(tb)

        @pl.when(it == 5)
        def _():
            mine(tb)

    lax.fori_loop(0, 6, step, None)

    def finish(side, t):
        here = columns(side, t)
        to_owner(side, t).wait_recv()
        remote(peer_in.at[0, :, at_tile(t)], far_in.at[:, here], far_ss.at[t], far_rs.at[side * 3 + t], cross).wait_recv()
        far_in[:, here] = (acc_s[:, here] + term_in[:, here].astype(F32) + far_in[:, here].astype(F32)).astype(BF16)

    for t in range(2):
        lax.fori_loop(0, 2, lambda side, _: finish(side, t), None)
    finish(1, 2)

    for i in range(2):
        own(i).wait_send()
        for h in range(2):
            across(i, h).wait_send()
            passed(i, h).wait_send()
            to_far(i, h).wait_send()
            to_owner(i, h).wait_send()
    to_owner(1, 2).wait_send()

    @pl.when(c == 0)
    def _():
        to_peer(0, 2).wait_send()

    @pl.when(c == 1)
    def _():
        for b in range(2):
            to_far(b, 2).wait_send()


def _tables(tokens):
    half = HEAD // 2
    angle = np.arange(tokens)[:, None] * float(THETA) ** (-np.arange(half) / half)
    cos, sin = np.cos(angle), np.sin(angle)
    return np.concatenate([cos, cos], 1).astype(np.float32), np.concatenate([-sin, sin], 1).astype(np.float32)


def solution(mesh):
    def step(x, gain, wq, wk, wv, wo):
        n, d = x.shape
        tokens = 4 * n
        nq, nk = wq.shape[1], wk.shape[1]
        side = TILES[2][0] + TILES[2][1]
        cos, sin = _tables(tokens)
        vmem, dma = pltpu.VMEM, pltpu.SemaphoreType.DMA
        return pl.pallas_call(
            _layer,
            out_shape=pltpu.VMEM((n, d), BF16),
            in_specs=[pl.BlockSpec(memory_space=pltpu.HBM)] * 8,
            out_specs=pl.BlockSpec(memory_space=pltpu.VMEM),
            scratch_shapes=[
                vmem((tokens, d), BF16), vmem((n, d), BF16), vmem((d,), BF16), vmem((1, d), F32), vmem((tokens, HEAD), F32), vmem((tokens, HEAD), F32),
                vmem(wq.shape, BF16), vmem(wk.shape, BF16), vmem(wv.shape, BF16), vmem(wo.shape, BF16),
                vmem((tokens, nq), BF16), vmem((tokens, nk), BF16), vmem((nk // HEAD, HEAD + 16, tokens), BF16),
                vmem((nq // HEAD, n), F32), vmem((nq // HEAD, HEAD + 16, n), F32),
                vmem((2, n, side), BF16), vmem((2, n, side), BF16), vmem((n, d), BF16), vmem((n, d), F32),
                dma((8,)), dma((2,)), dma((2,)), dma((4,)), dma((4,)), dma((4,)), dma((4,)),
                *[dma((6,))] * 6, pltpu.SemaphoreType.REGULAR,
            ],
            compiler_params=pltpu.CompilerParams(collective_id=0, has_side_effects=True, vmem_limit_bytes=VMEM),
        )(x, gain, cos, sin, wq, wk, wv, wo)

    tokens, columns = P(("dp", "tp"), None), P(None, "tp")
    return jax.shard_map(
        step,
        mesh=mesh,
        in_specs=(tokens, P(None), columns, columns, columns, P("tp", None)),
        out_specs=tokens,
        check_vma=False,
    )
```

```python
import functools

import jax
import jax.numpy as jnp
import numpy as np
from jax import lax
from jax.experimental import pallas as pl
from jax.experimental.pallas import tpu as pltpu
from jax.sharding import PartitionSpec as P

HEAD = 128
THETA = 10000
HIDDEN = -float("inf")
LOG2E = 1.4426950408889634
VMEM = 67043328 - 2560 * 1024
MESH = pl.DeviceIdType.MESH
F32, BF16 = jnp.float32, jnp.bfloat16

B = 256
PIECES = ((0, 16), (16, 112))
TILES = ((0, 1024), (1024, 1024), (2048, 512))


def _dot(a, b, ca=1, cb=0):
    return lax.dot_general(a, b, (((ca,), (cb,)), ((), ())), preferred_element_type=F32)


def _layer(x_ref, gain_ref, cos_ref, sin_ref, wq_ref, wk_ref, wv_ref, wo_ref, far_in,
           xs, a_s, gain_s, wide_s, cos_s, sin_s, wq_s, wk_s, wv_s, wo_s, q_s, k_s, v_s, top_s, mix_s,
           peer_out, peer_in, term_in, acc_s,
           load_sem, own_ss, own_rs, x_ss, x_rs, pass_ss, pass_rs, half_ss, half_rs, far_ss, far_rs, term_ss, term_rs, in_sem):
    nq, nk = wq_s.shape[1], wk_s.shape[1]
    heads, group = nq // HEAD, nq // nk
    me = lax.axis_index("tp")
    p, c = lax.div(me, 2), lax.rem(me, 2)
    peer, cross = 2 * p + 1 - c, 2 * (1 - p) + c

    def rows(block, at=0, n=B):
        return pl.ds(pl.multiple_of(block * B + at, 16), n)

    def load(i, src, dst):
        return pltpu.make_async_copy(src, dst, load_sem.at[i])

    loads = [load(0, x_ref, xs.at[rows(me)]), load(1, gain_ref, gain_s), load(2, cos_ref, cos_s), load(3, sin_ref, sin_s),
             load(4, wk_ref, wk_s), load(5, wv_ref, wv_s), load(6, wq_ref, wq_s), load(7, wo_ref, wo_s)]
    def remote(src, dst, send, recv, to):
        return pltpu.make_async_remote_copy(src_ref=src, dst_ref=dst, send_sem=send, recv_sem=recv, device_id={"tp": to}, device_id_type=MESH)

    barrier = pltpu.get_barrier_semaphore()
    pl.semaphore_signal(barrier, inc=1, device_id={"tp": cross}, device_id_type=MESH)

    @pl.when(p == 0)
    def _():
        pl.semaphore_signal(barrier, inc=1, device_id={"tp": peer}, device_id_type=MESH)

    pl.semaphore_wait(barrier, 2 - p)

    def own(i):
        at = (1 - c if i == 0 else c) * (B // 2)
        return remote(x_ref.at[pl.ds(pl.multiple_of(at, B // 2), B // 2)], xs.at[rows(me, at, B // 2)], own_ss.at[i], own_rs.at[i], peer)

    def across(b, h, fresh=False):
        at, n = c * (B // 2) + PIECES[h][0], PIECES[h][1]
        there = xs.at[rows(2 * p + b, at, n)]
        src = x_ref.at[pl.ds(pl.multiple_of(at, 16), n)] if fresh else there
        return remote(src, there, x_ss.at[b * 2 + h], x_rs.at[b * 2 + h], cross)

    def passed(b, h):
        here = xs.at[rows(2 * (1 - p) + b, c * (B // 2) + PIECES[h][0], PIECES[h][1])]
        return remote(here, here, pass_ss.at[b * 2 + h], pass_rs.at[b * 2 + h], peer)

    @pl.when(c == 0)
    def _():
        across(0, 0, True).start()
        across(0, 1, True).start()

    @pl.when(c == 1)
    def _():
        across(1, 0, True).start()

    @pl.when(p == 0)
    def _():
        pl.semaphore_signal(in_sem, inc=1, device_id={"tp": peer}, device_id_type=MESH)
        for i in range(2):
            own(i).start()

    pl.semaphore_wait(in_sem, 1)

    @pl.when(p == 0)
    def _():
        pl.semaphore_signal(in_sem, inc=1, device_id={"tp": cross}, device_id_type=MESH)

    @pl.when(p == 1)
    def _():
        for i in range(2):
            own(i).start()

    for copy in loads:
        copy.start()
    own(0).wait_recv()

    @pl.when(c == 0)
    def _():
        across(1, 0).start()
        across(1, 1).start()

    @pl.when(c == 1)
    def _():
        across(0, 0).start()
        across(0, 1).start()
        across(1, 1, True).start()

    own(1).wait_recv()
    for copy in loads[:4]:
        copy.wait()
    wide_s[...] = gain_s[...].astype(F32).reshape(wide_s.shape)
    for g in range(nk // HEAD):
        v_s[g, HEAD:, :] = jnp.ones((v_s.shape[1] - HEAD, v_s.shape[2]), BF16)

    def norm(tb):
        def some(i, _):
            at = pl.ds(pl.multiple_of(tb * B + i * 16, 16), 16)
            wide = xs[at, :].astype(F32)
            scale = lax.rsqrt(jnp.mean(wide * wide, -1, keepdims=True) + 1e-6)
            a_s[pl.ds(pl.multiple_of(i * 16, 16), 16), :] = (wide * scale * wide_s[...]).astype(BF16)

        lax.fori_loop(0, B // 16, some, None)

    def project(tb):
        here = rows(tb)
        cos, sin = cos_s[here, :], sin_s[here, :]

        def turned(t):
            t = t.astype(BF16).astype(F32)
            return (t * cos + pltpu.roll(t, HEAD // 2, 1) * sin).astype(BF16)

        k = _dot(a_s[...], wk_s[...])
        for n in range(0, nk, HEAD):
            k_s[here, n : n + HEAD] = turned(k[:, n : n + HEAD])
        v = _dot(a_s[...], wv_s[...])
        for g in range(nk // HEAD):
            v_s[g, :HEAD, here] = v[:, g * HEAD : (g + 1) * HEAD].T.astype(BF16)

        def queries(i, _):
            at = pl.multiple_of(i * 512, 512)
            q = _dot(a_s[...], wq_s[:, pl.ds(at, 512)])
            for n in range(0, 512, HEAD):
                q_s[here, pl.ds(at + n, HEAD)] = turned(q[:, n : n + HEAD])

        lax.fori_loop(0, nq // 512, queries, None)

    def attend(tb):
        here = rows(tb)
        e = HEAD**-0.5 * LOG2E
        top_s[...] = jnp.full(top_s.shape, HIDDEN, F32)
        mix_s[...] = jnp.zeros(mix_s.shape, F32)

        def block(j, masked):
            keys = rows(j)
            seen = None
            if masked:
                seen = lax.broadcasted_iota(jnp.int32, (B, B), 0) <= lax.broadcasted_iota(jnp.int32, (B, B), 1)
            scores = [_dot(k_s[keys, h // group * HEAD : (h // group + 1) * HEAD], q_s[here, h * HEAD : (h + 1) * HEAD], 1, 1) for h in range(heads)]
            weights, keeps = [], []
            for h, s in enumerate(scores):
                if masked:
                    s = jnp.where(seen, s, HIDDEN)
                old = top_s[h : h + 1, :]
                top = jnp.maximum(old, s.max(axis=0, keepdims=True))
                top_s[h : h + 1, :] = top
                weights.append(jnp.exp2((s - top) * e).astype(BF16))
                keeps.append(jnp.exp2((old - top) * e))
            for h in range(heads):
                mix_s[h] = mix_s[h] * keeps[h] + _dot(v_s[h // group, :, keys], weights[h])

        lax.fori_loop(0, tb, lambda j, _: block(j, False), None)
        block(tb, True)
        for h in range(heads):
            out = mix_s[h, :HEAD, :] * (1 / mix_s[h, HEAD : HEAD + 1, :])
            q_s[here, h * HEAD : (h + 1) * HEAD] = out.T.astype(BF16)

    def columns(side, t):
        return pl.ds(pl.multiple_of(side * TILES[2][0] + TILES[t][0], TILES[2][1]), TILES[t][1])

    def part(tb, side, t):
        return _dot(q_s[rows(tb), :], wo_s[:, columns(side, t)])

    def at_tile(t):
        return pl.ds(*TILES[t])

    def to_peer(b, t):
        return remote(peer_out.at[b, :, at_tile(t)], peer_in.at[b, :, at_tile(t)], half_ss.at[b * 3 + t], half_rs.at[b * 3 + t], peer)

    def to_far(b, t):
        side = 1 if t == 2 else c
        return remote(peer_in.at[b, :, at_tile(t)], far_in.at[:, columns(side, t)], far_ss.at[b * 3 + t], far_rs.at[side * 3 + t], 2 * (1 - p) + b)

    def to_owner(side, t):
        return remote(peer_out.at[side, :, at_tile(t)], term_in.at[:, columns(side, t)], term_ss.at[side * 3 + t], term_rs.at[side * 3 + t], peer)

    def far(tb, b):
        def give(t):
            peer_out[b, :, at_tile(t)] = part(tb, 1 if t == 2 else 1 - c, t).astype(BF16)
            to_peer(b, t).start()

        def add(t):
            term = part(tb, 1 if t == 2 else c, t)
            to_peer(b, t).wait_recv()
            peer_in[b, :, at_tile(t)] = (term + peer_in[b, :, at_tile(t)].astype(F32)).astype(BF16)
            to_far(b, t).start()

        for t in range(2):
            give(t)
        for t in range(2):
            add(t)

        @pl.when(c == 0)
        def _():
            give(2)

        @pl.when(c == 1)
        def _():
            add(2)

    def near(tb):
        def give(side, t):
            peer_out[side, :, at_tile(t)] = part(tb, side, t).astype(BF16)
            to_owner(side, t).start()

        def both(side, _):
            for t in range(2):
                to_peer(side, t).wait_send()
                give(side, t)

        lax.fori_loop(0, 2, both, None)

        @pl.when(c == 0)
        def _():
            to_peer(1, 2).wait_send()

        give(1, 2)

    def mine(tb):
        def keep(side, t):
            acc_s[:, columns(side, t)] = xs[rows(tb), columns(side, t)].astype(F32) + part(tb, side, t)

        def both(side, _):
            for t in range(2):
                keep(side, t)

        lax.fori_loop(0, 2, both, None)
        keep(1, 2)

    def step(it, _):
        b = it - 2
        away = (it >= 2) & (it < 4)
        tb = jnp.where(it < 4, lax.rem(2 * p + it, 4), 2 * p + lax.rem(it + 1 + c, 2))

        @pl.when(away)
        def _():
            for h in range(2):
                across(b, h).wait_recv()
                passed(b, h).start()
            for h in range(2):
                passed(b, h).wait_recv()

        @pl.when(it < 4)
        def _():
            norm(tb)

            @pl.when(it == 0)
            def _():
                for copy in loads[4:7]:
                    copy.wait()

            project(tb)

        @pl.when(it == 2)
        def _():
            loads[7].wait()

        @pl.when(it >= 2)
        def _():
            attend(tb)

        @pl.when(away)
        def _():
            far(tb, b)

        @pl.when(it == 4)
        def _():
            near(tb)

        @pl.when(it == 5)
        def _():
            mine(tb)

    lax.fori_loop(0, 6, step, None)

    def finish(side, t):
        here = columns(side, t)
        to_owner(side, t).wait_recv()
        remote(peer_in.at[0, :, at_tile(t)], far_in.at[:, here], far_ss.at[t], far_rs.at[side * 3 + t], cross).wait_recv()
        far_in[:, here] = (acc_s[:, here] + term_in[:, here].astype(F32) + far_in[:, here].astype(F32)).astype(BF16)

    for t in range(2):
        lax.fori_loop(0, 2, lambda side, _: finish(side, t), None)
    finish(1, 2)

    for i in range(2):
        own(i).wait_send()
        for h in range(2):
            across(i, h).wait_send()
            passed(i, h).wait_send()
            to_far(i, h).wait_send()
            to_owner(i, h).wait_send()
    to_owner(1, 2).wait_send()

    @pl.when(c == 0)
    def _():
        to_peer(0, 2).wait_send()

    @pl.when(c == 1)
    def _():
        for b in range(2):
            to_far(b, 2).wait_send()


def _tables(tokens):
    half = HEAD // 2
    angle = np.arange(tokens)[:, None] * float(THETA) ** (-np.arange(half) / half)
    cos, sin = np.cos(angle), np.sin(angle)
    return np.concatenate([cos, cos], 1).astype(np.float32), np.concatenate([-sin, sin], 1).astype(np.float32)


def solution(mesh):
    def step(x, gain, wq, wk, wv, wo):
        n, d = x.shape
        tokens = 4 * n
        nq, nk = wq.shape[1], wk.shape[1]
        side = TILES[2][0] + TILES[2][1]
        cos, sin = _tables(tokens)
        vmem, dma = pltpu.VMEM, pltpu.SemaphoreType.DMA
        return pl.pallas_call(
            _layer,
            out_shape=pltpu.VMEM((n, d), BF16),
            in_specs=[pl.BlockSpec(memory_space=pltpu.HBM)] * 8,
            out_specs=pl.BlockSpec(memory_space=pltpu.VMEM),
            scratch_shapes=[
                vmem((tokens, d), BF16), vmem((n, d), BF16), vmem((d,), BF16), vmem((1, d), F32), vmem((tokens, HEAD), F32), vmem((tokens, HEAD), F32),
                vmem(wq.shape, BF16), vmem(wk.shape, BF16), vmem(wv.shape, BF16), vmem(wo.shape, BF16),
                vmem((tokens, nq), BF16), vmem((tokens, nk), BF16), vmem((nk // HEAD, HEAD + 16, tokens), BF16),
                vmem((nq // HEAD, n), F32), vmem((nq // HEAD, HEAD + 16, n), F32),
                vmem((2, n, side), BF16), vmem((2, n, side), BF16), vmem((n, d), BF16), vmem((n, d), F32),
                dma((8,)), dma((2,)), dma((2,)), dma((4,)), dma((4,)), dma((4,)), dma((4,)),
                *[dma((6,))] * 6, pltpu.SemaphoreType.REGULAR,
            ],
            compiler_params=pltpu.CompilerParams(collective_id=0, has_side_effects=True, vmem_limit_bytes=VMEM),
        )(x, gain, cos, sin, wq, wk, wv, wo)

    tokens, columns = P(("dp", "tp"), None), P(None, "tp")
    return jax.shard_map(
        step,
        mesh=mesh,
        in_specs=(tokens, P(None), columns, columns, columns, P("tp", None)),
        out_specs=tokens,
        check_vma=False,
    )
```

```python
import functools

import jax
import jax.numpy as jnp
import numpy as np
from jax import lax
from jax.experimental import pallas as pl
from jax.experimental.pallas import tpu as pltpu
from jax.sharding import PartitionSpec as P

HEAD = 128
THETA = 10000
HIDDEN = -float("inf")
LOG2E = 1.4426950408889634
VMEM = 67043328 - 2560 * 1024
MESH = pl.DeviceIdType.MESH
F32, BF16 = jnp.float32, jnp.bfloat16

B = 256
PIECES = ((0, 0, 128), (1, 0, 16), (1, 16, 112))
TILES = ((0, 1024), (1024, 1024), (2048, 512), (0, 2048))
REST, MAIN = 2, 3


def _dot(a, b, ca=1, cb=0):
    return lax.dot_general(a, b, (((ca,), (cb,)), ((), ())), preferred_element_type=F32)


def _layer(x_ref, gain_ref, turn_ref, wq_ref, wk_ref, wv_ref, wo_ref, far_in,
           xs, a_s, gain_s, wide_s, turn_s, wq_s, wk_s, wv_s, wo_s, q_s, k_s, v_s, top_s, mix_s,
           peer_out, peer_in, term_in, acc_s,
           load_sem, near_ss, near_rs, x_ss, x_rs, half_ss, half_rs, far_ss, far_rs, in_sem):
    nq, nk = wq_s.shape[1], wk_s.shape[1]
    heads, group = nq // HEAD, nq // nk
    me = lax.axis_index("tp")
    p, c = lax.div(me, 2), lax.rem(me, 2)
    peer, cross = 2 * p + 1 - c, 2 * (1 - p) + c

    def rows(block, at=0, n=B):
        return pl.ds(pl.multiple_of(block * B + at, 16), n)

    def load(i, src, dst):
        return pltpu.make_async_copy(src, dst, load_sem.at[i])

    loads = [load(0, x_ref, xs.at[rows(me)]), load(1, gain_ref, gain_s), load(2, turn_ref, turn_s),
             load(3, wk_ref, wk_s), load(4, wv_ref, wv_s), load(5, wq_ref, wq_s)]
    load_wo = load(0, wo_ref, wo_s)
    def remote(src, dst, send, recv, to):
        return pltpu.make_async_remote_copy(src_ref=src, dst_ref=dst, send_sem=send, recv_sem=recv, device_id={"tp": to}, device_id_type=MESH)

    barrier = pltpu.get_barrier_semaphore()
    pl.semaphore_signal(barrier, inc=1, device_id={"tp": cross}, device_id_type=MESH)

    @pl.when(p == 0)
    def _():
        pl.semaphore_signal(barrier, inc=1, device_id={"tp": peer}, device_id_type=MESH)

    pl.semaphore_wait(barrier, 2 - p)

    def own(i):
        at = (1 - c if i == 0 else c) * (B // 2)
        return remote(x_ref.at[pl.ds(pl.multiple_of(at, B // 2), B // 2)], xs.at[rows(me, at, B // 2)], near_ss.at[i], near_rs.at[i], peer)

    def across(i, fresh=False):
        b, at, n = PIECES[i]
        at = c * (B // 2) + at
        there = xs.at[rows(2 * p + b, at, n)]
        src = x_ref.at[pl.ds(pl.multiple_of(at, 16), n)] if fresh else there
        return remote(src, there, x_ss.at[i], x_rs.at[i], cross)

    def passed(i):
        b, at, n = PIECES[i]
        here = xs.at[rows(2 * (1 - p) + b, c * (B // 2) + at, n)]
        return remote(here, here, near_ss.at[2 + i], near_rs.at[2 + i], peer)

    @pl.when(c == 0)
    def _():
        across(0, True).start()

    @pl.when(c == 1)
    def _():
        across(1, True).start()

    @pl.when(p == 0)
    def _():
        pl.semaphore_signal(in_sem, inc=1, device_id={"tp": peer}, device_id_type=MESH)
        for i in range(2):
            own(i).start()

    pl.semaphore_wait(in_sem, 1)

    @pl.when(p == 0)
    def _():
        pl.semaphore_signal(in_sem, inc=1, device_id={"tp": cross}, device_id_type=MESH)

    @pl.when(p == 1)
    def _():
        for i in range(2):
            own(i).start()

    for copy in loads:
        copy.start()
    own(0).wait_recv()

    @pl.when(c == 0)
    def _():
        across(1).start()
        across(2).start()

    @pl.when(c == 1)
    def _():
        across(0).start()
        across(2, True).start()

    own(1).wait_recv()
    for copy in loads[:3]:
        copy.wait()
    load_wo.start()
    wide_s[...] = gain_s[...].astype(F32).reshape(wide_s.shape)
    for g in range(nk // HEAD):
        v_s[g, HEAD:, :] = jnp.ones((v_s.shape[1] - HEAD, v_s.shape[2]), BF16)

    def norm(tb):
        def some(i, _):
            at = pl.ds(pl.multiple_of(tb * B + i * 16, 16), 16)
            wide = xs[at, :].astype(F32)
            scale = lax.rsqrt(jnp.mean(wide * wide, -1, keepdims=True) + 1e-6)
            a_s[pl.ds(pl.multiple_of(i * 16, 16), 16), :] = (wide * scale * wide_s[...]).astype(BF16)

        lax.fori_loop(0, B // 16, some, None)

    def project(tb):
        here = rows(tb)
        cos, sin = turn_s[here, :HEAD], turn_s[here, HEAD:]

        def turned(t):
            t = t.astype(BF16).astype(F32)
            return (t * cos + pltpu.roll(t, HEAD // 2, 1) * sin).astype(BF16)

        k = _dot(a_s[...], wk_s[...])
        for n in range(0, nk, HEAD):
            k_s[here, n : n + HEAD] = turned(k[:, n : n + HEAD])
        v = _dot(a_s[...], wv_s[...])
        for g in range(nk // HEAD):
            v_s[g, :HEAD, here] = v[:, g * HEAD : (g + 1) * HEAD].T.astype(BF16)

        def queries(i, _):
            at = pl.multiple_of(i * 512, 512)
            q = _dot(a_s[...], wq_s[:, pl.ds(at, 512)])
            for n in range(0, 512, HEAD):
                q_s[here, pl.ds(at + n, HEAD)] = turned(q[:, n : n + HEAD])

        lax.fori_loop(0, nq // 512, queries, None)

    def attend(tb):
        here = rows(tb)
        e = HEAD**-0.5 * LOG2E
        top_s[...] = jnp.full(top_s.shape, HIDDEN, F32)
        mix_s[...] = jnp.zeros(mix_s.shape, F32)

        def block(j, masked):
            keys = rows(j)
            seen = None
            if masked:
                seen = lax.broadcasted_iota(jnp.int32, (B, B), 0) <= lax.broadcasted_iota(jnp.int32, (B, B), 1)
            scores = [_dot(k_s[keys, h // group * HEAD : (h // group + 1) * HEAD], q_s[here, h * HEAD : (h + 1) * HEAD], 1, 1) for h in range(heads)]
            weights, keeps = [], []
            for h, s in enumerate(scores):
                if masked:
                    s = jnp.where(seen, s, HIDDEN)
                old = top_s[h : h + 1, :]
                top = jnp.maximum(old, s.max(axis=0, keepdims=True))
                top_s[h : h + 1, :] = top
                weights.append(jnp.exp2((s - top) * e).astype(BF16))
                keeps.append(jnp.exp2((old - top) * e))
            for h in range(heads):
                mix_s[h] = mix_s[h] * keeps[h] + _dot(v_s[h // group, :, keys], weights[h])

        lax.fori_loop(0, tb, lambda j, _: block(j, False), None)
        block(tb, True)
        for h in range(heads):
            out = mix_s[h, :HEAD, :] * (1 / mix_s[h, HEAD : HEAD + 1, :])
            q_s[here, h * HEAD : (h + 1) * HEAD] = out.T.astype(BF16)

    def columns(side, t):
        return pl.ds(pl.multiple_of(side * TILES[MAIN][1] + TILES[t][0], TILES[REST][1]), TILES[t][1])

    def part(tb, side, t):
        return _dot(q_s[rows(tb), :], wo_s[:, columns(side, t)])

    def at_tile(t):
        return pl.ds(*TILES[t])

    def to_peer(b, t):
        return remote(peer_out.at[b, :, at_tile(t)], peer_in.at[b, :, at_tile(t)], half_ss.at[t], half_rs.at[t], peer)

    def to_far(b, t):
        side = 1 if t == REST else c
        return remote(peer_in.at[b, :, at_tile(t)], far_in.at[:, columns(side, t)], far_ss.at[b * 2 + t - 2], far_rs.at[2 if t == REST else side], 2 * (1 - p) + b)

    def to_owner(side, t):
        i = 4 if t == REST else side * 2 + t
        return remote(peer_out.at[side, :, at_tile(t)], term_in.at[:, columns(side, t)], near_ss.at[i], near_rs.at[i], peer)

    def far(tb, b):
        def give(t):
            peer_out[b, :, at_tile(t)] = part(tb, 1 if t == REST else 1 - c, t).astype(BF16)

            @pl.when(b == 1)
            def _():
                to_peer(0, t).wait_send()

            to_peer(b, t).start()

        def add(t):
            term = part(tb, 1 if t == REST else c, t)
            to_peer(b, t).wait_recv()
            peer_in[b, :, at_tile(t)] = (term + peer_in[b, :, at_tile(t)].astype(F32)).astype(BF16)

        for t in range(2):
            give(t)
        for t in range(2):
            add(t)
        to_far(b, MAIN).start()

        @pl.when(c == 0)
        def _():
            give(REST)

        @pl.when(c == 1)
        def _():
            add(REST)
            to_far(b, REST).start()

    def near(tb):
        def give(side, t):
            peer_out[side, :, at_tile(t)] = part(tb, side, t).astype(BF16)
            to_owner(side, t).start()

        def both(side, _):
            for t in range(2):
                give(side, t)

        for t in range(2):
            to_peer(1, t).wait_send()
            own(t).wait_send()

        @pl.when(c == 0)
        def _():
            to_peer(1, REST).wait_send()

        for i in range(len(PIECES)):
            passed(i).wait_send()
        lax.fori_loop(0, 2, both, None)
        give(1, REST)

    def mine(tb):
        def keep(side, t):
            acc_s[:, columns(side, t)] = xs[rows(tb), columns(side, t)].astype(F32) + part(tb, side, t)

        def both(side, _):
            for t in range(2):
                keep(side, t)

        lax.fori_loop(0, 2, both, None)
        keep(1, REST)

    def step(it, _):
        b = it - 2
        away = (it >= 2) & (it < 4)
        tb = jnp.where(it < 4, lax.rem(2 * p + it, 4), 2 * p + lax.rem(it + 1 + c, 2))

        def arrive(pieces):
            for i in pieces:
                across(i).wait_recv()
                passed(i).start()
            for i in pieces:
                passed(i).wait_recv()

        @pl.when(it == 2)
        def _():
            arrive((0,))

        @pl.when(it == 3)
        def _():
            arrive((1, 2))

        @pl.when(it < 4)
        def _():
            norm(tb)

            @pl.when(it == 0)
            def _():
                for copy in loads[3:]:
                    copy.wait()

            project(tb)

        @pl.when(it == 2)
        def _():
            load_wo.wait()

        @pl.when(it >= 2)
        def _():
            attend(tb)

        @pl.when(away)
        def _():
            far(tb, b)

        @pl.when(it == 4)
        def _():
            near(tb)

        @pl.when(it == 5)
        def _():
            mine(tb)

    lax.fori_loop(0, 6, step, None)

    def finish(side, t):
        here = columns(side, t)
        to_owner(side, t).wait_recv()
        far_in[:, here] = (acc_s[:, here] + term_in[:, here].astype(F32) + far_in[:, here].astype(F32)).astype(BF16)

    def sums(side, t):
        here = columns(side, t)
        return remote(peer_in.at[0, :, at_tile(t)], far_in.at[:, here], far_ss.at[t - 2], far_rs.at[2 if t == REST else side], cross)

    def main(side, _):
        sums(side, MAIN).wait_recv()
        for t in range(2):
            finish(side, t)

    lax.fori_loop(0, 2, main, None)
    sums(1, REST).wait_recv()
    finish(1, REST)

    for i in range(2):
        to_far(i, MAIN).wait_send()
        for t in range(2):
            to_owner(i, t).wait_send()
    for i in range(len(PIECES)):
        across(i).wait_send()
    to_owner(1, REST).wait_send()

    @pl.when(c == 1)
    def _():
        for b in range(2):
            to_far(b, REST).wait_send()


def _table(tokens):
    half = HEAD // 2
    angle = np.arange(tokens)[:, None] * float(THETA) ** (-np.arange(half) / half)
    cos, sin = np.cos(angle), np.sin(angle)
    return np.concatenate([cos, cos, -sin, sin], 1).astype(np.float32)


def solution(mesh):
    def step(x, gain, wq, wk, wv, wo):
        n, d = x.shape
        tokens = 4 * n
        nq, nk = wq.shape[1], wk.shape[1]
        side = TILES[REST][0] + TILES[REST][1]
        vmem, dma = pltpu.VMEM, pltpu.SemaphoreType.DMA
        return pl.pallas_call(
            _layer,
            out_shape=pltpu.VMEM((n, d), BF16),
            in_specs=[pl.BlockSpec(memory_space=pltpu.HBM)] * 7,
            out_specs=pl.BlockSpec(memory_space=pltpu.VMEM),
            scratch_shapes=[
                vmem((tokens, d), BF16), vmem((n, d), BF16), vmem((d,), BF16), vmem((1, d), F32), vmem((tokens, 2 * HEAD), F32),
                vmem(wq.shape, BF16), vmem(wk.shape, BF16), vmem(wv.shape, BF16), vmem(wo.shape, BF16),
                vmem((tokens, nq), BF16), vmem((tokens, nk), BF16), vmem((nk // HEAD, HEAD + 16, tokens), BF16),
                vmem((nq // HEAD, n), F32), vmem((nq // HEAD, HEAD + 16, n), F32),
                vmem((2, n, side), BF16), vmem((2, n, side), BF16), vmem((n, d), BF16), vmem((n, d), F32),
                dma((6,)), dma((2 + len(PIECES),)), dma((2 + len(PIECES),)), dma((len(PIECES),)), dma((len(PIECES),)),
                dma((3,)), dma((3,)), dma((4,)), dma((3,)), pltpu.SemaphoreType.REGULAR,
            ],
            compiler_params=pltpu.CompilerParams(collective_id=0, has_side_effects=True, vmem_limit_bytes=VMEM),
        )(x, gain, _table(tokens), wq, wk, wv, wo)

    tokens, columns = P(("dp", "tp"), None), P(None, "tp")
    return jax.shard_map(
        step,
        mesh=mesh,
        in_specs=(tokens, P(None), columns, columns, columns, P("tp", None)),
        out_specs=tokens,
        check_vma=False,
    )
```

```python
import functools

import jax
import jax.numpy as jnp
import numpy as np
from jax import lax
from jax.experimental import pallas as pl
from jax.experimental.pallas import tpu as pltpu
from jax.sharding import PartitionSpec as P

HEAD = 128
THETA = 10000
HIDDEN = -float("inf")
LOG2E = 1.4426950408889634
VMEM = 67043328 - 2560 * 1024
MESH = pl.DeviceIdType.MESH
F32, BF16 = jnp.float32, jnp.bfloat16

B = 256
PIECES = ((0, 0, 128), (1, 0, 16), (1, 16, 112))
TILES = ((0, 1024), (1024, 1024), (2048, 512), (0, 2048))
REST, MAIN = 2, 3


def _dot(a, b, ca=1, cb=0):
    return lax.dot_general(a, b, (((ca,), (cb,)), ((), ())), preferred_element_type=F32)


def _layer(x_ref, gain_ref, turn_ref, wq_ref, wk_ref, wv_ref, wo_ref, far_in,
           xs, a_s, gain_s, wide_s, turn_s, wq_s, wk_s, wv_s, wo_s, q_s, k_s, v_s, top_s, mix_s,
           peer_out, peer_in, term_in, acc_s,
           first_ss, near_rs, x_rs, half_rs, far_rs, in_sem):
    nq, nk = wq_s.shape[1], wk_s.shape[1]
    heads, group = nq // HEAD, nq // nk
    me = lax.axis_index("tp")
    p, c = lax.div(me, 2), lax.rem(me, 2)
    peer, cross = 2 * p + 1 - c, 2 * (1 - p) + c

    def rows(block, at=0, n=B):
        return pl.ds(pl.multiple_of(block * B + at, 16), n)

    def remote(src, dst, send, recv, to):
        return pltpu.make_async_remote_copy(src_ref=src, dst_ref=dst, send_sem=send, recv_sem=recv, device_id={"tp": to}, device_id_type=MESH)

    barrier = pltpu.get_barrier_semaphore()
    pl.semaphore_signal(barrier, inc=1, device_id={"tp": cross}, device_id_type=MESH)

    @pl.when(p == 0)
    def _():
        pl.semaphore_signal(barrier, inc=1, device_id={"tp": peer}, device_id_type=MESH)

    pl.semaphore_wait(barrier, 2 - p)

    def across(i, sem, fresh=False):
        b, at, n = PIECES[i]
        at = c * (B // 2) + at
        there = xs.at[rows(2 * p + b, at, n)]
        src = x_ref.at[pl.ds(pl.multiple_of(at, 16), n)] if fresh else there
        return remote(src, there, sem, x_rs.at[i], cross)

    @pl.when(c == 0)
    def _():
        across(0, first_ss.at[0], True).start()

    @pl.when(c == 1)
    def _():
        across(1, first_ss.at[0], True).start()

    def rest(load_sem, near_ss, x_ss, half_ss, far_ss):
        def own(i):
            at = (1 - c if i == 0 else c) * (B // 2)
            return remote(x_ref.at[pl.ds(pl.multiple_of(at, B // 2), B // 2)], xs.at[rows(me, at, B // 2)], near_ss.at[i], near_rs.at[i], peer)

        def passed(i):
            b, at, n = PIECES[i]
            here = xs.at[rows(2 * (1 - p) + b, c * (B // 2) + at, n)]
            return remote(here, here, near_ss.at[2 + i], near_rs.at[2 + i], peer)

        def load(i, src, dst):
            return pltpu.make_async_copy(src, dst, load_sem.at[i])

        loads = [load(0, x_ref, xs.at[rows(me)]), load(1, gain_ref, gain_s), load(2, turn_ref, turn_s),
                 load(3, wk_ref, wk_s), load(4, wv_ref, wv_s), load(5, wq_ref, wq_s)]
        load_wo = load(0, wo_ref, wo_s)
        @pl.when(p == 0)
        def _():
            pl.semaphore_signal(in_sem, inc=1, device_id={"tp": peer}, device_id_type=MESH)
            for i in range(2):
                own(i).start()

        pl.semaphore_wait(in_sem, 1)

        @pl.when(p == 0)
        def _():
            pl.semaphore_signal(in_sem, inc=1, device_id={"tp": cross}, device_id_type=MESH)

        @pl.when(p == 1)
        def _():
            for i in range(2):
                own(i).start()

        for copy in loads:
            copy.start()
        own(0).wait_recv()

        @pl.when(c == 0)
        def _():
            across(1, x_ss.at[0]).start()
            across(2, x_ss.at[1]).start()

        @pl.when(c == 1)
        def _():
            across(0, x_ss.at[0]).start()
            across(2, x_ss.at[1], True).start()

        own(1).wait_recv()
        for copy in loads[:3]:
            copy.wait()
        load_wo.start()
        wide_s[...] = gain_s[...].astype(F32).reshape(wide_s.shape)
        for g in range(nk // HEAD):
            v_s[g, HEAD:, :] = jnp.ones((v_s.shape[1] - HEAD, v_s.shape[2]), BF16)

        def norm(tb):
            def some(i, _):
                at = pl.ds(pl.multiple_of(tb * B + i * 16, 16), 16)
                wide = xs[at, :].astype(F32)
                scale = lax.rsqrt(jnp.mean(wide * wide, -1, keepdims=True) + 1e-6)
                a_s[pl.ds(pl.multiple_of(i * 16, 16), 16), :] = (wide * scale * wide_s[...]).astype(BF16)

            lax.fori_loop(0, B // 16, some, None)

        def project(tb):
            here = rows(tb)
            cos, sin = turn_s[here, :HEAD], turn_s[here, HEAD:]

            def turned(t):
                t = t.astype(BF16).astype(F32)
                return (t * cos + pltpu.roll(t, HEAD // 2, 1) * sin).astype(BF16)

            k = _dot(a_s[...], wk_s[...])
            for n in range(0, nk, HEAD):
                k_s[here, n : n + HEAD] = turned(k[:, n : n + HEAD])
            v = _dot(a_s[...], wv_s[...])
            for g in range(nk // HEAD):
                v_s[g, :HEAD, here] = v[:, g * HEAD : (g + 1) * HEAD].T.astype(BF16)

            def queries(i, _):
                at = pl.multiple_of(i * 512, 512)
                q = _dot(a_s[...], wq_s[:, pl.ds(at, 512)])
                for n in range(0, 512, HEAD):
                    q_s[here, pl.ds(at + n, HEAD)] = turned(q[:, n : n + HEAD])

            lax.fori_loop(0, nq // 512, queries, None)

        def attend(tb):
            here = rows(tb)
            e = HEAD**-0.5 * LOG2E
            top_s[...] = jnp.full(top_s.shape, HIDDEN, F32)
            mix_s[...] = jnp.zeros(mix_s.shape, F32)

            def block(j, masked):
                keys = rows(j)
                seen = None
                if masked:
                    seen = lax.broadcasted_iota(jnp.int32, (B, B), 0) <= lax.broadcasted_iota(jnp.int32, (B, B), 1)
                scores = [_dot(k_s[keys, h // group * HEAD : (h // group + 1) * HEAD], q_s[here, h * HEAD : (h + 1) * HEAD], 1, 1) for h in range(heads)]
                weights, keeps = [], []
                for h, s in enumerate(scores):
                    if masked:
                        s = jnp.where(seen, s, HIDDEN)
                    old = top_s[h : h + 1, :]
                    top = jnp.maximum(old, s.max(axis=0, keepdims=True))
                    top_s[h : h + 1, :] = top
                    weights.append(jnp.exp2((s - top) * e).astype(BF16))
                    keeps.append(jnp.exp2((old - top) * e))
                for h in range(heads):
                    mix_s[h] = mix_s[h] * keeps[h] + _dot(v_s[h // group, :, keys], weights[h])

            lax.fori_loop(0, tb, lambda j, _: block(j, False), None)
            block(tb, True)
            for h in range(heads):
                out = mix_s[h, :HEAD, :] * (1 / mix_s[h, HEAD : HEAD + 1, :])
                q_s[here, h * HEAD : (h + 1) * HEAD] = out.T.astype(BF16)

        def columns(side, t):
            return pl.ds(pl.multiple_of(side * TILES[MAIN][1] + TILES[t][0], TILES[REST][1]), TILES[t][1])

        def part(tb, side, t):
            return _dot(q_s[rows(tb), :], wo_s[:, columns(side, t)])

        def at_tile(t):
            return pl.ds(*TILES[t])

        def to_peer(b, t):
            return remote(peer_out.at[b, :, at_tile(t)], peer_in.at[b, :, at_tile(t)], half_ss.at[t], half_rs.at[t], peer)

        def to_far(b, t):
            side = 1 if t == REST else c
            return remote(peer_in.at[b, :, at_tile(t)], far_in.at[:, columns(side, t)], far_ss.at[b * 2 + t - 2], far_rs.at[2 if t == REST else side], 2 * (1 - p) + b)

        def to_owner(side, t):
            i = 4 if t == REST else side * 2 + t
            return remote(peer_out.at[side, :, at_tile(t)], term_in.at[:, columns(side, t)], near_ss.at[i], near_rs.at[i], peer)

        def far(tb, b):
            def give(t):
                peer_out[b, :, at_tile(t)] = part(tb, 1 if t == REST else 1 - c, t).astype(BF16)

                @pl.when(b == 1)
                def _():
                    to_peer(0, t).wait_send()

                to_peer(b, t).start()

            def add(t):
                term = part(tb, 1 if t == REST else c, t)
                to_peer(b, t).wait_recv()
                peer_in[b, :, at_tile(t)] = (term + peer_in[b, :, at_tile(t)].astype(F32)).astype(BF16)

            for t in range(2):
                give(t)
            for t in range(2):
                add(t)
            to_far(b, MAIN).start()

            @pl.when(c == 0)
            def _():
                give(REST)

            @pl.when(c == 1)
            def _():
                add(REST)
                to_far(b, REST).start()

        def near(tb):
            def give(side, t):
                peer_out[side, :, at_tile(t)] = part(tb, side, t).astype(BF16)
                to_owner(side, t).start()

            def both(side, _):
                for t in range(2):
                    give(side, t)

            for t in range(2):
                to_peer(1, t).wait_send()
                own(t).wait_send()

            @pl.when(c == 0)
            def _():
                to_peer(1, REST).wait_send()

            for i in range(len(PIECES)):
                passed(i).wait_send()
            lax.fori_loop(0, 2, both, None)
            give(1, REST)

        def mine(tb):
            def keep(side, t):
                acc_s[:, columns(side, t)] = xs[rows(tb), columns(side, t)].astype(F32) + part(tb, side, t)

            def both(side, _):
                for t in range(2):
                    keep(side, t)

            lax.fori_loop(0, 2, both, None)
            keep(1, REST)

        def step(it, _):
            b = it - 2
            away = (it >= 2) & (it < 4)
            tb = jnp.where(it < 4, lax.rem(2 * p + it, 4), 2 * p + lax.rem(it + 1 + c, 2))

            def arrive(pieces):
                for i in pieces:
                    across(i, x_ss.at[0]).wait_recv()
                    passed(i).start()
                for i in pieces:
                    passed(i).wait_recv()

            @pl.when(it == 2)
            def _():
                arrive((0,))

            @pl.when(it == 3)
            def _():
                arrive((1, 2))

            @pl.when(it < 4)
            def _():
                norm(tb)

                @pl.when(it == 0)
                def _():
                    for copy in loads[3:]:
                        copy.wait()

                project(tb)

            @pl.when(it == 2)
            def _():
                load_wo.wait()

            @pl.when(it >= 2)
            def _():
                attend(tb)

            @pl.when(away)
            def _():
                far(tb, b)

            @pl.when(it == 4)
            def _():
                near(tb)

            @pl.when(it == 5)
            def _():
                mine(tb)

        lax.fori_loop(0, 6, step, None)

        def finish(side, t):
            here = columns(side, t)
            to_owner(side, t).wait_recv()
            far_in[:, here] = (acc_s[:, here] + term_in[:, here].astype(F32) + far_in[:, here].astype(F32)).astype(BF16)

        def sums(side, t):
            here = columns(side, t)
            return remote(peer_in.at[0, :, at_tile(t)], far_in.at[:, here], far_ss.at[t - 2], far_rs.at[2 if t == REST else side], cross)

        def main(side, _):
            sums(side, MAIN).wait_recv()
            for t in range(2):
                finish(side, t)

        lax.fori_loop(0, 2, main, None)
        sums(1, REST).wait_recv()
        finish(1, REST)

        for i in range(2):
            to_far(i, MAIN).wait_send()
            for t in range(2):
                to_owner(i, t).wait_send()
        across(2, x_ss.at[1]).wait_send()

        @pl.when(c == 0)
        def _():
            across(0, first_ss.at[0]).wait_send()
            across(1, x_ss.at[0]).wait_send()

        to_owner(1, REST).wait_send()

        @pl.when(c == 1)
        def _():
            across(1, first_ss.at[0]).wait_send()
            across(0, x_ss.at[0]).wait_send()
            for b in range(2):
                to_far(b, REST).wait_send()

    dma = pltpu.SemaphoreType.DMA
    pl.run_scoped(rest, dma((6,)), dma((2 + len(PIECES),)), dma((2,)), dma((3,)), dma((4,)))


def _table(tokens):
    half = HEAD // 2
    angle = np.arange(tokens)[:, None] * float(THETA) ** (-np.arange(half) / half)
    cos, sin = np.cos(angle), np.sin(angle)
    return np.concatenate([cos, cos, -sin, sin], 1).astype(np.float32)


def solution(mesh):
    def step(x, gain, wq, wk, wv, wo):
        n, d = x.shape
        tokens = 4 * n
        nq, nk = wq.shape[1], wk.shape[1]
        side = TILES[REST][0] + TILES[REST][1]
        vmem, dma = pltpu.VMEM, pltpu.SemaphoreType.DMA
        return pl.pallas_call(
            _layer,
            out_shape=pltpu.VMEM((n, d), BF16),
            in_specs=[pl.BlockSpec(memory_space=pltpu.HBM)] * 7,
            out_specs=pl.BlockSpec(memory_space=pltpu.VMEM),
            scratch_shapes=[
                vmem((tokens, d), BF16), vmem((n, d), BF16), vmem((d,), BF16), vmem((1, d), F32), vmem((tokens, 2 * HEAD), F32),
                vmem(wq.shape, BF16), vmem(wk.shape, BF16), vmem(wv.shape, BF16), vmem(wo.shape, BF16),
                vmem((tokens, nq), BF16), vmem((tokens, nk), BF16), vmem((nk // HEAD, HEAD + 16, tokens), BF16),
                vmem((nq // HEAD, n), F32), vmem((nq // HEAD, HEAD + 16, n), F32),
                vmem((2, n, side), BF16), vmem((2, n, side), BF16), vmem((n, d), BF16), vmem((n, d), F32),
                dma((1,)), dma((2 + len(PIECES),)), dma((len(PIECES),)), dma((3,)), dma((3,)), pltpu.SemaphoreType.REGULAR,
            ],
            compiler_params=pltpu.CompilerParams(collective_id=0, has_side_effects=True, vmem_limit_bytes=VMEM),
        )(x, gain, _table(tokens), wq, wk, wv, wo)

    tokens, columns = P(("dp", "tp"), None), P(None, "tp")
    return jax.shard_map(
        step,
        mesh=mesh,
        in_specs=(tokens, P(None), columns, columns, columns, P("tp", None)),
        out_specs=tokens,
        check_vma=False,
    )
```

```python
import functools

import jax
import jax.numpy as jnp
import numpy as np
from jax import lax
from jax.experimental import pallas as pl
from jax.experimental.pallas import tpu as pltpu
from jax.sharding import PartitionSpec as P

HEAD = 128
THETA = 10000
HIDDEN = -float("inf")
LOG2E = 1.4426950408889634
VMEM = 67043328 - 2560 * 1024
MESH = pl.DeviceIdType.MESH
F32, BF16 = jnp.float32, jnp.bfloat16

B = 256
PIECES = ((0, 0, 128), (1, 0, 16), (1, 16, 112))
TILES = ((0, 1024), (1024, 1024), (2048, 512), (0, 2048))
REST, MAIN = 2, 3


def _dot(a, b, ca=1, cb=0):
    return lax.dot_general(a, b, (((ca,), (cb,)), ((), ())), preferred_element_type=F32)


def _layer(x_ref, gain_ref, turn_ref, wq_ref, wk_ref, wv_ref, wo_ref, far_in,
           xs, a_s, gain_s, wide_s, turn_s, wq_s, wk_s, wv_s, wo_s, q_s, k_s, v_s, top_s, mix_s,
           peer_out, peer_in, term_in, acc_s,
           first_ss, own_rs, x_rs, in_sem):
    nq, nk = wq_s.shape[1], wk_s.shape[1]
    heads, group = nq // HEAD, nq // nk
    me = lax.axis_index("tp")
    p, c = lax.div(me, 2), lax.rem(me, 2)
    peer, cross = 2 * p + 1 - c, 2 * (1 - p) + c

    def rows(block, at=0, n=B):
        return pl.ds(pl.multiple_of(block * B + at, 16), n)

    def remote(src, dst, send, recv, to):
        return pltpu.make_async_remote_copy(src_ref=src, dst_ref=dst, send_sem=send, recv_sem=recv, device_id={"tp": to}, device_id_type=MESH)

    barrier = pltpu.get_barrier_semaphore()
    pl.semaphore_signal(barrier, inc=1, device_id={"tp": cross}, device_id_type=MESH)

    @pl.when(p == 0)
    def _():
        pl.semaphore_signal(barrier, inc=1, device_id={"tp": peer}, device_id_type=MESH)

    pl.semaphore_wait(barrier, 2 - p)

    def across(i, sem, fresh=False):
        b, at, n = PIECES[i]
        at = c * (B // 2) + at
        there = xs.at[rows(2 * p + b, at, n)]
        src = x_ref.at[pl.ds(pl.multiple_of(at, 16), n)] if fresh else there
        return remote(src, there, sem, x_rs.at[i], cross)

    @pl.when(c == 0)
    def _():
        across(0, first_ss.at[0], True).start()

    @pl.when(c == 1)
    def _():
        across(1, first_ss.at[0], True).start()

    def rest(load_sem, near_ss, near_rs, x_ss, half_ss, half_rs, far_ss, far_rs):
        def own(i):
            at = (1 - c if i == 0 else c) * (B // 2)
            return remote(x_ref.at[pl.ds(pl.multiple_of(at, B // 2), B // 2)], xs.at[rows(me, at, B // 2)], near_ss.at[i], own_rs.at[i], peer)

        def passed(i):
            b, at, n = PIECES[i]
            here = xs.at[rows(2 * (1 - p) + b, c * (B // 2) + at, n)]
            return remote(here, here, near_ss.at[2 + i], near_rs.at[2 + i], peer)

        def load(i, src, dst):
            return pltpu.make_async_copy(src, dst, load_sem.at[i])

        loads = [load(0, x_ref, xs.at[rows(me)]), load(1, gain_ref, gain_s), load(2, turn_ref, turn_s),
                 load(3, wk_ref, wk_s), load(4, wv_ref, wv_s), load(5, wq_ref, wq_s)]
        load_wo = load(0, wo_ref, wo_s)
        @pl.when(p == 0)
        def _():
            pl.semaphore_signal(in_sem, inc=1, device_id={"tp": peer}, device_id_type=MESH)
            for i in range(2):
                own(i).start()

        pl.semaphore_wait(in_sem, 1)

        @pl.when(p == 0)
        def _():
            pl.semaphore_signal(in_sem, inc=1, device_id={"tp": cross}, device_id_type=MESH)

        @pl.when(p == 1)
        def _():
            for i in range(2):
                own(i).start()

        for copy in loads:
            copy.start()
        own(0).wait_recv()

        @pl.when(c == 0)
        def _():
            across(1, x_ss.at[0]).start()
            across(2, x_ss.at[1]).start()

        @pl.when(c == 1)
        def _():
            across(0, x_ss.at[0]).start()
            across(2, x_ss.at[1], True).start()

        own(1).wait_recv()
        for copy in loads[:3]:
            copy.wait()
        load_wo.start()
        wide_s[...] = gain_s[...].astype(F32).reshape(wide_s.shape)
        for g in range(nk // HEAD):
            v_s[g, HEAD:, :] = jnp.ones((v_s.shape[1] - HEAD, v_s.shape[2]), BF16)

        def norm(tb):
            def some(i, _):
                at = pl.ds(pl.multiple_of(tb * B + i * 16, 16), 16)
                wide = xs[at, :].astype(F32)
                scale = lax.rsqrt(jnp.mean(wide * wide, -1, keepdims=True) + 1e-6)
                a_s[pl.ds(pl.multiple_of(i * 16, 16), 16), :] = (wide * scale * wide_s[...]).astype(BF16)

            lax.fori_loop(0, B // 16, some, None)

        def project(tb):
            here = rows(tb)
            cos, sin = turn_s[here, :HEAD], turn_s[here, HEAD:]

            def turned(t):
                t = t.astype(BF16).astype(F32)
                return (t * cos + pltpu.roll(t, HEAD // 2, 1) * sin).astype(BF16)

            k = _dot(a_s[...], wk_s[...])
            for n in range(0, nk, HEAD):
                k_s[here, n : n + HEAD] = turned(k[:, n : n + HEAD])
            v = _dot(a_s[...], wv_s[...])
            for g in range(nk // HEAD):
                v_s[g, :HEAD, here] = v[:, g * HEAD : (g + 1) * HEAD].T.astype(BF16)

            def queries(i, _):
                at = pl.multiple_of(i * 512, 512)
                q = _dot(a_s[...], wq_s[:, pl.ds(at, 512)])
                for n in range(0, 512, HEAD):
                    q_s[here, pl.ds(at + n, HEAD)] = turned(q[:, n : n + HEAD])

            lax.fori_loop(0, nq // 512, queries, None)

        def attend(tb):
            here = rows(tb)
            e = HEAD**-0.5 * LOG2E
            top_s[...] = jnp.full(top_s.shape, HIDDEN, F32)
            mix_s[...] = jnp.zeros(mix_s.shape, F32)

            def block(j, masked):
                keys = rows(j)
                seen = None
                if masked:
                    seen = lax.broadcasted_iota(jnp.int32, (B, B), 0) <= lax.broadcasted_iota(jnp.int32, (B, B), 1)
                scores = [_dot(k_s[keys, h // group * HEAD : (h // group + 1) * HEAD], q_s[here, h * HEAD : (h + 1) * HEAD], 1, 1) for h in range(heads)]
                weights, keeps = [], []
                for h, s in enumerate(scores):
                    if masked:
                        s = jnp.where(seen, s, HIDDEN)
                    old = top_s[h : h + 1, :]
                    top = jnp.maximum(old, s.max(axis=0, keepdims=True))
                    top_s[h : h + 1, :] = top
                    weights.append(jnp.exp2((s - top) * e).astype(BF16))
                    keeps.append(jnp.exp2((old - top) * e))
                for h in range(heads):
                    mix_s[h] = mix_s[h] * keeps[h] + _dot(v_s[h // group, :, keys], weights[h])

            lax.fori_loop(0, tb, lambda j, _: block(j, False), None)
            block(tb, True)
            for h in range(heads):
                out = mix_s[h, :HEAD, :] * (1 / mix_s[h, HEAD : HEAD + 1, :])
                q_s[here, h * HEAD : (h + 1) * HEAD] = out.T.astype(BF16)

        def columns(side, t):
            return pl.ds(pl.multiple_of(side * TILES[MAIN][1] + TILES[t][0], TILES[REST][1]), TILES[t][1])

        def part(tb, side, t):
            return _dot(q_s[rows(tb), :], wo_s[:, columns(side, t)])

        def at_tile(t):
            return pl.ds(*TILES[t])

        def to_peer(b, t):
            return remote(peer_out.at[b, :, at_tile(t)], peer_in.at[b, :, at_tile(t)], half_ss.at[t], half_rs.at[t], peer)

        def to_far(b, t):
            side = 1 if t == REST else c
            return remote(peer_in.at[b, :, at_tile(t)], far_in.at[:, columns(side, t)], far_ss.at[b * 2 + t - 2], far_rs.at[2 if t == REST else side], 2 * (1 - p) + b)

        def to_owner(side, t):
            i = 4 if t == REST else side * 2 + t
            return remote(peer_out.at[side, :, at_tile(t)], term_in.at[:, columns(side, t)], near_ss.at[i], near_rs.at[i], peer)

        def far(tb, b):
            def give(t):
                peer_out[b, :, at_tile(t)] = part(tb, 1 if t == REST else 1 - c, t).astype(BF16)

                @pl.when(b == 1)
                def _():
                    to_peer(0, t).wait_send()

                to_peer(b, t).start()

            def add(t):
                term = part(tb, 1 if t == REST else c, t)
                to_peer(b, t).wait_recv()
                peer_in[b, :, at_tile(t)] = (term + peer_in[b, :, at_tile(t)].astype(F32)).astype(BF16)

            for t in range(2):
                give(t)
            for t in range(2):
                add(t)
            to_far(b, MAIN).start()

            @pl.when(c == 0)
            def _():
                give(REST)

            @pl.when(c == 1)
            def _():
                add(REST)
                to_far(b, REST).start()

        def near(tb):
            def give(side, t):
                peer_out[side, :, at_tile(t)] = part(tb, side, t).astype(BF16)
                to_owner(side, t).start()

            def both(side, _):
                for t in range(2):
                    give(side, t)

            for t in range(2):
                to_peer(1, t).wait_send()
                own(t).wait_send()

            @pl.when(c == 0)
            def _():
                to_peer(1, REST).wait_send()

            for i in range(len(PIECES)):
                passed(i).wait_send()
            lax.fori_loop(0, 2, both, None)
            give(1, REST)

        def mine(tb):
            def keep(side, t):
                acc_s[:, columns(side, t)] = xs[rows(tb), columns(side, t)].astype(F32) + part(tb, side, t)

            def both(side, _):
                for t in range(2):
                    keep(side, t)

            lax.fori_loop(0, 2, both, None)
            keep(1, REST)

        def step(it, _):
            b = it - 2
            away = (it >= 2) & (it < 4)
            tb = jnp.where(it < 4, lax.rem(2 * p + it, 4), 2 * p + lax.rem(it + 1 + c, 2))

            def arrive(pieces):
                for i in pieces:
                    across(i, x_ss.at[0]).wait_recv()
                    passed(i).start()
                for i in pieces:
                    passed(i).wait_recv()

            @pl.when(it == 2)
            def _():
                arrive((0,))

            @pl.when(it == 3)
            def _():
                arrive((1, 2))

            @pl.when(it < 4)
            def _():
                norm(tb)

                @pl.when(it == 0)
                def _():
                    for copy in loads[3:]:
                        copy.wait()

                project(tb)

            @pl.when(it == 2)
            def _():
                load_wo.wait()

            @pl.when(it >= 2)
            def _():
                attend(tb)

            @pl.when(away)
            def _():
                far(tb, b)

            @pl.when(it == 4)
            def _():
                near(tb)

            @pl.when(it == 5)
            def _():
                mine(tb)

        lax.fori_loop(0, 6, step, None)

        def finish(side, t):
            here = columns(side, t)
            to_owner(side, t).wait_recv()
            far_in[:, here] = (acc_s[:, here] + term_in[:, here].astype(F32) + far_in[:, here].astype(F32)).astype(BF16)

        def sums(side, t):
            here = columns(side, t)
            return remote(peer_in.at[0, :, at_tile(t)], far_in.at[:, here], far_ss.at[t - 2], far_rs.at[2 if t == REST else side], cross)

        def main(side, _):
            sums(side, MAIN).wait_recv()
            for t in range(2):
                finish(side, t)

        lax.fori_loop(0, 2, main, None)
        sums(1, REST).wait_recv()
        finish(1, REST)

        for i in range(2):
            to_far(i, MAIN).wait_send()
            for t in range(2):
                to_owner(i, t).wait_send()
        across(2, x_ss.at[1]).wait_send()

        @pl.when(c == 0)
        def _():
            across(0, first_ss.at[0]).wait_send()
            across(1, x_ss.at[0]).wait_send()

        to_owner(1, REST).wait_send()

        @pl.when(c == 1)
        def _():
            across(1, first_ss.at[0]).wait_send()
            across(0, x_ss.at[0]).wait_send()
            for b in range(2):
                to_far(b, REST).wait_send()

    dma = pltpu.SemaphoreType.DMA
    near = dma((2 + len(PIECES),))
    pl.run_scoped(rest, dma((6,)), near, near, dma((2,)), dma((3,)), dma((3,)), dma((4,)), dma((3,)))


def _table(tokens):
    half = HEAD // 2
    angle = np.arange(tokens)[:, None] * float(THETA) ** (-np.arange(half) / half)
    cos, sin = np.cos(angle), np.sin(angle)
    return np.concatenate([cos, cos, -sin, sin], 1).astype(np.float32)


def solution(mesh):
    def step(x, gain, wq, wk, wv, wo):
        n, d = x.shape
        tokens = 4 * n
        nq, nk = wq.shape[1], wk.shape[1]
        side = TILES[REST][0] + TILES[REST][1]
        vmem, dma = pltpu.VMEM, pltpu.SemaphoreType.DMA
        return pl.pallas_call(
            _layer,
            out_shape=pltpu.VMEM((n, d), BF16),
            in_specs=[pl.BlockSpec(memory_space=pltpu.HBM)] * 7,
            out_specs=pl.BlockSpec(memory_space=pltpu.VMEM),
            scratch_shapes=[
                vmem((tokens, d), BF16), vmem((n, d), BF16), vmem((d,), BF16), vmem((1, d), F32), vmem((tokens, 2 * HEAD), F32),
                vmem(wq.shape, BF16), vmem(wk.shape, BF16), vmem(wv.shape, BF16), vmem(wo.shape, BF16),
                vmem((tokens, nq), BF16), vmem((tokens, nk), BF16), vmem((nk // HEAD, HEAD + 16, tokens), BF16),
                vmem((nq // HEAD, n), F32), vmem((nq // HEAD, HEAD + 16, n), F32),
                vmem((2, n, side), BF16), vmem((2, n, side), BF16), vmem((n, d), BF16), vmem((n, d), F32),
                dma((1,)), dma((2,)), dma((len(PIECES),)), pltpu.SemaphoreType.REGULAR,
            ],
            compiler_params=pltpu.CompilerParams(collective_id=0, has_side_effects=True, vmem_limit_bytes=VMEM),
        )(x, gain, _table(tokens), wq, wk, wv, wo)

    tokens, columns = P(("dp", "tp"), None), P(None, "tp")
    return jax.shard_map(
        step,
        mesh=mesh,
        in_specs=(tokens, P(None), columns, columns, columns, P("tp", None)),
        out_specs=tokens,
        check_vma=False,
    )
```

```python
import functools

import jax
import jax.numpy as jnp
import numpy as np
from jax import lax
from jax.experimental import pallas as pl
from jax.experimental.pallas import tpu as pltpu
from jax.sharding import PartitionSpec as P

HEAD = 128
THETA = 10000
HIDDEN = -float("inf")
LOG2E = 1.4426950408889634
VMEM = 67043328 - 2560 * 1024
MESH = pl.DeviceIdType.MESH
F32, BF16 = jnp.float32, jnp.bfloat16

B = 256
PIECES = ((0, 0, 128), (1, 0, 16), (1, 16, 112))
TILES = ((0, 1024), (1024, 1024), (2048, 512), (0, 2048), (2048, 384), (2432, 128))
REST, MAIN, LATE, LAST = 2, 3, 4, 5


def _dot(a, b, ca=1, cb=0):
    return lax.dot_general(a, b, (((ca,), (cb,)), ((), ())), preferred_element_type=F32)


def _layer(x_ref, gain_ref, turn_ref, wq_ref, wk_ref, wv_ref, wo_ref, far_in,
           xs, a_s, gain_s, wide_s, turn_s, wq_s, wk_s, wv_s, wo_s, q_s, k_s, v_s, top_s, mix_s,
           peer_out, peer_in, term_in, acc_s,
           first_ss, own_rs, x_rs, in_sem):
    nq, nk = wq_s.shape[1], wk_s.shape[1]
    heads, group = nq // HEAD, nq // nk
    me = lax.axis_index("tp")
    p, c = lax.div(me, 2), lax.rem(me, 2)
    peer, cross = 2 * p + 1 - c, 2 * (1 - p) + c

    def rows(block, at=0, n=B):
        return pl.ds(pl.multiple_of(block * B + at, 16), n)

    def remote(src, dst, send, recv, to):
        return pltpu.make_async_remote_copy(src_ref=src, dst_ref=dst, send_sem=send, recv_sem=recv, device_id={"tp": to}, device_id_type=MESH)

    barrier = pltpu.get_barrier_semaphore()
    pl.semaphore_signal(barrier, inc=1, device_id={"tp": cross}, device_id_type=MESH)

    @pl.when(p == 0)
    def _():
        pl.semaphore_signal(barrier, inc=1, device_id={"tp": peer}, device_id_type=MESH)

    pl.semaphore_wait(barrier, 2 - p)

    def across(i, sem, fresh=False):
        b, at, n = PIECES[i]
        at = c * (B // 2) + at
        there = xs.at[rows(2 * p + b, at, n)]
        src = x_ref.at[pl.ds(pl.multiple_of(at, 16), n)] if fresh else there
        return remote(src, there, sem, x_rs.at[i], cross)

    @pl.when(c == 0)
    def _():
        across(0, first_ss.at[0], True).start()

    @pl.when(c == 1)
    def _():
        across(1, first_ss.at[0], True).start()

    def rest(load_sem, near_ss, near_rs, x_ss, half_ss, half_rs, far_ss, far_rs):
        def own(i):
            at = (1 - c if i == 0 else c) * (B // 2)
            return remote(x_ref.at[pl.ds(pl.multiple_of(at, B // 2), B // 2)], xs.at[rows(me, at, B // 2)], near_ss.at[i], own_rs.at[i], peer)

        def passed(i):
            b, at, n = PIECES[i]
            here = xs.at[rows(2 * (1 - p) + b, c * (B // 2) + at, n)]
            return remote(here, here, near_ss.at[2 + i], near_rs.at[2 + i], peer)

        def load(i, src, dst):
            return pltpu.make_async_copy(src, dst, load_sem.at[i])

        loads = [load(0, x_ref, xs.at[rows(me)]), load(1, gain_ref, gain_s), load(2, turn_ref, turn_s),
                 load(3, wk_ref, wk_s), load(4, wv_ref, wv_s), load(5, wq_ref, wq_s)]
        load_wo = load(0, wo_ref, wo_s)
        @pl.when(p == 0)
        def _():
            pl.semaphore_signal(in_sem, inc=1, device_id={"tp": peer}, device_id_type=MESH)
            for i in range(2):
                own(i).start()

        pl.semaphore_wait(in_sem, 1)

        @pl.when(p == 0)
        def _():
            pl.semaphore_signal(in_sem, inc=1, device_id={"tp": cross}, device_id_type=MESH)

        @pl.when(p == 1)
        def _():
            for i in range(2):
                own(i).start()

        for copy in loads:
            copy.start()
        own(0).wait_recv()

        @pl.when(c == 0)
        def _():
            across(1, x_ss.at[0]).start()
            across(2, x_ss.at[1]).start()

        @pl.when(c == 1)
        def _():
            across(0, x_ss.at[0]).start()
            across(2, x_ss.at[1], True).start()

        own(1).wait_recv()
        for copy in loads[:3]:
            copy.wait()
        load_wo.start()
        wide_s[...] = gain_s[...].astype(F32).reshape(wide_s.shape)
        for g in range(nk // HEAD):
            v_s[g, HEAD:, :] = jnp.ones((v_s.shape[1] - HEAD, v_s.shape[2]), BF16)

        def norm(tb):
            def some(i, _):
                at = pl.ds(pl.multiple_of(tb * B + i * 16, 16), 16)
                wide = xs[at, :].astype(F32)
                scale = lax.rsqrt(jnp.mean(wide * wide, -1, keepdims=True) + 1e-6)
                a_s[pl.ds(pl.multiple_of(i * 16, 16), 16), :] = (wide * scale * wide_s[...]).astype(BF16)

            lax.fori_loop(0, B // 16, some, None)

        def project(tb):
            here = rows(tb)
            cos, sin = turn_s[here, :HEAD], turn_s[here, HEAD:]

            def turned(t):
                t = t.astype(BF16).astype(F32)
                return (t * cos + pltpu.roll(t, HEAD // 2, 1) * sin).astype(BF16)

            k = _dot(a_s[...], wk_s[...])
            for n in range(0, nk, HEAD):
                k_s[here, n : n + HEAD] = turned(k[:, n : n + HEAD])
            v = _dot(a_s[...], wv_s[...])
            for g in range(nk // HEAD):
                v_s[g, :HEAD, here] = v[:, g * HEAD : (g + 1) * HEAD].T.astype(BF16)

            def queries(i, _):
                at = pl.multiple_of(i * 512, 512)
                q = _dot(a_s[...], wq_s[:, pl.ds(at, 512)])
                for n in range(0, 512, HEAD):
                    q_s[here, pl.ds(at + n, HEAD)] = turned(q[:, n : n + HEAD])

            lax.fori_loop(0, nq // 512, queries, None)

        def attend(tb):
            here = rows(tb)
            e = HEAD**-0.5 * LOG2E
            top_s[...] = jnp.full(top_s.shape, HIDDEN, F32)
            mix_s[...] = jnp.zeros(mix_s.shape, F32)

            def block(j, masked):
                keys = rows(j)
                seen = None
                if masked:
                    seen = lax.broadcasted_iota(jnp.int32, (B, B), 0) <= lax.broadcasted_iota(jnp.int32, (B, B), 1)
                scores = [_dot(k_s[keys, h // group * HEAD : (h // group + 1) * HEAD], q_s[here, h * HEAD : (h + 1) * HEAD], 1, 1) for h in range(heads)]
                weights, keeps = [], []
                for h, s in enumerate(scores):
                    if masked:
                        s = jnp.where(seen, s, HIDDEN)
                    old = top_s[h : h + 1, :]
                    top = jnp.maximum(old, s.max(axis=0, keepdims=True))
                    top_s[h : h + 1, :] = top
                    weights.append(jnp.exp2((s - top) * e).astype(BF16))
                    keeps.append(jnp.exp2((old - top) * e))
                for h in range(heads):
                    mix_s[h] = mix_s[h] * keeps[h] + _dot(v_s[h // group, :, keys], weights[h])

            lax.fori_loop(0, tb, lambda j, _: block(j, False), None)
            block(tb, True)
            for h in range(heads):
                out = mix_s[h, :HEAD, :] * (1 / mix_s[h, HEAD : HEAD + 1, :])
                q_s[here, h * HEAD : (h + 1) * HEAD] = out.T.astype(BF16)

        def columns(side, t):
            return pl.ds(pl.multiple_of(side * TILES[MAIN][1] + TILES[t][0], HEAD), TILES[t][1])

        def part(tb, side, t):
            return _dot(q_s[rows(tb), :], wo_s[:, columns(side, t)])

        def at_tile(t):
            return pl.ds(*TILES[t])

        def to_peer(b, t):
            return remote(peer_out.at[b, :, at_tile(t)], peer_in.at[b, :, at_tile(t)], half_ss.at[t], half_rs.at[t], peer)

        def to_far(b, t):
            side = c if t == MAIN else 1
            return remote(peer_in.at[b, :, at_tile(t)], far_in.at[:, columns(side, t)], far_ss.at[b * 3 + t - MAIN], far_rs.at[side + t - MAIN], 2 * (1 - p) + b)

        def to_owner(side, t):
            i = 4 if t == REST else side * 2 + t
            return remote(peer_out.at[side, :, at_tile(t)], term_in.at[:, columns(side, t)], near_ss.at[i], near_rs.at[i], peer)

        def far(tb, b):
            def give(t):
                peer_out[b, :, at_tile(t)] = part(tb, 1 if t == REST else 1 - c, t).astype(BF16)

                @pl.when(b == 1)
                def _():
                    to_peer(0, t).wait_send()

                to_peer(b, t).start()

            def add(t):
                term = part(tb, 1 if t == REST else c, t)
                to_peer(b, t).wait_recv()
                peer_in[b, :, at_tile(t)] = (term + peer_in[b, :, at_tile(t)].astype(F32)).astype(BF16)

            for t in range(2):
                give(t)
            for t in range(2):
                add(t)
            to_far(b, MAIN).start()

            @pl.when(c == 0)
            def _():
                give(REST)

            @pl.when(c == 1)
            def _():
                add(REST)
                to_far(b, LATE).start()
                to_far(b, LAST).start()

        def near(tb):
            def give(side, t):
                peer_out[side, :, at_tile(t)] = part(tb, side, t).astype(BF16)
                to_owner(side, t).start()

            def both(side, _):
                for t in range(2):
                    give(side, t)

            for t in range(2):
                to_peer(1, t).wait_send()
                own(t).wait_send()

            @pl.when(c == 0)
            def _():
                to_peer(1, REST).wait_send()

            for i in range(len(PIECES)):
                passed(i).wait_send()
            lax.fori_loop(0, 2, both, None)
            give(1, REST)

        def mine(tb):
            def keep(side, t):
                acc_s[:, columns(side, t)] = xs[rows(tb), columns(side, t)].astype(F32) + part(tb, side, t)

            def both(side, _):
                for t in range(2):
                    keep(side, t)

            lax.fori_loop(0, 2, both, None)
            keep(1, REST)

        def step(it, _):
            b = it - 2
            away = (it >= 2) & (it < 4)
            tb = jnp.where(it < 4, lax.rem(2 * p + it, 4), 2 * p + lax.rem(it + 1 + c, 2))

            def arrive(pieces):
                for i in pieces:
                    across(i, x_ss.at[0]).wait_recv()
                    passed(i).start()
                for i in pieces:
                    passed(i).wait_recv()

            @pl.when(it == 2)
            def _():
                arrive((0,))

            @pl.when(it == 3)
            def _():
                arrive((1, 2))

            @pl.when(it < 4)
            def _():
                norm(tb)

                @pl.when(it == 0)
                def _():
                    for copy in loads[3:]:
                        copy.wait()

                project(tb)

            @pl.when(it == 2)
            def _():
                load_wo.wait()

            @pl.when(it >= 2)
            def _():
                attend(tb)

            @pl.when(away)
            def _():
                far(tb, b)

            @pl.when(it == 4)
            def _():
                near(tb)

            @pl.when(it == 5)
            def _():
                mine(tb)

        lax.fori_loop(0, 6, step, None)

        def finish(side, t):
            here = columns(side, t)
            far_in[:, here] = (acc_s[:, here] + term_in[:, here].astype(F32) + far_in[:, here].astype(F32)).astype(BF16)

        def sums(side, t):
            return remote(peer_in.at[0, :, at_tile(t)], far_in.at[:, columns(side, t)], far_ss.at[t - MAIN], far_rs.at[side + t - MAIN], cross)

        def main(side, _):
            sums(side, MAIN).wait_recv()
            for t in range(2):
                to_owner(side, t).wait_recv()
                finish(side, t)

        lax.fori_loop(0, 2, main, None)
        to_owner(1, REST).wait_recv()

        for i in range(2):
            to_far(i, MAIN).wait_send()
            for t in range(2):
                to_owner(i, t).wait_send()
        to_owner(1, REST).wait_send()
        across(2, x_ss.at[1]).wait_send()

        @pl.when(c == 0)
        def _():
            across(0, first_ss.at[0]).wait_send()
            across(1, x_ss.at[0]).wait_send()

        @pl.when(c == 1)
        def _():
            across(1, first_ss.at[0]).wait_send()
            across(0, x_ss.at[0]).wait_send()
            to_far(0, LATE).wait_send()
            to_far(0, LAST).wait_send()

        for t in (LATE, LAST):
            sums(1, t).wait_recv()
            finish(1, t)

        @pl.when(c == 1)
        def _():
            to_far(1, LATE).wait_send()
            to_far(1, LAST).wait_send()

    dma = pltpu.SemaphoreType.DMA
    near = dma((2 + len(PIECES),))
    pl.run_scoped(rest, dma((6,)), near, near, dma((2,)), dma((3,)), dma((3,)), dma((6,)), dma((4,)))


def _table(tokens):
    half = HEAD // 2
    angle = np.arange(tokens)[:, None] * float(THETA) ** (-np.arange(half) / half)
    cos, sin = np.cos(angle), np.sin(angle)
    return np.concatenate([cos, cos, -sin, sin], 1).astype(np.float32)


def solution(mesh):
    def step(x, gain, wq, wk, wv, wo):
        n, d = x.shape
        tokens = 4 * n
        nq, nk = wq.shape[1], wk.shape[1]
        side = TILES[REST][0] + TILES[REST][1]
        vmem, dma = pltpu.VMEM, pltpu.SemaphoreType.DMA
        return pl.pallas_call(
            _layer,
            out_shape=pltpu.VMEM((n, d), BF16),
            in_specs=[pl.BlockSpec(memory_space=pltpu.HBM)] * 7,
            out_specs=pl.BlockSpec(memory_space=pltpu.VMEM),
            scratch_shapes=[
                vmem((tokens, d), BF16), vmem((n, d), BF16), vmem((d,), BF16), vmem((1, d), F32), vmem((tokens, 2 * HEAD), F32),
                vmem(wq.shape, BF16), vmem(wk.shape, BF16), vmem(wv.shape, BF16), vmem(wo.shape, BF16),
                vmem((tokens, nq), BF16), vmem((tokens, nk), BF16), vmem((nk // HEAD, HEAD + 16, tokens), BF16),
                vmem((nq // HEAD, n), F32), vmem((nq // HEAD, HEAD + 16, n), F32),
                vmem((2, n, side), BF16), vmem((2, n, side), BF16), vmem((n, d), BF16), vmem((n, d), F32),
                dma((1,)), dma((2,)), dma((len(PIECES),)), pltpu.SemaphoreType.REGULAR,
            ],
            compiler_params=pltpu.CompilerParams(collective_id=0, has_side_effects=True, vmem_limit_bytes=VMEM),
        )(x, gain, _table(tokens), wq, wk, wv, wo)

    tokens, columns = P(("dp", "tp"), None), P(None, "tp")
    return jax.shard_map(
        step,
        mesh=mesh,
        in_specs=(tokens, P(None), columns, columns, columns, P("tp", None)),
        out_specs=tokens,
        check_vma=False,
    )
```

```python
import functools

import jax
import jax.numpy as jnp
import numpy as np
from jax import lax
from jax.experimental import pallas as pl
from jax.experimental.pallas import tpu as pltpu
from jax.sharding import PartitionSpec as P

HEAD = 128
THETA = 10000
HIDDEN = -float("inf")
LOG2E = 1.4426950408889634
VMEM = 67043328 - 2560 * 1024
MESH = pl.DeviceIdType.MESH
F32, BF16 = jnp.float32, jnp.bfloat16

B = 256
PIECES = ((0, 0, 128), (1, 0, 16), (1, 16, 112))
TILES = ((0, 1024), (1024, 1024), (2048, 512), (0, 2048), (2048, 384), (2432, 128))
REST, MAIN, LATE, LAST = 2, 3, 4, 5


def _dot(a, b, ca=1, cb=0):
    return lax.dot_general(a, b, (((ca,), (cb,)), ((), ())), preferred_element_type=F32)


def _layer(x_ref, gain_ref, turn_ref, wq_ref, wk_ref, wv_ref, wo_ref, far_in,
           xs, a_s, gain_s, wide_s, turn_s, wq_s, wk_s, wv_s, wo_s, q_s, k_s, v_s, top_s, mix_s,
           peer_out, peer_in, term_in, acc_s,
           first_ss, own_rs, x_rs, in_sem):
    nq, nk = wq_s.shape[1], wk_s.shape[1]
    heads, group = nq // HEAD, nq // nk
    me = lax.axis_index("tp")
    p, c = lax.div(me, 2), lax.rem(me, 2)
    peer, cross = 2 * p + 1 - c, 2 * (1 - p) + c

    def rows(block, at=0, n=B):
        return pl.ds(pl.multiple_of(block * B + at, 16), n)

    def remote(src, dst, send, recv, to):
        return pltpu.make_async_remote_copy(src_ref=src, dst_ref=dst, send_sem=send, recv_sem=recv, device_id={"tp": to}, device_id_type=MESH)

    barrier = pltpu.get_barrier_semaphore()
    pl.semaphore_signal(barrier, inc=1, device_id={"tp": cross}, device_id_type=MESH)

    @pl.when(p == 0)
    def _():
        pl.semaphore_signal(barrier, inc=1, device_id={"tp": peer}, device_id_type=MESH)

    pl.semaphore_wait(barrier, 2 - p)

    def across(i, sem, fresh=False):
        b, at, n = PIECES[i]
        at = c * (B // 2) + at
        there = xs.at[rows(2 * p + b, at, n)]
        src = x_ref.at[pl.ds(pl.multiple_of(at, 16), n)] if fresh else there
        return remote(src, there, sem, x_rs.at[b], cross)

    @pl.when(c == 0)
    def _():
        across(0, first_ss.at[0], True).start()

    @pl.when(c == 1)
    def _():
        across(1, first_ss.at[0], True).start()

    def rest(load_sem, near_ss, near_rs, x_ss, half_ss, half_rs, far_ss, far_rs):
        def own(i):
            at = (1 - c if i == 0 else c) * (B // 2)
            return remote(x_ref.at[pl.ds(pl.multiple_of(at, B // 2), B // 2)], xs.at[rows(me, at, B // 2)], near_ss.at[i], own_rs.at[i], peer)

        def came(b):
            return xs.at[rows(2 * (1 - p) + b, c * (B // 2), B // 2)]

        def passed(b):
            return remote(came(b), came(b), near_ss.at[2 + b], near_rs.at[2 + b], peer)

        def load(i, src, dst):
            return pltpu.make_async_copy(src, dst, load_sem.at[i])

        loads = [load(0, x_ref, xs.at[rows(me)]), load(1, gain_ref, gain_s), load(2, turn_ref, turn_s),
                 load(3, wk_ref, wk_s), load(4, wv_ref, wv_s), load(5, wq_ref, wq_s)]
        load_wo = load(0, wo_ref, wo_s)
        @pl.when(p == 0)
        def _():
            pl.semaphore_signal(in_sem, inc=1, device_id={"tp": peer}, device_id_type=MESH)
            for i in range(2):
                own(i).start()

        pl.semaphore_wait(in_sem, 1)

        @pl.when(p == 0)
        def _():
            pl.semaphore_signal(in_sem, inc=1, device_id={"tp": cross}, device_id_type=MESH)

        @pl.when(p == 1)
        def _():
            for i in range(2):
                own(i).start()

        for copy in loads:
            copy.start()
        own(0).wait_recv()

        @pl.when(c == 0)
        def _():
            across(1, x_ss.at[0]).start()
            across(2, x_ss.at[1]).start()

        @pl.when(c == 1)
        def _():
            across(0, x_ss.at[0]).start()
            across(2, x_ss.at[1], True).start()

        own(1).wait_recv()
        for copy in loads[:3]:
            copy.wait()
        load_wo.start()
        wide_s[...] = gain_s[...].astype(F32).reshape(wide_s.shape)
        for g in range(nk // HEAD):
            v_s[g, HEAD:, :] = jnp.ones((v_s.shape[1] - HEAD, v_s.shape[2]), BF16)

        def norm(tb):
            def some(i, _):
                at = pl.ds(pl.multiple_of(tb * B + i * 16, 16), 16)
                wide = xs[at, :].astype(F32)
                scale = lax.rsqrt(jnp.mean(wide * wide, -1, keepdims=True) + 1e-6)
                a_s[pl.ds(pl.multiple_of(i * 16, 16), 16), :] = (wide * scale * wide_s[...]).astype(BF16)

            lax.fori_loop(0, B // 16, some, None)

        def project(tb, first):
            def loaded(i):
                @pl.when(first)
                def _():
                    loads[i].wait()

            here = rows(tb)
            cos, sin = turn_s[here, :HEAD], turn_s[here, HEAD:]

            def turned(t):
                t = t.astype(BF16).astype(F32)
                return (t * cos + pltpu.roll(t, HEAD // 2, 1) * sin).astype(BF16)

            loaded(3)
            k = _dot(a_s[...], wk_s[...])
            for n in range(0, nk, HEAD):
                k_s[here, n : n + HEAD] = turned(k[:, n : n + HEAD])
            loaded(4)
            v = _dot(a_s[...], wv_s[...])
            for g in range(nk // HEAD):
                v_s[g, :HEAD, here] = v[:, g * HEAD : (g + 1) * HEAD].T.astype(BF16)

            def queries(i, _):
                at = pl.multiple_of(i * 512, 512)
                q = _dot(a_s[...], wq_s[:, pl.ds(at, 512)])
                for n in range(0, 512, HEAD):
                    q_s[here, pl.ds(at + n, HEAD)] = turned(q[:, n : n + HEAD])

            loaded(5)
            lax.fori_loop(0, nq // 512, queries, None)

        def attend(tb):
            here = rows(tb)
            e = HEAD**-0.5 * LOG2E
            top_s[...] = jnp.full(top_s.shape, HIDDEN, F32)
            mix_s[...] = jnp.zeros(mix_s.shape, F32)

            def block(j, masked):
                keys = rows(j)
                seen = None
                if masked:
                    seen = lax.broadcasted_iota(jnp.int32, (B, B), 0) <= lax.broadcasted_iota(jnp.int32, (B, B), 1)
                scores = [_dot(k_s[keys, h // group * HEAD : (h // group + 1) * HEAD], q_s[here, h * HEAD : (h + 1) * HEAD], 1, 1) for h in range(heads)]
                weights, keeps = [], []
                for h, s in enumerate(scores):
                    if masked:
                        s = jnp.where(seen, s, HIDDEN)
                    old = top_s[h : h + 1, :]
                    top = jnp.maximum(old, s.max(axis=0, keepdims=True))
                    top_s[h : h + 1, :] = top
                    weights.append(jnp.exp2((s - top) * e).astype(BF16))
                    keeps.append(jnp.exp2((old - top) * e))
                for h in range(heads):
                    mix_s[h] = mix_s[h] * keeps[h] + _dot(v_s[h // group, :, keys], weights[h])

            lax.fori_loop(0, tb, lambda j, _: block(j, False), None)
            block(tb, True)
            for h in range(heads):
                out = mix_s[h, :HEAD, :] * (1 / mix_s[h, HEAD : HEAD + 1, :])
                q_s[here, h * HEAD : (h + 1) * HEAD] = out.T.astype(BF16)

        def columns(side, t):
            return pl.ds(pl.multiple_of(side * TILES[MAIN][1] + TILES[t][0], HEAD), TILES[t][1])

        def part(tb, side, t):
            return _dot(q_s[rows(tb), :], wo_s[:, columns(side, t)])

        def at_tile(t):
            return pl.ds(*TILES[t])

        def to_peer(b, t):
            return remote(peer_out.at[b, :, at_tile(t)], peer_in.at[b, :, at_tile(t)], half_ss.at[t], half_rs.at[t], peer)

        def to_far(b, t):
            side = c if t == MAIN else 1
            return remote(peer_in.at[b, :, at_tile(t)], far_in.at[:, columns(side, t)], far_ss.at[b * 3 + t - MAIN], far_rs.at[side + t - MAIN], 2 * (1 - p) + b)

        def to_owner(side, t):
            i = 4 if t == REST else side * 2 + t
            return remote(peer_out.at[side, :, at_tile(t)], term_in.at[:, columns(side, t)], near_ss.at[i], near_rs.at[i], peer)

        def far(tb, b):
            def give(t):
                peer_out[b, :, at_tile(t)] = part(tb, 1 if t == REST else 1 - c, t).astype(BF16)

                @pl.when(b == 1)
                def _():
                    to_peer(0, t).wait_send()

                to_peer(b, t).start()

            def add(t):
                term = part(tb, 1 if t == REST else c, t)
                to_peer(b, t).wait_recv()
                peer_in[b, :, at_tile(t)] = (term + peer_in[b, :, at_tile(t)].astype(F32)).astype(BF16)

            for t in range(2):
                give(t)
            for t in range(2):
                add(t)
            to_far(b, MAIN).start()

            @pl.when(c == 0)
            def _():
                give(REST)

            @pl.when(c == 1)
            def _():
                add(REST)
                to_far(b, LATE).start()
                to_far(b, LAST).start()

        def near(tb):
            def give(side, t):
                peer_out[side, :, at_tile(t)] = part(tb, side, t).astype(BF16)
                to_owner(side, t).start()

            def both(side, _):
                for t in range(2):
                    give(side, t)

            for t in range(2):
                to_peer(1, t).wait_send()
                own(t).wait_send()

            @pl.when(c == 0)
            def _():
                to_peer(1, REST).wait_send()

            for b in range(2):
                passed(b).wait_send()
            lax.fori_loop(0, 2, both, None)
            give(1, REST)

        def mine(tb):
            def keep(side, t):
                acc_s[:, columns(side, t)] = xs[rows(tb), columns(side, t)].astype(F32) + part(tb, side, t)

            def both(side, _):
                for t in range(2):
                    keep(side, t)

            lax.fori_loop(0, 2, both, None)
            keep(1, REST)

        def step(it, _):
            b = it - 2
            away = (it >= 2) & (it < 4)
            tb = jnp.where(it < 4, lax.rem(2 * p + it, 4), 2 * p + lax.rem(it + 1 + c, 2))

            @pl.when(away)
            def _():
                remote(came(b), came(b), x_ss.at[0], x_rs.at[b], cross).wait_recv()
                passed(b).start()
                passed(b).wait_recv()

            @pl.when(it < 4)
            def _():
                norm(tb)
                project(tb, it == 0)

            @pl.when(it == 2)
            def _():
                load_wo.wait()

            @pl.when(it >= 2)
            def _():
                attend(tb)

            @pl.when(away)
            def _():
                far(tb, b)

            @pl.when(it == 4)
            def _():
                near(tb)

            @pl.when(it == 5)
            def _():
                mine(tb)

        lax.fori_loop(0, 6, step, None)

        def finish(side, t):
            here = columns(side, t)
            far_in[:, here] = (acc_s[:, here] + term_in[:, here].astype(F32) + far_in[:, here].astype(F32)).astype(BF16)

        def sums(side, t):
            return remote(peer_in.at[0, :, at_tile(t)], far_in.at[:, columns(side, t)], far_ss.at[t - MAIN], far_rs.at[side + t - MAIN], cross)

        def main(side, _):
            sums(side, MAIN).wait_recv()
            for t in range(2):
                to_owner(side, t).wait_recv()
                finish(side, t)

        lax.fori_loop(0, 2, main, None)
        to_owner(1, REST).wait_recv()

        for i in range(2):
            to_far(i, MAIN).wait_send()
            for t in range(2):
                to_owner(i, t).wait_send()
        to_owner(1, REST).wait_send()
        across(2, x_ss.at[1]).wait_send()

        @pl.when(c == 0)
        def _():
            across(0, first_ss.at[0]).wait_send()
            across(1, x_ss.at[0]).wait_send()

        @pl.when(c == 1)
        def _():
            across(1, first_ss.at[0]).wait_send()
            across(0, x_ss.at[0]).wait_send()
            to_far(0, LATE).wait_send()
            to_far(0, LAST).wait_send()

        for t in (LATE, LAST):
            sums(1, t).wait_recv()
            finish(1, t)

        @pl.when(c == 1)
        def _():
            to_far(1, LATE).wait_send()
            to_far(1, LAST).wait_send()

    dma = pltpu.SemaphoreType.DMA
    near = dma((5,))
    pl.run_scoped(rest, dma((6,)), near, near, dma((2,)), dma((3,)), dma((3,)), dma((6,)), dma((4,)))


def _table(tokens):
    half = HEAD // 2
    angle = np.arange(tokens)[:, None] * float(THETA) ** (-np.arange(half) / half)
    cos, sin = np.cos(angle), np.sin(angle)
    return np.concatenate([cos, cos, -sin, sin], 1).astype(np.float32)


def solution(mesh):
    def step(x, gain, wq, wk, wv, wo):
        n, d = x.shape
        tokens = 4 * n
        nq, nk = wq.shape[1], wk.shape[1]
        side = TILES[REST][0] + TILES[REST][1]
        vmem, dma = pltpu.VMEM, pltpu.SemaphoreType.DMA
        return pl.pallas_call(
            _layer,
            out_shape=pltpu.VMEM((n, d), BF16),
            in_specs=[pl.BlockSpec(memory_space=pltpu.HBM)] * 7,
            out_specs=pl.BlockSpec(memory_space=pltpu.VMEM),
            scratch_shapes=[
                vmem((tokens, d), BF16), vmem((n, d), BF16), vmem((d,), BF16), vmem((1, d), F32), vmem((tokens, 2 * HEAD), F32),
                vmem(wq.shape, BF16), vmem(wk.shape, BF16), vmem(wv.shape, BF16), vmem(wo.shape, BF16),
                vmem((tokens, nq), BF16), vmem((tokens, nk), BF16), vmem((nk // HEAD, HEAD + 16, tokens), BF16),
                vmem((nq // HEAD, n), F32), vmem((nq // HEAD, HEAD + 16, n), F32),
                vmem((2, n, side), BF16), vmem((2, n, side), BF16), vmem((n, d), BF16), vmem((n, d), F32),
                dma((1,)), dma((2,)), dma((2,)), pltpu.SemaphoreType.REGULAR,
            ],
            compiler_params=pltpu.CompilerParams(collective_id=0, has_side_effects=True, vmem_limit_bytes=VMEM),
        )(x, gain, _table(tokens), wq, wk, wv, wo)

    tokens, columns = P(("dp", "tp"), None), P(None, "tp")
    return jax.shard_map(
        step,
        mesh=mesh,
        in_specs=(tokens, P(None), columns, columns, columns, P("tp", None)),
        out_specs=tokens,
        check_vma=False,
    )
```

```python
import functools

import jax
import jax.numpy as jnp
import numpy as np
from jax import lax
from jax.experimental import pallas as pl
from jax.experimental.pallas import tpu as pltpu
from jax.sharding import PartitionSpec as P

HEAD = 128
THETA = 10000
HIDDEN = -float("inf")
LOG2E = 1.4426950408889634
VMEM = 67043328 - 2560 * 1024
MESH = pl.DeviceIdType.MESH
F32, BF16 = jnp.float32, jnp.bfloat16

B = 256
PIECES = ((0, 0, 128), (1, 0, 16), (1, 16, 112))
TILES = ((0, 1024), (1024, 1024), (2048, 512), (0, 2048), (2048, 384), (2432, 128))
REST, MAIN, LATE, LAST = 2, 3, 4, 5


def _dot(a, b, ca=1, cb=0):
    return lax.dot_general(a, b, (((ca,), (cb,)), ((), ())), preferred_element_type=F32)


def _layer(x_ref, gain_ref, turn_ref, wq_ref, wk_ref, wv_ref, wo_ref, far_in,
           xs, a_s, gain_s, wide_s, turn_s, wq_s, wk_s, wv_s, wo_s, q_s, k_s, v_s, top_s, mix_s,
           peer_out, peer_in, term_in, acc_s,
           first_ss, own_rs, x_rs, in_sem):
    nq, nk = wq_s.shape[1], wk_s.shape[1]
    heads, group = nq // HEAD, nq // nk
    me = lax.axis_index("tp")
    p, c = lax.div(me, 2), lax.rem(me, 2)
    peer, cross = 2 * p + 1 - c, 2 * (1 - p) + c

    def rows(block, at=0, n=B):
        return pl.ds(pl.multiple_of(block * B + at, 16), n)

    def remote(src, dst, send, recv, to):
        return pltpu.make_async_remote_copy(src_ref=src, dst_ref=dst, send_sem=send, recv_sem=recv, device_id={"tp": to}, device_id_type=MESH)

    barrier = pltpu.get_barrier_semaphore()
    pl.semaphore_signal(barrier, inc=1, device_id={"tp": cross}, device_id_type=MESH)

    @pl.when(p == 0)
    def _():
        pl.semaphore_signal(barrier, inc=1, device_id={"tp": peer}, device_id_type=MESH)

    pl.semaphore_wait(barrier, 2 - p)

    def across(i, sem, fresh=False):
        b, at, n = PIECES[i]
        at = c * (B // 2) + at
        there = xs.at[rows(2 * p + b, at, n)]
        src = x_ref.at[pl.ds(pl.multiple_of(at, 16), n)] if fresh else there
        return remote(src, there, sem, x_rs.at[b], cross)

    @pl.when(c == 0)
    def _():
        across(0, first_ss.at[0], True).start()

    @pl.when(c == 1)
    def _():
        across(1, first_ss.at[0], True).start()

    def rest(load_sem, near_ss, near_rs, x_ss, half_ss, half_rs, far_ss, far_rs):
        def own(i):
            at = (1 - c if i == 0 else c) * (B // 2)
            return remote(x_ref.at[pl.ds(pl.multiple_of(at, B // 2), B // 2)], xs.at[rows(me, at, B // 2)], near_ss.at[i], near_rs.at[1] if i else own_rs.at[0], peer)

        def came(b):
            return xs.at[rows(2 * (1 - p) + b, c * (B // 2), B // 2)]

        def passed(b):
            return remote(came(b), came(b), near_ss.at[2 + b], near_rs.at[2 + b], peer)

        def load(i, src, dst):
            return pltpu.make_async_copy(src, dst, load_sem.at[i])

        loads = [load(0, x_ref, xs.at[rows(me)]), load(1, gain_ref, gain_s), load(2, turn_ref, turn_s),
                 load(3, wk_ref, wk_s), load(4, wv_ref, wv_s), load(5, wq_ref, wq_s)]
        load_wo = load(0, wo_ref, wo_s)
        @pl.when(p == 0)
        def _():
            pl.semaphore_signal(in_sem, inc=1, device_id={"tp": peer}, device_id_type=MESH)
            own(0).start()

        pl.semaphore_wait(in_sem, 1)

        @pl.when(p == 0)
        def _():
            pl.semaphore_signal(in_sem, inc=1, device_id={"tp": cross}, device_id_type=MESH)

        @pl.when(p == 1)
        def _():
            own(0).start()

        for copy in loads:
            copy.start()
        own(0).wait_recv()

        @pl.when(c == 0)
        def _():
            across(1, x_ss.at[0]).start()
            across(2, x_ss.at[1]).start()

        @pl.when(c == 1)
        def _():
            across(0, x_ss.at[0]).start()
            across(2, x_ss.at[1], True).start()

        own(1).start()
        own(1).wait_recv()
        for copy in loads[:3]:
            copy.wait()
        load_wo.start()
        wide_s[...] = gain_s[...].astype(F32).reshape(wide_s.shape)
        for g in range(nk // HEAD):
            v_s[g, HEAD:, :] = jnp.ones((v_s.shape[1] - HEAD, v_s.shape[2]), BF16)

        def norm(tb):
            def some(i, _):
                at = pl.ds(pl.multiple_of(tb * B + i * 16, 16), 16)
                wide = xs[at, :].astype(F32)
                scale = lax.rsqrt(jnp.mean(wide * wide, -1, keepdims=True) + 1e-6)
                a_s[pl.ds(pl.multiple_of(i * 16, 16), 16), :] = (wide * scale * wide_s[...]).astype(BF16)

            lax.fori_loop(0, B // 16, some, None)

        def project(tb, first):
            def loaded(i):
                @pl.when(first)
                def _():
                    loads[i].wait()

            here = rows(tb)
            cos, sin = turn_s[here, :HEAD], turn_s[here, HEAD:]

            def turned(t):
                t = t.astype(BF16).astype(F32)
                return (t * cos + pltpu.roll(t, HEAD // 2, 1) * sin).astype(BF16)

            loaded(3)
            k = _dot(a_s[...], wk_s[...])
            for n in range(0, nk, HEAD):
                k_s[here, n : n + HEAD] = turned(k[:, n : n + HEAD])
            loaded(4)
            v = _dot(a_s[...], wv_s[...])
            for g in range(nk // HEAD):
                v_s[g, :HEAD, here] = v[:, g * HEAD : (g + 1) * HEAD].T.astype(BF16)

            def queries(i, _):
                at = pl.multiple_of(i * 512, 512)
                q = _dot(a_s[...], wq_s[:, pl.ds(at, 512)])
                for n in range(0, 512, HEAD):
                    q_s[here, pl.ds(at + n, HEAD)] = turned(q[:, n : n + HEAD])

            loaded(5)
            lax.fori_loop(0, nq // 512, queries, None)

        def attend(tb):
            here = rows(tb)
            e = HEAD**-0.5 * LOG2E
            top_s[...] = jnp.full(top_s.shape, HIDDEN, F32)
            mix_s[...] = jnp.zeros(mix_s.shape, F32)

            def block(j, masked):
                keys = rows(j)
                seen = None
                if masked:
                    seen = lax.broadcasted_iota(jnp.int32, (B, B), 0) <= lax.broadcasted_iota(jnp.int32, (B, B), 1)
                scores = [_dot(k_s[keys, h // group * HEAD : (h // group + 1) * HEAD], q_s[here, h * HEAD : (h + 1) * HEAD], 1, 1) for h in range(heads)]
                weights, keeps = [], []
                for h, s in enumerate(scores):
                    if masked:
                        s = jnp.where(seen, s, HIDDEN)
                    old = top_s[h : h + 1, :]
                    top = jnp.maximum(old, s.max(axis=0, keepdims=True))
                    top_s[h : h + 1, :] = top
                    weights.append(jnp.exp2((s - top) * e).astype(BF16))
                    keeps.append(jnp.exp2((old - top) * e))
                for h in range(heads):
                    mix_s[h] = mix_s[h] * keeps[h] + _dot(v_s[h // group, :, keys], weights[h])

            lax.fori_loop(0, tb, lambda j, _: block(j, False), None)
            block(tb, True)
            for h in range(heads):
                out = mix_s[h, :HEAD, :] * (1 / mix_s[h, HEAD : HEAD + 1, :])
                q_s[here, h * HEAD : (h + 1) * HEAD] = out.T.astype(BF16)

        def columns(side, t):
            return pl.ds(pl.multiple_of(side * TILES[MAIN][1] + TILES[t][0], HEAD), TILES[t][1])

        def part(tb, side, t):
            return _dot(q_s[rows(tb), :], wo_s[:, columns(side, t)])

        def at_tile(t):
            return pl.ds(*TILES[t])

        def to_peer(b, t):
            return remote(peer_out.at[b, :, at_tile(t)], peer_in.at[b, :, at_tile(t)], half_ss.at[t], half_rs.at[t], peer)

        def to_far(b, t):
            side = c if t == MAIN else 1
            return remote(peer_in.at[b, :, at_tile(t)], far_in.at[:, columns(side, t)], far_ss.at[b * 3 + t - MAIN], far_rs.at[side + t - MAIN], 2 * (1 - p) + b)

        def to_owner(side, t):
            i = 4 if t == REST else side * 2 + t
            return remote(peer_out.at[side, :, at_tile(t)], term_in.at[:, columns(side, t)], near_ss.at[i], near_rs.at[i], peer)

        def far(tb, b):
            def give(t):
                peer_out[b, :, at_tile(t)] = part(tb, 1 if t == REST else 1 - c, t).astype(BF16)

                @pl.when(b == 1)
                def _():
                    to_peer(0, t).wait_send()

                to_peer(b, t).start()

            def add(t):
                term = part(tb, 1 if t == REST else c, t)
                to_peer(b, t).wait_recv()
                peer_in[b, :, at_tile(t)] = (term + peer_in[b, :, at_tile(t)].astype(F32)).astype(BF16)

            for t in range(2):
                give(t)
            for t in range(2):
                add(t)
            to_far(b, MAIN).start()

            @pl.when(c == 0)
            def _():
                give(REST)

            @pl.when(c == 1)
            def _():
                add(REST)
                to_far(b, LATE).start()
                to_far(b, LAST).start()

        def near(tb):
            def give(side, t):
                peer_out[side, :, at_tile(t)] = part(tb, side, t).astype(BF16)
                to_owner(side, t).start()

            def both(side, _):
                for t in range(2):
                    give(side, t)

            for t in range(2):
                to_peer(1, t).wait_send()
                own(t).wait_send()

            @pl.when(c == 0)
            def _():
                to_peer(1, REST).wait_send()

            for b in range(2):
                passed(b).wait_send()
            lax.fori_loop(0, 2, both, None)
            give(1, REST)

        def mine(tb):
            def keep(side, t):
                acc_s[:, columns(side, t)] = xs[rows(tb), columns(side, t)].astype(F32) + part(tb, side, t)

            def both(side, _):
                for t in range(2):
                    keep(side, t)

            lax.fori_loop(0, 2, both, None)
            keep(1, REST)

        def step(it, _):
            b = it - 2
            away = (it >= 2) & (it < 4)
            tb = jnp.where(it < 4, lax.rem(2 * p + it, 4), 2 * p + lax.rem(it + 1 + c, 2))

            @pl.when(away)
            def _():
                remote(came(b), came(b), x_ss.at[0], x_rs.at[b], cross).wait_recv()
                passed(b).start()
                passed(b).wait_recv()

            @pl.when(it < 4)
            def _():
                norm(tb)
                project(tb, it == 0)

            @pl.when(it == 2)
            def _():
                load_wo.wait()

            @pl.when(it >= 2)
            def _():
                attend(tb)

            @pl.when(away)
            def _():
                far(tb, b)

            @pl.when(it == 4)
            def _():
                near(tb)

            @pl.when(it == 5)
            def _():
                mine(tb)

        lax.fori_loop(0, 6, step, None)

        def finish(side, t):
            here = columns(side, t)
            far_in[:, here] = (acc_s[:, here] + term_in[:, here].astype(F32) + far_in[:, here].astype(F32)).astype(BF16)

        def sums(side, t):
            return remote(peer_in.at[0, :, at_tile(t)], far_in.at[:, columns(side, t)], far_ss.at[t - MAIN], far_rs.at[side + t - MAIN], cross)

        def main(side, _):
            sums(side, MAIN).wait_recv()
            for t in range(2):
                to_owner(side, t).wait_recv()
                finish(side, t)

        lax.fori_loop(0, 2, main, None)
        to_owner(1, REST).wait_recv()

        for i in range(2):
            to_far(i, MAIN).wait_send()
            for t in range(2):
                to_owner(i, t).wait_send()
        to_owner(1, REST).wait_send()
        across(2, x_ss.at[1]).wait_send()

        @pl.when(c == 0)
        def _():
            across(0, first_ss.at[0]).wait_send()
            across(1, x_ss.at[0]).wait_send()

        @pl.when(c == 1)
        def _():
            across(1, first_ss.at[0]).wait_send()
            across(0, x_ss.at[0]).wait_send()
            to_far(0, LATE).wait_send()
            to_far(0, LAST).wait_send()

        for t in (LATE, LAST):
            sums(1, t).wait_recv()
            finish(1, t)

        @pl.when(c == 1)
        def _():
            to_far(1, LATE).wait_send()
            to_far(1, LAST).wait_send()

    dma = pltpu.SemaphoreType.DMA
    near = dma((5,))
    pl.run_scoped(rest, dma((6,)), near, near, dma((2,)), dma((3,)), dma((3,)), dma((6,)), dma((4,)))


def _table(tokens):
    half = HEAD // 2
    angle = np.arange(tokens)[:, None] * float(THETA) ** (-np.arange(half) / half)
    cos, sin = np.cos(angle), np.sin(angle)
    return np.concatenate([cos, cos, -sin, sin], 1).astype(np.float32)


def solution(mesh):
    def step(x, gain, wq, wk, wv, wo):
        n, d = x.shape
        tokens = 4 * n
        nq, nk = wq.shape[1], wk.shape[1]
        side = TILES[REST][0] + TILES[REST][1]
        vmem, dma = pltpu.VMEM, pltpu.SemaphoreType.DMA
        return pl.pallas_call(
            _layer,
            out_shape=pltpu.VMEM((n, d), BF16),
            in_specs=[pl.BlockSpec(memory_space=pltpu.HBM)] * 7,
            out_specs=pl.BlockSpec(memory_space=pltpu.VMEM),
            scratch_shapes=[
                vmem((tokens, d), BF16), vmem((n, d), BF16), vmem((d,), BF16), vmem((1, d), F32), vmem((tokens, 2 * HEAD), F32),
                vmem(wq.shape, BF16), vmem(wk.shape, BF16), vmem(wv.shape, BF16), vmem(wo.shape, BF16),
                vmem((tokens, nq), BF16), vmem((tokens, nk), BF16), vmem((nk // HEAD, HEAD + 16, tokens), BF16),
                vmem((nq // HEAD, n), F32), vmem((nq // HEAD, HEAD + 16, n), F32),
                vmem((2, n, side), BF16), vmem((2, n, side), BF16), vmem((n, d), BF16), vmem((n, d), F32),
                dma((1,)), dma((1,)), dma((2,)), pltpu.SemaphoreType.REGULAR,
            ],
            compiler_params=pltpu.CompilerParams(collective_id=0, has_side_effects=True, vmem_limit_bytes=VMEM),
        )(x, gain, _table(tokens), wq, wk, wv, wo)

    tokens, columns = P(("dp", "tp"), None), P(None, "tp")
    return jax.shard_map(
        step,
        mesh=mesh,
        in_specs=(tokens, P(None), columns, columns, columns, P("tp", None)),
        out_specs=tokens,
        check_vma=False,
    )
```

```python
import functools

import jax
import jax.numpy as jnp
import numpy as np
from jax import lax
from jax.experimental import pallas as pl
from jax.experimental.pallas import tpu as pltpu
from jax.sharding import PartitionSpec as P

HEAD = 128
THETA = 10000
HIDDEN = -float("inf")
LOG2E = 1.4426950408889634
VMEM = 67043328 - 2560 * 1024
MESH = pl.DeviceIdType.MESH
F32, BF16 = jnp.float32, jnp.bfloat16

B = 256
PIECES = ((0, 0, 128), (1, 0, 16), (1, 16, 112))
TILES = ((0, 1024), (1024, 1024), (2048, 512), (0, 2048), (2048, 384), (2432, 128))
REST, MAIN, LATE, LAST = 2, 3, 4, 5


def _dot(a, b, ca=1, cb=0):
    return lax.dot_general(a, b, (((ca,), (cb,)), ((), ())), preferred_element_type=F32)


def _layer(x_ref, gain_ref, turn_ref, wq_ref, wk_ref, wv_ref, wo_ref, far_in,
           xs, a_s, gain_s, wide_s, turn_s, wq_s, wk_s, wv_s, wo_s, q_s, k_s, v_s, top_s, mix_s,
           peer_out, peer_in, term_in, acc_s,
           first_ss, own_rs, x_rs, in_sem):
    nq, nk = wq_s.shape[1], wk_s.shape[1]
    heads, group = nq // HEAD, nq // nk
    me = lax.axis_index("tp")
    p, c = lax.div(me, 2), lax.rem(me, 2)
    peer, cross = 2 * p + 1 - c, 2 * (1 - p) + c

    def rows(block, at=0, n=B):
        return pl.ds(pl.multiple_of(block * B + at, 16), n)

    def remote(src, dst, send, recv, to):
        return pltpu.make_async_remote_copy(src_ref=src, dst_ref=dst, send_sem=send, recv_sem=recv, device_id={"tp": to}, device_id_type=MESH)

    barrier = pltpu.get_barrier_semaphore()
    pl.semaphore_signal(barrier, inc=1, device_id={"tp": cross}, device_id_type=MESH)

    @pl.when(p == 0)
    def _():
        pl.semaphore_signal(barrier, inc=1, device_id={"tp": peer}, device_id_type=MESH)

    pl.semaphore_wait(barrier, 2 - p)

    def across(i, sem, fresh=False):
        b, at, n = PIECES[i]
        at = c * (B // 2) + at
        there = xs.at[rows(2 * p + b, at, n)]
        src = x_ref.at[pl.ds(pl.multiple_of(at, 16), n)] if fresh else there
        return remote(src, there, sem, x_rs.at[b], cross)

    @pl.when(c == 0)
    def _():
        across(0, first_ss.at[0], True).start()

    @pl.when(c == 1)
    def _():
        across(1, first_ss.at[0], True).start()

    def rest(load_sem, near_ss, near_rs, x_ss, half_ss, half_rs, far_ss, far_rs):
        def own(i):
            at = (1 - c if i == 0 else c) * (B // 2)
            here = xs.at[rows(me, at, B // 2)]
            src = here if i else x_ref.at[pl.ds(pl.multiple_of(at, B // 2), B // 2)]
            return remote(src, here, near_ss.at[i], near_rs.at[1] if i else own_rs.at[0], peer)

        def came(b):
            return xs.at[rows(2 * (1 - p) + b, c * (B // 2), B // 2)]

        def passed(b):
            return remote(came(b), came(b), near_ss.at[2 + b], near_rs.at[2 + b], peer)

        def load(i, src, dst):
            return pltpu.make_async_copy(src, dst, load_sem.at[i])

        loads = [load(0, x_ref, xs.at[rows(me)]), load(1, gain_ref, gain_s), load(2, turn_ref, turn_s),
                 load(3, wk_ref, wk_s), load(4, wv_ref, wv_s), load(5, wq_ref, wq_s)]
        load_wo = load(0, wo_ref, wo_s)
        @pl.when(p == 0)
        def _():
            pl.semaphore_signal(in_sem, inc=1, device_id={"tp": peer}, device_id_type=MESH)
            own(0).start()

        pl.semaphore_wait(in_sem, 1)

        @pl.when(p == 0)
        def _():
            pl.semaphore_signal(in_sem, inc=1, device_id={"tp": cross}, device_id_type=MESH)

        @pl.when(p == 1)
        def _():
            own(0).start()

        for copy in loads:
            copy.start()
        own(0).wait_recv()
        loads[0].wait()

        @pl.when(c == 0)
        def _():
            across(1, x_ss.at[0]).start()
            across(2, x_ss.at[1]).start()

        @pl.when(c == 1)
        def _():
            across(0, x_ss.at[0]).start()
            across(2, x_ss.at[1]).start()

        own(1).start()
        own(1).wait_recv()
        for copy in loads[1:3]:
            copy.wait()
        load_wo.start()
        wide_s[...] = gain_s[...].astype(F32).reshape(wide_s.shape)
        for g in range(nk // HEAD):
            v_s[g, HEAD:, :] = jnp.ones((v_s.shape[1] - HEAD, v_s.shape[2]), BF16)

        def norm(tb):
            def some(i, _):
                at = pl.ds(pl.multiple_of(tb * B + i * 16, 16), 16)
                wide = xs[at, :].astype(F32)
                scale = lax.rsqrt(jnp.mean(wide * wide, -1, keepdims=True) + 1e-6)
                a_s[pl.ds(pl.multiple_of(i * 16, 16), 16), :] = (wide * scale * wide_s[...]).astype(BF16)

            lax.fori_loop(0, B // 16, some, None)

        def project(tb, first):
            def loaded(i):
                @pl.when(first)
                def _():
                    loads[i].wait()

            here = rows(tb)
            cos, sin = turn_s[here, :HEAD], turn_s[here, HEAD:]

            def turned(t):
                t = t.astype(BF16).astype(F32)
                return (t * cos + pltpu.roll(t, HEAD // 2, 1) * sin).astype(BF16)

            loaded(3)
            k = _dot(a_s[...], wk_s[...])
            for n in range(0, nk, HEAD):
                k_s[here, n : n + HEAD] = turned(k[:, n : n + HEAD])
            loaded(4)
            v = _dot(a_s[...], wv_s[...])
            for g in range(nk // HEAD):
                v_s[g, :HEAD, here] = v[:, g * HEAD : (g + 1) * HEAD].T.astype(BF16)

            def queries(i, _):
                at = pl.multiple_of(i * 512, 512)
                q = _dot(a_s[...], wq_s[:, pl.ds(at, 512)])
                for n in range(0, 512, HEAD):
                    q_s[here, pl.ds(at + n, HEAD)] = turned(q[:, n : n + HEAD])

            loaded(5)
            lax.fori_loop(0, nq // 512, queries, None)

        def attend(tb):
            here = rows(tb)
            e = HEAD**-0.5 * LOG2E
            top_s[...] = jnp.full(top_s.shape, HIDDEN, F32)
            mix_s[...] = jnp.zeros(mix_s.shape, F32)

            def block(j, masked):
                keys = rows(j)
                seen = None
                if masked:
                    seen = lax.broadcasted_iota(jnp.int32, (B, B), 0) <= lax.broadcasted_iota(jnp.int32, (B, B), 1)
                scores = [_dot(k_s[keys, h // group * HEAD : (h // group + 1) * HEAD], q_s[here, h * HEAD : (h + 1) * HEAD], 1, 1) for h in range(heads)]
                weights, keeps = [], []
                for h, s in enumerate(scores):
                    if masked:
                        s = jnp.where(seen, s, HIDDEN)
                    old = top_s[h : h + 1, :]
                    top = jnp.maximum(old, s.max(axis=0, keepdims=True))
                    top_s[h : h + 1, :] = top
                    weights.append(jnp.exp2((s - top) * e).astype(BF16))
                    keeps.append(jnp.exp2((old - top) * e))
                for h in range(heads):
                    mix_s[h] = mix_s[h] * keeps[h] + _dot(v_s[h // group, :, keys], weights[h])

            lax.fori_loop(0, tb, lambda j, _: block(j, False), None)
            block(tb, True)
            for h in range(heads):
                out = mix_s[h, :HEAD, :] * (1 / mix_s[h, HEAD : HEAD + 1, :])
                q_s[here, h * HEAD : (h + 1) * HEAD] = out.T.astype(BF16)

        def columns(side, t):
            return pl.ds(pl.multiple_of(side * TILES[MAIN][1] + TILES[t][0], HEAD), TILES[t][1])

        def part(tb, side, t):
            return _dot(q_s[rows(tb), :], wo_s[:, columns(side, t)])

        def at_tile(t):
            return pl.ds(*TILES[t])

        def to_peer(b, t):
            return remote(peer_out.at[b, :, at_tile(t)], peer_in.at[b, :, at_tile(t)], half_ss.at[t], half_rs.at[t], peer)

        def to_far(b, t):
            side = c if t == MAIN else 1
            return remote(peer_in.at[b, :, at_tile(t)], far_in.at[:, columns(side, t)], far_ss.at[b * 3 + t - MAIN], far_rs.at[side + t - MAIN], 2 * (1 - p) + b)

        def to_owner(side, t):
            i = 4 if t == REST else side * 2 + t
            return remote(peer_out.at[side, :, at_tile(t)], term_in.at[:, columns(side, t)], near_ss.at[i], near_rs.at[i], peer)

        def far(tb, b):
            def give(t):
                peer_out[b, :, at_tile(t)] = part(tb, 1 if t == REST else 1 - c, t).astype(BF16)

                @pl.when(b == 1)
                def _():
                    to_peer(0, t).wait_send()

                to_peer(b, t).start()

            def add(t):
                term = part(tb, 1 if t == REST else c, t)
                to_peer(b, t).wait_recv()
                peer_in[b, :, at_tile(t)] = (term + peer_in[b, :, at_tile(t)].astype(F32)).astype(BF16)

            for t in range(2):
                give(t)
            for t in range(2):
                add(t)
            to_far(b, MAIN).start()

            @pl.when(c == 0)
            def _():
                give(REST)

            @pl.when(c == 1)
            def _():
                add(REST)
                to_far(b, LATE).start()
                to_far(b, LAST).start()

        def near(tb):
            def give(side, t):
                peer_out[side, :, at_tile(t)] = part(tb, side, t).astype(BF16)
                to_owner(side, t).start()

            def both(side, _):
                for t in range(2):
                    give(side, t)

            for t in range(2):
                to_peer(1, t).wait_send()
                own(t).wait_send()

            @pl.when(c == 0)
            def _():
                to_peer(1, REST).wait_send()

            for b in range(2):
                passed(b).wait_send()
            lax.fori_loop(0, 2, both, None)
            give(1, REST)

        def mine(tb):
            def keep(side, t):
                acc_s[:, columns(side, t)] = xs[rows(tb), columns(side, t)].astype(F32) + part(tb, side, t)

            def both(side, _):
                for t in range(2):
                    keep(side, t)

            lax.fori_loop(0, 2, both, None)
            keep(1, REST)

        def step(it, _):
            b = it - 2
            away = (it >= 2) & (it < 4)
            tb = jnp.where(it < 4, lax.rem(2 * p + it, 4), 2 * p + lax.rem(it + 1 + c, 2))

            @pl.when(away)
            def _():
                remote(came(b), came(b), x_ss.at[0], x_rs.at[b], cross).wait_recv()
                passed(b).start()
                passed(b).wait_recv()

            @pl.when(it < 4)
            def _():
                norm(tb)
                project(tb, it == 0)

            @pl.when(it == 2)
            def _():
                load_wo.wait()

            @pl.when(it >= 2)
            def _():
                attend(tb)

            @pl.when(away)
            def _():
                far(tb, b)

            @pl.when(it == 4)
            def _():
                near(tb)

            @pl.when(it == 5)
            def _():
                mine(tb)

        lax.fori_loop(0, 6, step, None)

        def finish(side, t):
            here = columns(side, t)
            far_in[:, here] = (acc_s[:, here] + term_in[:, here].astype(F32) + far_in[:, here].astype(F32)).astype(BF16)

        def sums(side, t):
            return remote(peer_in.at[0, :, at_tile(t)], far_in.at[:, columns(side, t)], far_ss.at[t - MAIN], far_rs.at[side + t - MAIN], cross)

        def main(side, _):
            sums(side, MAIN).wait_recv()
            for t in range(2):
                to_owner(side, t).wait_recv()
                finish(side, t)

        lax.fori_loop(0, 2, main, None)
        to_owner(1, REST).wait_recv()

        for i in range(2):
            to_far(i, MAIN).wait_send()
            for t in range(2):
                to_owner(i, t).wait_send()
        to_owner(1, REST).wait_send()
        across(2, x_ss.at[1]).wait_send()

        @pl.when(c == 0)
        def _():
            across(0, first_ss.at[0]).wait_send()
            across(1, x_ss.at[0]).wait_send()

        @pl.when(c == 1)
        def _():
            across(1, first_ss.at[0]).wait_send()
            across(0, x_ss.at[0]).wait_send()
            to_far(0, LATE).wait_send()
            to_far(0, LAST).wait_send()

        for t in (LATE, LAST):
            sums(1, t).wait_recv()
            finish(1, t)

        @pl.when(c == 1)
        def _():
            to_far(1, LATE).wait_send()
            to_far(1, LAST).wait_send()

    dma = pltpu.SemaphoreType.DMA
    near = dma((5,))
    pl.run_scoped(rest, dma((6,)), near, near, dma((2,)), dma((3,)), dma((3,)), dma((6,)), dma((4,)))


def _table(tokens):
    half = HEAD // 2
    angle = np.arange(tokens)[:, None] * float(THETA) ** (-np.arange(half) / half)
    cos, sin = np.cos(angle), np.sin(angle)
    return np.concatenate([cos, cos, -sin, sin], 1).astype(np.float32)


def solution(mesh):
    def step(x, gain, wq, wk, wv, wo):
        n, d = x.shape
        tokens = 4 * n
        nq, nk = wq.shape[1], wk.shape[1]
        side = TILES[REST][0] + TILES[REST][1]
        vmem, dma = pltpu.VMEM, pltpu.SemaphoreType.DMA
        return pl.pallas_call(
            _layer,
            out_shape=pltpu.VMEM((n, d), BF16),
            in_specs=[pl.BlockSpec(memory_space=pltpu.HBM)] * 7,
            out_specs=pl.BlockSpec(memory_space=pltpu.VMEM),
            scratch_shapes=[
                vmem((tokens, d), BF16), vmem((n, d), BF16), vmem((d,), BF16), vmem((1, d), F32), vmem((tokens, 2 * HEAD), F32),
                vmem(wq.shape, BF16), vmem(wk.shape, BF16), vmem(wv.shape, BF16), vmem(wo.shape, BF16),
                vmem((tokens, nq), BF16), vmem((tokens, nk), BF16), vmem((nk // HEAD, HEAD + 16, tokens), BF16),
                vmem((nq // HEAD, n), F32), vmem((nq // HEAD, HEAD + 16, n), F32),
                vmem((2, n, side), BF16), vmem((2, n, side), BF16), vmem((n, d), BF16), vmem((n, d), F32),
                dma((1,)), dma((1,)), dma((2,)), pltpu.SemaphoreType.REGULAR,
            ],
            compiler_params=pltpu.CompilerParams(collective_id=0, has_side_effects=True, vmem_limit_bytes=VMEM),
        )(x, gain, _table(tokens), wq, wk, wv, wo)

    tokens, columns = P(("dp", "tp"), None), P(None, "tp")
    return jax.shard_map(
        step,
        mesh=mesh,
        in_specs=(tokens, P(None), columns, columns, columns, P("tp", None)),
        out_specs=tokens,
        check_vma=False,
    )
```

```python
import functools

import jax
import jax.numpy as jnp
import numpy as np
from jax import lax
from jax.experimental import pallas as pl
from jax.experimental.pallas import tpu as pltpu
from jax.sharding import PartitionSpec as P

HEAD = 128
THETA = 10000
HIDDEN = -float("inf")
LOG2E = 1.4426950408889634
VMEM = 67043328 - 2560 * 1024
MESH = pl.DeviceIdType.MESH
F32, BF16 = jnp.float32, jnp.bfloat16

B = 256
PIECES = ((0, 0, 128), (1, 0, 16), (1, 16, 112))
TILES = ((0, 1024), (1024, 1024), (2048, 512), (2048, 384), (2432, 128))
REST, LATE, LAST = 2, 3, 4


def _dot(a, b, ca=1, cb=0):
    return lax.dot_general(a, b, (((ca,), (cb,)), ((), ())), preferred_element_type=F32)


def _layer(x_ref, gain_ref, turn_ref, wq_ref, wk_ref, wv_ref, wo_ref, far_in,
           xs, a_s, gain_s, wide_s, turn_s, wq_s, wk_s, wv_s, wo_s, q_s, k_s, v_s, top_s, mix_s,
           peer_out, peer_in, term_in, acc_s,
           first_ss, own_rs, x_rs, in_sem):
    nq, nk = wq_s.shape[1], wk_s.shape[1]
    heads, group = nq // HEAD, nq // nk
    me = lax.axis_index("tp")
    p, c = lax.div(me, 2), lax.rem(me, 2)
    peer, cross = 2 * p + 1 - c, 2 * (1 - p) + c

    def rows(block, at=0, n=B):
        return pl.ds(pl.multiple_of(block * B + at, 16), n)

    def remote(src, dst, send, recv, to):
        return pltpu.make_async_remote_copy(src_ref=src, dst_ref=dst, send_sem=send, recv_sem=recv, device_id={"tp": to}, device_id_type=MESH)

    barrier = pltpu.get_barrier_semaphore()
    pl.semaphore_signal(barrier, inc=1, device_id={"tp": cross}, device_id_type=MESH)

    @pl.when(p == 0)
    def _():
        pl.semaphore_signal(barrier, inc=1, device_id={"tp": peer}, device_id_type=MESH)

    pl.semaphore_wait(barrier, 2 - p)

    def across(i, sem, fresh=False):
        b, at, n = PIECES[i]
        at = c * (B // 2) + at
        there = xs.at[rows(2 * p + b, at, n)]
        src = x_ref.at[pl.ds(pl.multiple_of(at, 16), n)] if fresh else there
        return remote(src, there, sem, x_rs.at[b], cross)

    @pl.when(c == 0)
    def _():
        across(0, first_ss.at[0], True).start()

    @pl.when(c == 1)
    def _():
        across(1, first_ss.at[0], True).start()

    def rest(load_sem, near_ss, near_rs, x_ss, half_ss, half_rs, far_ss, far_rs):
        def own(i):
            at = (1 - c if i == 0 else c) * (B // 2)
            here = xs.at[rows(me, at, B // 2)]
            src = here if i else x_ref.at[pl.ds(pl.multiple_of(at, B // 2), B // 2)]
            return remote(src, here, near_ss.at[i], near_rs.at[1] if i else own_rs.at[0], peer)

        def came(b):
            return xs.at[rows(2 * (1 - p) + b, c * (B // 2), B // 2)]

        def passed(b):
            return remote(came(b), came(b), near_ss.at[2 + b], near_rs.at[2 + b], peer)

        def load(i, src, dst):
            return pltpu.make_async_copy(src, dst, load_sem.at[i])

        loads = [load(0, x_ref, xs.at[rows(me)]), load(1, gain_ref, gain_s), load(2, turn_ref, turn_s),
                 load(3, wk_ref, wk_s), load(4, wv_ref, wv_s), load(5, wq_ref, wq_s)]
        load_wo = load(0, wo_ref, wo_s)
        @pl.when(p == 0)
        def _():
            pl.semaphore_signal(in_sem, inc=1, device_id={"tp": peer}, device_id_type=MESH)
            own(0).start()

        pl.semaphore_wait(in_sem, 1)

        @pl.when(p == 0)
        def _():
            pl.semaphore_signal(in_sem, inc=1, device_id={"tp": cross}, device_id_type=MESH)

        @pl.when(p == 1)
        def _():
            own(0).start()

        for copy in loads:
            copy.start()
        own(0).wait_recv()
        loads[0].wait()

        @pl.when(c == 0)
        def _():
            across(1, x_ss.at[0]).start()
            across(2, x_ss.at[1]).start()

        @pl.when(c == 1)
        def _():
            across(0, x_ss.at[0]).start()
            across(2, x_ss.at[1]).start()

        own(1).start()
        own(1).wait_recv()
        for copy in loads[1:3]:
            copy.wait()
        load_wo.start()
        wide_s[...] = gain_s[...].astype(F32).reshape(wide_s.shape)
        for g in range(nk // HEAD):
            v_s[g, HEAD:, :] = jnp.ones((v_s.shape[1] - HEAD, v_s.shape[2]), BF16)

        def norm(tb):
            def some(i, _):
                at = pl.ds(pl.multiple_of(tb * B + i * 16, 16), 16)
                wide = xs[at, :].astype(F32)
                scale = lax.rsqrt(jnp.mean(wide * wide, -1, keepdims=True) + 1e-6)
                a_s[pl.ds(pl.multiple_of(i * 16, 16), 16), :] = (wide * scale * wide_s[...]).astype(BF16)

            lax.fori_loop(0, B // 16, some, None)

        def project(tb, first):
            def loaded(i):
                @pl.when(first)
                def _():
                    loads[i].wait()

            here = rows(tb)
            cos, sin = turn_s[here, :HEAD], turn_s[here, HEAD:]

            def turned(t):
                t = t.astype(BF16).astype(F32)
                return (t * cos + pltpu.roll(t, HEAD // 2, 1) * sin).astype(BF16)

            loaded(3)
            k = _dot(a_s[...], wk_s[...])
            for n in range(0, nk, HEAD):
                k_s[here, n : n + HEAD] = turned(k[:, n : n + HEAD])
            loaded(4)
            v = _dot(a_s[...], wv_s[...])
            for g in range(nk // HEAD):
                v_s[g, :HEAD, here] = v[:, g * HEAD : (g + 1) * HEAD].T.astype(BF16)

            def queries(i, _):
                at = pl.multiple_of(i * 512, 512)
                q = _dot(a_s[...], wq_s[:, pl.ds(at, 512)])
                for n in range(0, 512, HEAD):
                    q_s[here, pl.ds(at + n, HEAD)] = turned(q[:, n : n + HEAD])

            loaded(5)
            lax.fori_loop(0, nq // 512, queries, None)

        def attend(tb):
            here = rows(tb)
            e = HEAD**-0.5 * LOG2E
            top_s[...] = jnp.full(top_s.shape, HIDDEN, F32)
            mix_s[...] = jnp.zeros(mix_s.shape, F32)

            def block(j, masked):
                keys = rows(j)
                seen = None
                if masked:
                    seen = lax.broadcasted_iota(jnp.int32, (B, B), 0) <= lax.broadcasted_iota(jnp.int32, (B, B), 1)
                scores = [_dot(k_s[keys, h // group * HEAD : (h // group + 1) * HEAD], q_s[here, h * HEAD : (h + 1) * HEAD], 1, 1) for h in range(heads)]
                weights, keeps = [], []
                for h, s in enumerate(scores):
                    if masked:
                        s = jnp.where(seen, s, HIDDEN)
                    old = top_s[h : h + 1, :]
                    top = jnp.maximum(old, s.max(axis=0, keepdims=True))
                    top_s[h : h + 1, :] = top
                    weights.append(jnp.exp2((s - top) * e).astype(BF16))
                    keeps.append(jnp.exp2((old - top) * e))
                for h in range(heads):
                    mix_s[h] = mix_s[h] * keeps[h] + _dot(v_s[h // group, :, keys], weights[h])

            lax.fori_loop(0, tb, lambda j, _: block(j, False), None)
            block(tb, True)
            for h in range(heads):
                out = mix_s[h, :HEAD, :] * (1 / mix_s[h, HEAD : HEAD + 1, :])
                q_s[here, h * HEAD : (h + 1) * HEAD] = out.T.astype(BF16)

        def columns(side, t):
            return pl.ds(pl.multiple_of(side * TILES[REST][0] + TILES[t][0], HEAD), TILES[t][1])

        def part(tb, side, t):
            return _dot(q_s[rows(tb), :], wo_s[:, columns(side, t)])

        def at_tile(t):
            return pl.ds(*TILES[t])

        def to_peer(b, t):
            return remote(peer_out.at[b, :, at_tile(t)], peer_in.at[b, :, at_tile(t)], half_ss.at[t], half_rs.at[t], peer)

        def came_at(side, t):
            return side * 2 + t if t < REST else t + 1

        def to_far(b, t):
            side = c if t < REST else 1
            return remote(peer_in.at[b, :, at_tile(t)], far_in.at[:, columns(side, t)], far_ss.at[b * 5 + t], far_rs.at[came_at(side, t)], 2 * (1 - p) + b)

        def to_owner(side, t):
            i = 4 if t == REST else side * 2 + t
            return remote(peer_out.at[side, :, at_tile(t)], term_in.at[:, columns(side, t)], near_ss.at[i], near_rs.at[i], peer)

        def far(tb, b):
            def give(t):
                peer_out[b, :, at_tile(t)] = part(tb, 1 if t == REST else 1 - c, t).astype(BF16)

                @pl.when(b == 1)
                def _():
                    to_peer(0, t).wait_send()

                to_peer(b, t).start()

            def add(t):
                term = part(tb, 1 if t == REST else c, t)
                to_peer(b, t).wait_recv()
                peer_in[b, :, at_tile(t)] = (term + peer_in[b, :, at_tile(t)].astype(F32)).astype(BF16)

            for t in range(2):
                give(t)
            for t in range(2):
                add(t)
                to_far(b, t).start()

            @pl.when(c == 0)
            def _():
                give(REST)

            @pl.when(c == 1)
            def _():
                add(REST)
                to_far(b, LATE).start()
                to_far(b, LAST).start()

        def near(tb):
            def give(side, t):
                peer_out[side, :, at_tile(t)] = part(tb, side, t).astype(BF16)
                to_owner(side, t).start()

            def both(side, _):
                for t in range(2):
                    give(side, t)

            for t in range(2):
                to_peer(1, t).wait_send()
                own(t).wait_send()

            @pl.when(c == 0)
            def _():
                to_peer(1, REST).wait_send()

            for b in range(2):
                passed(b).wait_send()
            lax.fori_loop(0, 2, both, None)
            give(1, REST)

        def mine(tb):
            def keep(side, t):
                acc_s[:, columns(side, t)] = xs[rows(tb), columns(side, t)].astype(F32) + part(tb, side, t)

            def both(side, _):
                for t in range(2):
                    keep(side, t)

            lax.fori_loop(0, 2, both, None)
            keep(1, REST)

        def step(it, _):
            b = it - 2
            away = (it >= 2) & (it < 4)
            tb = jnp.where(it < 4, lax.rem(2 * p + it, 4), 2 * p + lax.rem(it + 1 + c, 2))

            @pl.when(away)
            def _():
                remote(came(b), came(b), x_ss.at[0], x_rs.at[b], cross).wait_recv()
                passed(b).start()
                passed(b).wait_recv()

            @pl.when(it < 4)
            def _():
                norm(tb)
                project(tb, it == 0)

            @pl.when(it == 2)
            def _():
                load_wo.wait()

            @pl.when(it >= 2)
            def _():
                attend(tb)

            @pl.when(away)
            def _():
                far(tb, b)

            @pl.when(it == 4)
            def _():
                near(tb)

            @pl.when(it == 5)
            def _():
                mine(tb)

        lax.fori_loop(0, 6, step, None)

        def finish(side, t):
            here = columns(side, t)
            far_in[:, here] = (acc_s[:, here] + term_in[:, here].astype(F32) + far_in[:, here].astype(F32)).astype(BF16)

        def sums(side, t):
            return remote(peer_in.at[0, :, at_tile(t)], far_in.at[:, columns(side, t)], far_ss.at[t], far_rs.at[came_at(side, t)], cross)

        def main(side, _):
            for t in range(2):
                sums(side, t).wait_recv()
                to_owner(side, t).wait_recv()
                finish(side, t)

        lax.fori_loop(0, 2, main, None)
        to_owner(1, REST).wait_recv()

        for i in range(2):
            for t in range(2):
                to_far(i, t).wait_send()
                to_owner(i, t).wait_send()
        to_owner(1, REST).wait_send()
        across(2, x_ss.at[1]).wait_send()

        @pl.when(c == 0)
        def _():
            across(0, first_ss.at[0]).wait_send()
            across(1, x_ss.at[0]).wait_send()

        @pl.when(c == 1)
        def _():
            across(1, first_ss.at[0]).wait_send()
            across(0, x_ss.at[0]).wait_send()
            to_far(0, LATE).wait_send()
            to_far(0, LAST).wait_send()

        for t in (LATE, LAST):
            sums(1, t).wait_recv()
            finish(1, t)

        @pl.when(c == 1)
        def _():
            to_far(1, LATE).wait_send()
            to_far(1, LAST).wait_send()

    dma = pltpu.SemaphoreType.DMA
    near = dma((5,))
    pl.run_scoped(rest, dma((6,)), near, near, dma((2,)), dma((3,)), dma((3,)), dma((10,)), dma((6,)))


def _table(tokens):
    half = HEAD // 2
    angle = np.arange(tokens)[:, None] * float(THETA) ** (-np.arange(half) / half)
    cos, sin = np.cos(angle), np.sin(angle)
    return np.concatenate([cos, cos, -sin, sin], 1).astype(np.float32)


def solution(mesh):
    def step(x, gain, wq, wk, wv, wo):
        n, d = x.shape
        tokens = 4 * n
        nq, nk = wq.shape[1], wk.shape[1]
        side = TILES[REST][0] + TILES[REST][1]
        vmem, dma = pltpu.VMEM, pltpu.SemaphoreType.DMA
        return pl.pallas_call(
            _layer,
            out_shape=pltpu.VMEM((n, d), BF16),
            in_specs=[pl.BlockSpec(memory_space=pltpu.HBM)] * 7,
            out_specs=pl.BlockSpec(memory_space=pltpu.VMEM),
            scratch_shapes=[
                vmem((tokens, d), BF16), vmem((n, d), BF16), vmem((d,), BF16), vmem((1, d), F32), vmem((tokens, 2 * HEAD), F32),
                vmem(wq.shape, BF16), vmem(wk.shape, BF16), vmem(wv.shape, BF16), vmem(wo.shape, BF16),
                vmem((tokens, nq), BF16), vmem((tokens, nk), BF16), vmem((nk // HEAD, HEAD + 16, tokens), BF16),
                vmem((nq // HEAD, n), F32), vmem((nq // HEAD, HEAD + 16, n), F32),
                vmem((2, n, side), BF16), vmem((2, n, side), BF16), vmem((n, d), BF16), vmem((n, d), F32),
                dma((1,)), dma((1,)), dma((2,)), pltpu.SemaphoreType.REGULAR,
            ],
            compiler_params=pltpu.CompilerParams(collective_id=0, has_side_effects=True, vmem_limit_bytes=VMEM),
        )(x, gain, _table(tokens), wq, wk, wv, wo)

    tokens, columns = P(("dp", "tp"), None), P(None, "tp")
    return jax.shard_map(
        step,
        mesh=mesh,
        in_specs=(tokens, P(None), columns, columns, columns, P("tp", None)),
        out_specs=tokens,
        check_vma=False,
    )
```

```python
import functools

import jax
import jax.numpy as jnp
import numpy as np
from jax import lax
from jax.experimental import pallas as pl
from jax.experimental.pallas import tpu as pltpu
from jax.sharding import PartitionSpec as P

HEAD = 128
THETA = 10000
HIDDEN = -float("inf")
LOG2E = 1.4426950408889634
VMEM = 67043328 - 2560 * 1024
MESH = pl.DeviceIdType.MESH
F32, BF16 = jnp.float32, jnp.bfloat16

B = 256
PIECES = ((0, 0, 128), (1, 0, 16), (1, 16, 112))
TILES = ((0, 1024), (1024, 1024), (2048, 512), (2048, 384), (2432, 128))
REST, LATE, LAST = 2, 3, 4


def _dot(a, b, ca=1, cb=0):
    return lax.dot_general(a, b, (((ca,), (cb,)), ((), ())), preferred_element_type=F32)


def _layer(x_ref, gain_ref, turn_ref, wq_ref, wk_ref, wv_ref, wo_ref, far_in,
           xs, a_s, gain_s, wide_s, turn_s, wq_s, wk_s, wv_s, wo_s, q_s, k_s, v_s, top_s, mix_s,
           peer_out, peer_in, term_in, acc_s,
           first_ss, own_rs, x_rs, in_sem):
    nq, nk = wq_s.shape[1], wk_s.shape[1]
    heads, group = nq // HEAD, nq // nk
    me = lax.axis_index("tp")
    p, c = lax.div(me, 2), lax.rem(me, 2)
    peer, cross = 2 * p + 1 - c, 2 * (1 - p) + c

    def rows(block, at=0, n=B):
        return pl.ds(pl.multiple_of(block * B + at, 16), n)

    def remote(src, dst, send, recv, to):
        return pltpu.make_async_remote_copy(src_ref=src, dst_ref=dst, send_sem=send, recv_sem=recv, device_id={"tp": to}, device_id_type=MESH)

    barrier = pltpu.get_barrier_semaphore()
    pl.semaphore_signal(barrier, inc=1, device_id={"tp": cross}, device_id_type=MESH)

    @pl.when(p == 0)
    def _():
        pl.semaphore_signal(barrier, inc=1, device_id={"tp": peer}, device_id_type=MESH)

    pl.semaphore_wait(barrier, 2 - p)

    def across(i, sem, fresh=False):
        b, at, n = PIECES[i]
        at = c * (B // 2) + at
        there = xs.at[rows(2 * p + b, at, n)]
        src = x_ref.at[pl.ds(pl.multiple_of(at, 16), n)] if fresh else there
        return remote(src, there, sem, x_rs.at[b], cross)

    @pl.when(c == 0)
    def _():
        across(0, first_ss.at[0], True).start()

    @pl.when(c == 1)
    def _():
        across(1, first_ss.at[0], True).start()

    def rest(load_sem, near_ss, near_rs, x_ss, half_ss, half_rs, far_ss, far_rs):
        def own(i):
            at = (1 - c if i == 0 else c) * (B // 2)
            here = xs.at[rows(me, at, B // 2)]
            src = here if i else x_ref.at[pl.ds(pl.multiple_of(at, B // 2), B // 2)]
            return remote(src, here, near_ss.at[i], near_rs.at[1] if i else own_rs.at[0], peer)

        def came(b):
            return xs.at[rows(2 * (1 - p) + b, c * (B // 2), B // 2)]

        def passed(b):
            return remote(came(b), came(b), near_ss.at[2 + b], near_rs.at[2 + b], peer)

        def load(i, src, dst):
            return pltpu.make_async_copy(src, dst, load_sem.at[i])

        loads = [load(0, x_ref, xs.at[rows(me)]), load(1, gain_ref, gain_s), load(2, turn_ref, turn_s),
                 load(3, wk_ref, wk_s), load(4, wv_ref, wv_s), load(5, wq_ref, wq_s)]
        load_wo = load(0, wo_ref, wo_s)
        @pl.when(p == 0)
        def _():
            pl.semaphore_signal(in_sem, inc=1, device_id={"tp": peer}, device_id_type=MESH)
            own(0).start()

        pl.semaphore_wait(in_sem, 1)

        @pl.when(p == 0)
        def _():
            pl.semaphore_signal(in_sem, inc=1, device_id={"tp": cross}, device_id_type=MESH)

        @pl.when(p == 1)
        def _():
            own(0).start()

        for copy in loads:
            copy.start()
        own(0).wait_recv()
        loads[0].wait()

        @pl.when(c == 0)
        def _():
            across(1, x_ss.at[0]).start()
            across(2, x_ss.at[1]).start()

        @pl.when(c == 1)
        def _():
            across(0, x_ss.at[0]).start()
            across(2, x_ss.at[1]).start()

        own(1).start()
        own(1).wait_recv()
        for copy in loads[1:3]:
            copy.wait()
        load_wo.start()
        wide_s[...] = gain_s[...].astype(F32).reshape(wide_s.shape)
        for g in range(nk // HEAD):
            v_s[g, HEAD:, :] = jnp.ones((v_s.shape[1] - HEAD, v_s.shape[2]), BF16)

        def norm(tb):
            def some(i, _):
                at = pl.ds(pl.multiple_of(tb * B + i * 16, 16), 16)
                wide = xs[at, :].astype(F32)
                scale = lax.rsqrt(jnp.mean(wide * wide, -1, keepdims=True) + 1e-6)
                a_s[pl.ds(pl.multiple_of(i * 16, 16), 16), :] = (wide * scale * wide_s[...]).astype(BF16)

            lax.fori_loop(0, B // 16, some, None)

        def project(tb, first):
            def loaded(i):
                @pl.when(first)
                def _():
                    loads[i].wait()

            here = rows(tb)
            cos, sin = turn_s[here, :HEAD], turn_s[here, HEAD:]

            def turned(t):
                t = t.astype(BF16).astype(F32)
                return (t * cos + pltpu.roll(t, HEAD // 2, 1) * sin).astype(BF16)

            loaded(3)
            k = _dot(a_s[...], wk_s[...])
            for n in range(0, nk, HEAD):
                k_s[here, n : n + HEAD] = turned(k[:, n : n + HEAD])
            loaded(4)
            v = _dot(a_s[...], wv_s[...])
            for g in range(nk // HEAD):
                v_s[g, :HEAD, here] = v[:, g * HEAD : (g + 1) * HEAD].T.astype(BF16)

            def queries(i, _):
                at = pl.multiple_of(i * 512, 512)
                q = _dot(a_s[...], wq_s[:, pl.ds(at, 512)])
                for n in range(0, 512, HEAD):
                    q_s[here, pl.ds(at + n, HEAD)] = turned(q[:, n : n + HEAD])

            loaded(5)
            lax.fori_loop(0, nq // 512, queries, None)

        def attend(tb):
            here = rows(tb)
            e = HEAD**-0.5 * LOG2E
            top_s[...] = jnp.full(top_s.shape, HIDDEN, F32)
            mix_s[...] = jnp.zeros(mix_s.shape, F32)

            def block(j, masked):
                keys = rows(j)
                seen = None
                if masked:
                    seen = lax.broadcasted_iota(jnp.int32, (B, B), 0) <= lax.broadcasted_iota(jnp.int32, (B, B), 1)
                scores = [_dot(k_s[keys, h // group * HEAD : (h // group + 1) * HEAD], q_s[here, h * HEAD : (h + 1) * HEAD], 1, 1) for h in range(heads)]
                weights, keeps = [], []
                for h, s in enumerate(scores):
                    if masked:
                        s = jnp.where(seen, s, HIDDEN)
                    old = top_s[h : h + 1, :]
                    top = jnp.maximum(old, s.max(axis=0, keepdims=True))
                    top_s[h : h + 1, :] = top
                    weights.append(jnp.exp2((s - top) * e).astype(BF16))
                    keeps.append(jnp.exp2((old - top) * e))
                for h in range(heads):
                    mix_s[h] = mix_s[h] * keeps[h] + _dot(v_s[h // group, :, keys], weights[h])

            lax.fori_loop(0, tb, lambda j, _: block(j, False), None)
            block(tb, True)
            for h in range(heads):
                out = mix_s[h, :HEAD, :] * (1 / mix_s[h, HEAD : HEAD + 1, :])
                q_s[here, h * HEAD : (h + 1) * HEAD] = out.T.astype(BF16)

        def columns(side, t):
            return pl.ds(pl.multiple_of(side * TILES[REST][0] + TILES[t][0], HEAD), TILES[t][1])

        def part(tb, side, t):
            return _dot(q_s[rows(tb), :], wo_s[:, columns(side, t)])

        def at_tile(t):
            return pl.ds(*TILES[t])

        def to_peer(b, t):
            return remote(peer_out.at[b, :, at_tile(t)], peer_in.at[b, :, at_tile(t)], half_ss.at[t], half_rs.at[t], peer)

        def came_at(side, t):
            return side * 2 + t if t < REST else t + 1

        def to_far(b, t):
            side = c if t < REST else 1
            return remote(peer_in.at[b, :, at_tile(t)], far_in.at[:, columns(side, t)], far_ss.at[b * 5 + t], far_rs.at[came_at(side, t)], 2 * (1 - p) + b)

        def to_owner(side, t):
            i = 4 if t == REST else side * 2 + t
            return remote(peer_out.at[side, :, at_tile(t)], term_in.at[:, columns(side, t)], near_ss.at[i], near_rs.at[i], peer)

        def far(tb, b):
            def give(t):
                peer_out[b, :, at_tile(t)] = part(tb, 1 if t == REST else 1 - c, t).astype(BF16)

                @pl.when(b == 1)
                def _():
                    to_peer(0, t).wait_send()

                to_peer(b, t).start()

            def add(t):
                term = part(tb, 1 if t == REST else c, t)
                to_peer(b, t).wait_recv()
                peer_in[b, :, at_tile(t)] = (term + peer_in[b, :, at_tile(t)].astype(F32)).astype(BF16)

            for t in range(2):
                give(t)
            for t in range(2):
                add(t)
                to_far(b, t).start()

            @pl.when(c == 0)
            def _():
                give(REST)

            @pl.when(c == 1)
            def _():
                add(REST)
                to_far(b, LATE).start()
                to_far(b, LAST).start()

        def near(tb):
            def give(side, t):
                peer_out[side, :, at_tile(t)] = part(tb, side, t).astype(BF16)
                to_owner(side, t).start()

            def both(side, _):
                for t in range(2):
                    give(side, t)

            for t in range(2):
                to_peer(1, t).wait_send()
                own(t).wait_send()

            @pl.when(c == 0)
            def _():
                to_peer(1, REST).wait_send()

            for b in range(2):
                passed(b).wait_send()
            lax.fori_loop(0, 2, both, None)
            give(1, REST)

        def mine(tb):
            def keep(side, t):
                acc_s[:, columns(side, t)] = xs[rows(tb), columns(side, t)].astype(F32) + part(tb, side, t)

            def both(side, _):
                for t in range(2):
                    keep(side, t)

            lax.fori_loop(0, 2, both, None)
            keep(1, REST)

        def step(it, _):
            b = it - 2
            away = (it >= 2) & (it < 4)
            tb = jnp.where(it < 4, lax.rem(2 * p + it, 4), 2 * p + lax.rem(it + 1 + c, 2))

            @pl.when(away)
            def _():
                remote(came(b), came(b), x_ss.at[0], x_rs.at[b], cross).wait_recv()
                passed(b).start()
                passed(b).wait_recv()

            @pl.when(it < 4)
            def _():
                norm(tb)
                project(tb, it == 0)

            @pl.when(it == 2)
            def _():
                load_wo.wait()

            @pl.when(it >= 2)
            def _():
                attend(tb)

            @pl.when(away)
            def _():
                far(tb, b)

            @pl.when(it == 4)
            def _():
                near(tb)

            @pl.when(it == 5)
            def _():
                mine(tb)

        lax.fori_loop(0, 6, step, None)

        def finish(side, t):
            here = columns(side, t)
            far_in[:, here] = (acc_s[:, here] + term_in[:, here].astype(F32) + far_in[:, here].astype(F32)).astype(BF16)

        def sums(side, t):
            return remote(peer_in.at[0, :, at_tile(t)], far_in.at[:, columns(side, t)], far_ss.at[t], far_rs.at[came_at(side, t)], cross)

        def main(side, _):
            for t in range(2):
                sums(side, t).wait_recv()
                to_owner(side, t).wait_recv()
                finish(side, t)

        lax.fori_loop(0, 2, main, None)
        to_owner(1, REST).wait_recv()
        rest_at = columns(1, REST)
        acc_s[:, rest_at] = acc_s[:, rest_at] + term_in[:, rest_at].astype(F32)

        for i in range(2):
            for t in range(2):
                to_far(i, t).wait_send()
                to_owner(i, t).wait_send()
        to_owner(1, REST).wait_send()
        across(2, x_ss.at[1]).wait_send()

        @pl.when(c == 0)
        def _():
            across(0, first_ss.at[0]).wait_send()
            across(1, x_ss.at[0]).wait_send()

        @pl.when(c == 1)
        def _():
            across(1, first_ss.at[0]).wait_send()
            across(0, x_ss.at[0]).wait_send()
            to_far(0, LATE).wait_send()
            to_far(0, LAST).wait_send()

        for t in (LATE, LAST):
            sums(1, t).wait_recv()
            here = columns(1, t)
            far_in[:, here] = (acc_s[:, here] + far_in[:, here].astype(F32)).astype(BF16)

        @pl.when(c == 1)
        def _():
            to_far(1, LATE).wait_send()
            to_far(1, LAST).wait_send()

    dma = pltpu.SemaphoreType.DMA
    near = dma((5,))
    pl.run_scoped(rest, dma((6,)), near, near, dma((2,)), dma((3,)), dma((3,)), dma((10,)), dma((6,)))


def _table(tokens):
    half = HEAD // 2
    angle = np.arange(tokens)[:, None] * float(THETA) ** (-np.arange(half) / half)
    cos, sin = np.cos(angle), np.sin(angle)
    return np.concatenate([cos, cos, -sin, sin], 1).astype(np.float32)


def solution(mesh):
    def step(x, gain, wq, wk, wv, wo):
        n, d = x.shape
        tokens = 4 * n
        nq, nk = wq.shape[1], wk.shape[1]
        side = TILES[REST][0] + TILES[REST][1]
        vmem, dma = pltpu.VMEM, pltpu.SemaphoreType.DMA
        return pl.pallas_call(
            _layer,
            out_shape=pltpu.VMEM((n, d), BF16),
            in_specs=[pl.BlockSpec(memory_space=pltpu.HBM)] * 7,
            out_specs=pl.BlockSpec(memory_space=pltpu.VMEM),
            scratch_shapes=[
                vmem((tokens, d), BF16), vmem((n, d), BF16), vmem((d,), BF16), vmem((1, d), F32), vmem((tokens, 2 * HEAD), F32),
                vmem(wq.shape, BF16), vmem(wk.shape, BF16), vmem(wv.shape, BF16), vmem(wo.shape, BF16),
                vmem((tokens, nq), BF16), vmem((tokens, nk), BF16), vmem((nk // HEAD, HEAD + 16, tokens), BF16),
                vmem((nq // HEAD, n), F32), vmem((nq // HEAD, HEAD + 16, n), F32),
                vmem((2, n, side), BF16), vmem((2, n, side), BF16), vmem((n, d), BF16), vmem((n, d), F32),
                dma((1,)), dma((1,)), dma((2,)), pltpu.SemaphoreType.REGULAR,
            ],
            compiler_params=pltpu.CompilerParams(collective_id=0, has_side_effects=True, vmem_limit_bytes=VMEM),
        )(x, gain, _table(tokens), wq, wk, wv, wo)

    tokens, columns = P(("dp", "tp"), None), P(None, "tp")
    return jax.shard_map(
        step,
        mesh=mesh,
        in_specs=(tokens, P(None), columns, columns, columns, P("tp", None)),
        out_specs=tokens,
        check_vma=False,
    )
```

```python
import functools

import jax
import jax.numpy as jnp
import numpy as np
from jax import lax
from jax.experimental import pallas as pl
from jax.experimental.pallas import tpu as pltpu
from jax.sharding import PartitionSpec as P

HEAD = 128
THETA = 10000
HIDDEN = -float("inf")
LOG2E = 1.4426950408889634
VMEM = 67043328 - 2560 * 1024
MESH = pl.DeviceIdType.MESH
F32, BF16 = jnp.float32, jnp.bfloat16

B = 256
PIECES = ((0, 0, 128), (1, 0, 32), (1, 32, 96))
TILES = ((0, 1024), (1024, 1024), (2048, 512), (2048, 384), (2432, 128))
REST, LATE, LAST = 2, 3, 4


def _dot(a, b, ca=1, cb=0):
    return lax.dot_general(a, b, (((ca,), (cb,)), ((), ())), preferred_element_type=F32)


def _layer(x_ref, gain_ref, turn_ref, wq_ref, wk_ref, wv_ref, wo_ref, far_in,
           xs, a_s, gain_s, wide_s, turn_s, wq_s, wk_s, wv_s, wo_s, q_s, k_s, v_s, top_s, mix_s,
           peer_out, peer_in, term_in, acc_s,
           first_ss, own_rs, x_rs, in_sem):
    nq, nk = wq_s.shape[1], wk_s.shape[1]
    heads, group = nq // HEAD, nq // nk
    me = lax.axis_index("tp")
    p, c = lax.div(me, 2), lax.rem(me, 2)
    peer, cross = 2 * p + 1 - c, 2 * (1 - p) + c

    def rows(block, at=0, n=B):
        return pl.ds(pl.multiple_of(block * B + at, 16), n)

    def remote(src, dst, send, recv, to):
        return pltpu.make_async_remote_copy(src_ref=src, dst_ref=dst, send_sem=send, recv_sem=recv, device_id={"tp": to}, device_id_type=MESH)

    barrier = pltpu.get_barrier_semaphore()
    pl.semaphore_signal(barrier, inc=1, device_id={"tp": cross}, device_id_type=MESH)

    @pl.when(p == 0)
    def _():
        pl.semaphore_signal(barrier, inc=1, device_id={"tp": peer}, device_id_type=MESH)

    pl.semaphore_wait(barrier, 2 - p)

    def across(i, sem, fresh=False):
        b, at, n = PIECES[i]
        at = c * (B // 2) + at
        there = xs.at[rows(2 * p + b, at, n)]
        src = x_ref.at[pl.ds(pl.multiple_of(at, 16), n)] if fresh else there
        return remote(src, there, sem, x_rs.at[b], cross)

    @pl.when(c == 0)
    def _():
        across(0, first_ss.at[0], True).start()

    @pl.when(c == 1)
    def _():
        across(1, first_ss.at[0], True).start()

    def rest(load_sem, near_ss, near_rs, x_ss, half_ss, half_rs, far_ss, far_rs):
        def own(i):
            at = (1 - c if i == 0 else c) * (B // 2)
            here = xs.at[rows(me, at, B // 2)]
            src = here if i else x_ref.at[pl.ds(pl.multiple_of(at, B // 2), B // 2)]
            return remote(src, here, near_ss.at[i], near_rs.at[1] if i else own_rs.at[0], peer)

        def came(b):
            return xs.at[rows(2 * (1 - p) + b, c * (B // 2), B // 2)]

        def passed(b):
            return remote(came(b), came(b), near_ss.at[2 + b], near_rs.at[2 + b], peer)

        def load(i, src, dst):
            return pltpu.make_async_copy(src, dst, load_sem.at[i])

        loads = [load(0, x_ref, xs.at[rows(me)]), load(1, gain_ref, gain_s), load(2, turn_ref, turn_s),
                 load(3, wk_ref, wk_s), load(4, wv_ref, wv_s), load(5, wq_ref, wq_s)]
        load_wo = load(0, wo_ref, wo_s)
        @pl.when(p == 0)
        def _():
            pl.semaphore_signal(in_sem, inc=1, device_id={"tp": peer}, device_id_type=MESH)
            own(0).start()

        pl.semaphore_wait(in_sem, 1)

        @pl.when(p == 0)
        def _():
            pl.semaphore_signal(in_sem, inc=1, device_id={"tp": cross}, device_id_type=MESH)

        @pl.when(p == 1)
        def _():
            own(0).start()

        for copy in loads:
            copy.start()
        own(0).wait_recv()
        loads[0].wait()

        @pl.when(c == 0)
        def _():
            across(1, x_ss.at[0]).start()
            across(2, x_ss.at[1]).start()

        @pl.when(c == 1)
        def _():
            across(0, x_ss.at[0]).start()
            across(2, x_ss.at[1]).start()

        own(1).start()
        own(1).wait_recv()
        for copy in loads[1:3]:
            copy.wait()
        load_wo.start()
        wide_s[...] = gain_s[...].astype(F32).reshape(wide_s.shape)
        for g in range(nk // HEAD):
            v_s[g, HEAD:, :] = jnp.ones((v_s.shape[1] - HEAD, v_s.shape[2]), BF16)

        def norm(tb):
            def some(i, _):
                at = pl.ds(pl.multiple_of(tb * B + i * 16, 16), 16)
                wide = xs[at, :].astype(F32)
                scale = lax.rsqrt(jnp.mean(wide * wide, -1, keepdims=True) + 1e-6)
                a_s[pl.ds(pl.multiple_of(i * 16, 16), 16), :] = (wide * scale * wide_s[...]).astype(BF16)

            lax.fori_loop(0, B // 16, some, None)

        def project(tb, first):
            def loaded(i):
                @pl.when(first)
                def _():
                    loads[i].wait()

            here = rows(tb)
            cos, sin = turn_s[here, :HEAD], turn_s[here, HEAD:]

            def turned(t):
                t = t.astype(BF16).astype(F32)
                return (t * cos + pltpu.roll(t, HEAD // 2, 1) * sin).astype(BF16)

            loaded(3)
            k = _dot(a_s[...], wk_s[...])
            for n in range(0, nk, HEAD):
                k_s[here, n : n + HEAD] = turned(k[:, n : n + HEAD])
            loaded(4)
            v = _dot(a_s[...], wv_s[...])
            for g in range(nk // HEAD):
                v_s[g, :HEAD, here] = v[:, g * HEAD : (g + 1) * HEAD].T.astype(BF16)

            def queries(i, _):
                at = pl.multiple_of(i * 512, 512)
                q = _dot(a_s[...], wq_s[:, pl.ds(at, 512)])
                for n in range(0, 512, HEAD):
                    q_s[here, pl.ds(at + n, HEAD)] = turned(q[:, n : n + HEAD])

            loaded(5)
            lax.fori_loop(0, nq // 512, queries, None)

        def attend(tb):
            here = rows(tb)
            e = HEAD**-0.5 * LOG2E
            top_s[...] = jnp.full(top_s.shape, HIDDEN, F32)
            mix_s[...] = jnp.zeros(mix_s.shape, F32)

            def block(j, masked):
                keys = rows(j)
                seen = None
                if masked:
                    seen = lax.broadcasted_iota(jnp.int32, (B, B), 0) <= lax.broadcasted_iota(jnp.int32, (B, B), 1)
                scores = [_dot(k_s[keys, h // group * HEAD : (h // group + 1) * HEAD], q_s[here, h * HEAD : (h + 1) * HEAD], 1, 1) for h in range(heads)]
                weights, keeps = [], []
                for h, s in enumerate(scores):
                    if masked:
                        s = jnp.where(seen, s, HIDDEN)
                    old = top_s[h : h + 1, :]
                    top = jnp.maximum(old, s.max(axis=0, keepdims=True))
                    top_s[h : h + 1, :] = top
                    weights.append(jnp.exp2((s - top) * e).astype(BF16))
                    keeps.append(jnp.exp2((old - top) * e))
                for h in range(heads):
                    mix_s[h] = mix_s[h] * keeps[h] + _dot(v_s[h // group, :, keys], weights[h])

            lax.fori_loop(0, tb, lambda j, _: block(j, False), None)
            block(tb, True)
            for h in range(heads):
                out = mix_s[h, :HEAD, :] * (1 / mix_s[h, HEAD : HEAD + 1, :])
                q_s[here, h * HEAD : (h + 1) * HEAD] = out.T.astype(BF16)

        def columns(side, t):
            return pl.ds(pl.multiple_of(side * TILES[REST][0] + TILES[t][0], HEAD), TILES[t][1])

        def part(tb, side, t):
            return _dot(q_s[rows(tb), :], wo_s[:, columns(side, t)])

        def at_tile(t):
            return pl.ds(*TILES[t])

        def to_peer(b, t):
            return remote(peer_out.at[b, :, at_tile(t)], peer_in.at[b, :, at_tile(t)], half_ss.at[t], half_rs.at[t], peer)

        def came_at(side, t):
            return side * 2 + t if t < REST else t + 1

        def to_far(b, t):
            side = c if t < REST else 1
            return remote(peer_in.at[b, :, at_tile(t)], far_in.at[:, columns(side, t)], far_ss.at[b * 5 + t], far_rs.at[came_at(side, t)], 2 * (1 - p) + b)

        def to_owner(side, t):
            i = 4 if t == REST else side * 2 + t
            return remote(peer_out.at[side, :, at_tile(t)], term_in.at[:, columns(side, t)], near_ss.at[i], near_rs.at[i], peer)

        def far(tb, b):
            def give(t):
                peer_out[b, :, at_tile(t)] = part(tb, 1 if t == REST else 1 - c, t).astype(BF16)

                @pl.when(b == 1)
                def _():
                    to_peer(0, t).wait_send()

                to_peer(b, t).start()

            def add(t):
                term = part(tb, 1 if t == REST else c, t)
                to_peer(b, t).wait_recv()
                peer_in[b, :, at_tile(t)] = (term + peer_in[b, :, at_tile(t)].astype(F32)).astype(BF16)

            for t in range(2):
                give(t)
            for t in range(2):
                add(t)
                to_far(b, t).start()

            @pl.when(c == 0)
            def _():
                give(REST)

            @pl.when(c == 1)
            def _():
                add(REST)
                to_far(b, LATE).start()
                to_far(b, LAST).start()

        def near(tb):
            def give(side, t):
                peer_out[side, :, at_tile(t)] = part(tb, side, t).astype(BF16)
                to_owner(side, t).start()

            def both(side, _):
                for t in range(2):
                    give(side, t)

            for t in range(2):
                to_peer(1, t).wait_send()
                own(t).wait_send()

            @pl.when(c == 0)
            def _():
                to_peer(1, REST).wait_send()

            for b in range(2):
                passed(b).wait_send()
            lax.fori_loop(0, 2, both, None)
            give(1, REST)

        def mine(tb):
            def keep(side, t):
                acc_s[:, columns(side, t)] = xs[rows(tb), columns(side, t)].astype(F32) + part(tb, side, t)

            def both(side, _):
                for t in range(2):
                    keep(side, t)

            lax.fori_loop(0, 2, both, None)
            keep(1, REST)

        def step(it, _):
            b = it - 2
            away = (it >= 2) & (it < 4)
            tb = jnp.where(it < 4, lax.rem(2 * p + it, 4), 2 * p + lax.rem(it + 1 + c, 2))

            @pl.when(away)
            def _():
                remote(came(b), came(b), x_ss.at[0], x_rs.at[b], cross).wait_recv()
                passed(b).start()
                passed(b).wait_recv()

            @pl.when(it < 4)
            def _():
                norm(tb)
                project(tb, it == 0)

            @pl.when(it == 2)
            def _():
                load_wo.wait()

            @pl.when(it >= 2)
            def _():
                attend(tb)

            @pl.when(away)
            def _():
                far(tb, b)

            @pl.when(it == 4)
            def _():
                near(tb)

            @pl.when(it == 5)
            def _():
                mine(tb)

        lax.fori_loop(0, 6, step, None)

        def finish(side, t):
            here = columns(side, t)
            far_in[:, here] = (acc_s[:, here] + term_in[:, here].astype(F32) + far_in[:, here].astype(F32)).astype(BF16)

        def sums(side, t):
            return remote(peer_in.at[0, :, at_tile(t)], far_in.at[:, columns(side, t)], far_ss.at[t], far_rs.at[came_at(side, t)], cross)

        def main(side, _):
            for t in range(2):
                sums(side, t).wait_recv()
                to_owner(side, t).wait_recv()
                finish(side, t)

        lax.fori_loop(0, 2, main, None)
        to_owner(1, REST).wait_recv()
        rest_at = columns(1, REST)
        acc_s[:, rest_at] = acc_s[:, rest_at] + term_in[:, rest_at].astype(F32)

        for i in range(2):
            for t in range(2):
                to_far(i, t).wait_send()
                to_owner(i, t).wait_send()
        to_owner(1, REST).wait_send()
        across(2, x_ss.at[1]).wait_send()

        @pl.when(c == 0)
        def _():
            across(0, first_ss.at[0]).wait_send()
            across(1, x_ss.at[0]).wait_send()

        @pl.when(c == 1)
        def _():
            across(1, first_ss.at[0]).wait_send()
            across(0, x_ss.at[0]).wait_send()
            to_far(0, LATE).wait_send()
            to_far(0, LAST).wait_send()

        for t in (LATE, LAST):
            sums(1, t).wait_recv()
            here = columns(1, t)
            far_in[:, here] = (acc_s[:, here] + far_in[:, here].astype(F32)).astype(BF16)

        @pl.when(c == 1)
        def _():
            to_far(1, LATE).wait_send()
            to_far(1, LAST).wait_send()

    dma = pltpu.SemaphoreType.DMA
    near = dma((5,))
    pl.run_scoped(rest, dma((6,)), near, near, dma((2,)), dma((3,)), dma((3,)), dma((10,)), dma((6,)))


def _table(tokens):
    half = HEAD // 2
    angle = np.arange(tokens)[:, None] * float(THETA) ** (-np.arange(half) / half)
    cos, sin = np.cos(angle), np.sin(angle)
    return np.concatenate([cos, cos, -sin, sin], 1).astype(np.float32)


def solution(mesh):
    def step(x, gain, wq, wk, wv, wo):
        n, d = x.shape
        tokens = 4 * n
        nq, nk = wq.shape[1], wk.shape[1]
        side = TILES[REST][0] + TILES[REST][1]
        vmem, dma = pltpu.VMEM, pltpu.SemaphoreType.DMA
        return pl.pallas_call(
            _layer,
            out_shape=pltpu.VMEM((n, d), BF16),
            in_specs=[pl.BlockSpec(memory_space=pltpu.HBM)] * 7,
            out_specs=pl.BlockSpec(memory_space=pltpu.VMEM),
            scratch_shapes=[
                vmem((tokens, d), BF16), vmem((n, d), BF16), vmem((d,), BF16), vmem((1, d), F32), vmem((tokens, 2 * HEAD), F32),
                vmem(wq.shape, BF16), vmem(wk.shape, BF16), vmem(wv.shape, BF16), vmem(wo.shape, BF16),
                vmem((tokens, nq), BF16), vmem((tokens, nk), BF16), vmem((nk // HEAD, HEAD + 16, tokens), BF16),
                vmem((nq // HEAD, n), F32), vmem((nq // HEAD, HEAD + 16, n), F32),
                vmem((2, n, side), BF16), vmem((2, n, side), BF16), vmem((n, d), BF16), vmem((n, d), F32),
                dma((1,)), dma((1,)), dma((2,)), pltpu.SemaphoreType.REGULAR,
            ],
            compiler_params=pltpu.CompilerParams(collective_id=0, has_side_effects=True, vmem_limit_bytes=VMEM),
        )(x, gain, _table(tokens), wq, wk, wv, wo)

    tokens, columns = P(("dp", "tp"), None), P(None, "tp")
    return jax.shard_map(
        step,
        mesh=mesh,
        in_specs=(tokens, P(None), columns, columns, columns, P("tp", None)),
        out_specs=tokens,
        check_vma=False,
    )
```
